32 devices in a mesh: dp: 4 (over y, z), sp: 8 (over x, core).
Axes of the slice: x: 4, y: 2, z: 2, core: 2. Of those that a mesh axis runs over, the one named last changes fastest.
The devices are a block of a 4x4x8 slice.
Arguments:
- hidden: bfloat16 [8192, 4096], P(('dp', 'sp')), parts along dimension 0
- w_q: bfloat16 [4096, 4096], replicated
- w_k: bfloat16 [4096, 1024], replicated
- w_v: bfloat16 [4096, 1024], replicated
- w_o: bfloat16 [4096, 4096], replicated
- expert_ids: int32 [8192, 2], P(('dp', 'sp')), parts along dimension 0
- router_probs: float32 [8192, 16], P(('dp', 'sp')), parts along dimension 0
Outputs:
- output 1: bfloat16 [8192, 4096], P(('dp', 'sp')), parts along dimension 0
- output 2: bfloat16 [64, 2048, 4096], P(('dp', 'sp')), parts along dimension 0
There are 4 independent parts. The reference program is written for one: setup_inputs(seed, part) draws one part's arguments, and reference() takes and returns one part's arrays. A program takes and returns all parts, laid end to end along the dimension named above; an argument that names none is the same for every part.
All inputs are finite; a program needn't handle non-finite values.
Results may differ from the reference program's by a relative error of at most 0.00968718.
Values are sent between devices in bfloat16 or wider.
A program may use at most 768 MiB of HBM per device.

```python
import math
import jax
import jax.numpy as jnp
from jax import lax

D = 4096
HEADS = 32
KV_HEADS = 8
HEAD = 128
EXPERTS = 16
TOKENS_DEV = 256
GROUP = 8

SEQ = TOKENS_DEV * GROUP
Q_PER_KV = HEADS // KV_HEADS
Q_WIDTH = HEADS * HEAD
KV_WIDTH = KV_HEADS * HEAD
SCORE_SCALE = 1.0 / math.sqrt(HEAD)


def draw_routes(route_key):
    key_first, key_second, key_pick, key_cold, key_order = jax.random.split(route_key, 5)
    hot_first = jax.random.randint(key_first, (), 0, EXPERTS)
    hot_second = (hot_first + 1 + jax.random.randint(key_second, (), 0, EXPERTS - 1)) % EXPERTS
    pick_hot = jax.random.randint(key_pick, (SEQ,), 0, 2)
    cold_ids = (hot_first + 1 + jax.random.randint(key_cold, (SEQ,), 0, EXPERTS - 1)) % EXPERTS
    other_ids = jnp.where(pick_hot == 1, hot_second, cold_ids)
    first_ids = jnp.full((SEQ,), hot_first)
    swap_bits = jax.random.randint(key_order, (SEQ,), 0, 2)
    col_zero = jnp.where(swap_bits == 1, other_ids, first_ids)
    col_one = jnp.where(swap_bits == 1, first_ids, other_ids)
    return jnp.stack([col_zero, col_one], axis=1).astype(jnp.int32)


def setup_inputs(seed: int = 0, part: int = 0) -> dict:
    base_key = jax.random.key(seed)
    part_key = jax.random.fold_in(base_key, part)
    weight_keys = jax.random.split(base_key, 4)
    part_keys = jax.random.split(part_key, 3)
    q_gain = math.sqrt(0.5 * math.log(SEQ))
    o_gain = 0.5 * SEQ ** 0.25
    hidden = jax.random.normal(part_keys[0], (SEQ, D), jnp.float32).astype(jnp.bfloat16)
    w_q = (jax.random.normal(weight_keys[0], (D, Q_WIDTH), jnp.float32) * (q_gain / math.sqrt(D))).astype(jnp.bfloat16)
    w_k = (jax.random.normal(weight_keys[1], (D, KV_WIDTH), jnp.float32) / math.sqrt(D)).astype(jnp.bfloat16)
    w_v = (jax.random.normal(weight_keys[2], (D, KV_WIDTH), jnp.float32) / math.sqrt(D)).astype(jnp.bfloat16)
    w_o = (jax.random.normal(weight_keys[3], (Q_WIDTH, D), jnp.float32) * (o_gain / math.sqrt(Q_WIDTH))).astype(jnp.bfloat16)
    expert_ids = draw_routes(part_keys[1])
    router_probs = jax.nn.softmax(1.5 * jax.random.normal(part_keys[2], (SEQ, EXPERTS), jnp.float32), axis=1)
    return {'hidden': hidden, 'w_q': w_q, 'w_k': w_k, 'w_v': w_v, 'w_o': w_o, 'expert_ids': expert_ids, 'router_probs': router_probs}


def reference(hidden, w_q, w_k, w_v, w_o, expert_ids, router_probs):
    q_all = jnp.dot(hidden, w_q, preferred_element_type=jnp.float32).astype(jnp.bfloat16)
    k_all = jnp.dot(hidden, w_k, preferred_element_type=jnp.float32).astype(jnp.bfloat16)
    v_all = jnp.dot(hidden, w_v, preferred_element_type=jnp.float32).astype(jnp.bfloat16)
    q_groups = q_all.reshape(SEQ, KV_HEADS, Q_PER_KV, HEAD).transpose(1, 0, 2, 3)
    k_groups = k_all.reshape(SEQ, KV_HEADS, HEAD).transpose(1, 0, 2)
    v_groups = v_all.reshape(SEQ, KV_HEADS, HEAD).transpose(1, 0, 2)
    positions = jnp.arange(SEQ)
    causal = positions[:, None] >= positions[None, :]

    def one_group(group_in):
        q_grp, k_grp, v_grp = group_in
        scores = jnp.einsum('qmd,kd->mqk', q_grp.astype(jnp.float32), k_grp.astype(jnp.float32)) * SCORE_SCALE
        scores = jnp.where(causal[None, :, :], scores, -1e30)
        weights = jax.nn.softmax(scores, axis=-1).astype(jnp.bfloat16)
        out_grp = jnp.einsum('mqk,kd->qmd', weights.astype(jnp.float32), v_grp.astype(jnp.float32))
        return out_grp.astype(jnp.bfloat16)

    attn_out = lax.map(one_group, (q_groups, k_groups, v_groups))
    attn_out = attn_out.transpose(1, 0, 2, 3).reshape(SEQ, Q_WIDTH)
    out_proj = jnp.dot(attn_out, w_o, preferred_element_type=jnp.float32)
    hidden_out = (hidden.astype(jnp.float32) + out_proj).astype(jnp.bfloat16)
    picked = jnp.take_along_axis(router_probs, expert_ids, axis=1)
    gate_w = picked / jnp.sum(picked, axis=1, keepdims=True)
    gated = (gate_w[:, :, None] * hidden_out.astype(jnp.float32)[:, None, :]).astype(jnp.bfloat16)
    ids_blk = expert_ids.reshape(GROUP, TOKENS_DEV, 2)
    token_hits = jnp.sum((ids_blk[:, :, :, None] == jnp.arange(EXPERTS)).astype(jnp.int32), axis=2)
    earlier = jnp.cumsum(token_hits, axis=1) - token_hits
    slot_rank = jnp.take_along_axis(earlier, ids_blk, axis=2)
    dest_rows = jnp.arange(GROUP)[:, None, None] * TOKENS_DEV + slot_rank
    buffer = jnp.zeros((EXPERTS, GROUP * TOKENS_DEV, D), jnp.bfloat16)
    buffer = buffer.at[ids_blk, dest_rows].set(gated.reshape(GROUP, TOKENS_DEV, 2, D))
    return (hidden_out, buffer)
```

```python
import functools
import math

import jax
import jax.numpy as jnp
from jax import lax
from jax.experimental import pallas as pl
from jax.experimental.pallas import tpu as pltpu
from jax.sharding import PartitionSpec as P

HEAD = 128
EXP2_SCALE = math.log2(math.e) / math.sqrt(HEAD)
MESH = pl.DeviceIdType.MESH
TILE = 512
SLOTS = 8
PER_TILE = TILE // HEAD
VMEM_LIMIT = 67_000_000


def block_kernel(group, n_exp, x_hbm, wq, wk, wv, wo, ids_ref, probs_ref, h_all, meta_all,
                 xb, wbuf, kv, q_s, acc, ml, o_s, h_s, meta_s,
                 x_sem, w_sem, k_send, kr_l, kr_r, kr_o, kr_p, h_send, hr_l, hr_r, hr_o, hr_p, m_send, m_recv, m_loc):
    tok = xb.shape[0]
    q_tiles = wq.shape[1] // TILE
    kv_tiles = 2 * wk.shape[1] // TILE
    k_tiles = kv_tiles // 2
    o_tiles = wo.shape[1] // TILE
    me = lax.axis_index("sp")
    core = lax.rem(me, 2)
    chip = lax.div(me, 2)
    right = lax.rem(me + 2, group)
    left = lax.rem(me + group - 2, group)
    partner = me + 1 - 2 * core
    opp = lax.rem(me + 4, group)
    own = pl.ds(0, tok)
    other = pl.ds(tok, tok)

    def remote(src, dst, send, recv, dev):
        return pltpu.make_async_remote_copy(src_ref=src, dst_ref=dst, send_sem=send, recv_sem=recv,
                                            device_id={"sp": dev}, device_id_type=MESH)

    def got(ref, sem):
        pltpu.make_async_copy(ref, ref, sem).wait()

    def w_copy(arr, col, slot):
        if not isinstance(col, int):
            col = pl.multiple_of(col, TILE)
        return pltpu.make_async_copy(arr.at[:, pl.ds(col, TILE)], wbuf.at[slot], w_sem.at[slot])

    x_copy = pltpu.make_async_copy(x_hbm, xb, x_sem)
    x_copy.start()
    for p in range(SLOTS):
        if p < k_tiles:
            w_copy(wk, p * TILE, p).start()
        elif p < kv_tiles:
            w_copy(wv, (p - k_tiles) * TILE, p).start()
        else:
            w_copy(wq, (p - kv_tiles) * TILE, p).start()

    barrier = pltpu.get_barrier_semaphore()
    for d in range(1, group):
        pl.semaphore_signal(barrier, inc=1, device_id={"sp": lax.rem(me + d, group)}, device_id_type=MESH)
    x_copy.wait()

    def kv_tile(p, carry):
        w_copy(wk, 0, p).wait()
        y = jnp.dot(xb[...], wbuf[p], preferred_element_type=jnp.float32).astype(jnp.bfloat16)
        for h in range(PER_TILE):
            kv[0, p, h, 0:tok, :] = y[:, h * HEAD:(h + 1) * HEAD]
        w_copy(wq, (SLOTS - kv_tiles + p) * TILE, p).start()

        @pl.when(p == 0)
        def _():
            pl.semaphore_wait(barrier, group - 1)

        src = kv.at[0, p, :, own, :]
        remote(src, kv.at[3, p, :, own, :], k_send.at[0], kr_l.at[p], right).start()
        remote(src, kv.at[1, p, :, own, :], k_send.at[1], kr_r.at[p], left).start()
        remote(src, kv.at[0, p, :, other, :], k_send.at[2], kr_p.at[0], partner).start()
        return carry

    lax.fori_loop(0, kv_tiles, kv_tile, 0)

    def q_tile(n, carry):
        slot = lax.rem(kv_tiles + n, SLOTS)
        w_copy(wq, 0, slot).wait()
        y = jnp.dot(xb[...], wbuf[slot], preferred_element_type=jnp.float32).astype(jnp.bfloat16)
        for h in range(PER_TILE):
            q_s[n, h * tok:(h + 1) * tok, :] = y[:, h * HEAD:(h + 1) * HEAD]
        w_copy(wo, n * TILE, slot).start()
        return carry

    lax.fori_loop(0, q_tiles, q_tile, 0)

    def to_partner_kv(r, p):
        remote(kv.at[r, p, :, own, :], kv.at[r, p, :, other, :], k_send.at[2 + r], kr_p.at[r], partner).start()

    for p in range(k_tiles):
        got(kv.at[3, p, :, own, :], kr_l.at[p])
        remote(kv.at[3, p, :, own, :], kv.at[2, p, :, own, :], k_send.at[6], kr_o.at[p], right).start()
        to_partner_kv(3, p)

    lane_e = lax.broadcasted_iota(jnp.int32, (tok, n_exp), 1)
    lane = lax.broadcasted_iota(jnp.int32, (tok, HEAD), 1)
    id0 = ids_ref[:, 0:1]
    id1 = ids_ref[:, 1:2]
    probs = probs_ref[...]
    p0 = jnp.sum(jnp.where(lane_e == id0, probs, 0.0), axis=1, keepdims=True)
    p1 = jnp.sum(jnp.where(lane_e == id1, probs, 0.0), axis=1, keepdims=True)
    total = p0 + p1
    hits = (lane == id0) | (lane == id1)
    before = (lax.broadcasted_iota(jnp.int32, (tok, tok), 1)
              < lax.broadcasted_iota(jnp.int32, (tok, tok), 0)).astype(jnp.float32).astype(jnp.bfloat16)
    earlier = jnp.dot(before, hits.astype(jnp.float32).astype(jnp.bfloat16), preferred_element_type=jnp.float32)
    slot_of = jnp.where(hits, earlier, -1.0)
    gate_of = jnp.where(lane == id0 + n_exp, p0 / total, jnp.where(lane == id1 + n_exp, p1 / total, 0.0))
    meta = jnp.transpose(jnp.where(lane < n_exp, slot_of, gate_of))
    meta_s[...] = meta[0:2 * n_exp, :]

    row_i = lax.broadcasted_iota(jnp.int32, (tok, tok), 0)
    col_i = lax.broadcasted_iota(jnp.int32, (tok, tok), 1)

    def attend(r, keys, first=False, diagonal=False):
        def head_group(g, carry):
            kp = lax.div(g, PER_TILE)
            kh = lax.rem(g, PER_TILE)
            k = kv[r, kp, kh, keys, :]
            v = kv[r, k_tiles + kp, kh, keys, :]
            for h in range(PER_TILE):
                rows = pl.ds(h * tok, tok)
                s = lax.dot_general(q_s[g, rows, :], k, (((1,), (1,)), ((), ())), preferred_element_type=jnp.float32)
                if diagonal:
                    s = jnp.where(row_i >= col_i, s, -1e30)
                top = jnp.max(s, axis=1, keepdims=True)
                if not first:
                    old = ml[g, rows, 0:1]
                    top = jnp.maximum(old, top)
                e = jnp.exp2((s - top) * EXP2_SCALE)
                mass = jnp.sum(e, axis=1, keepdims=True)
                out = jnp.dot(e.astype(jnp.bfloat16), v, preferred_element_type=jnp.float32)
                if not first:
                    keep = jnp.exp2((old - top) * EXP2_SCALE)
                    mass = mass + keep * ml[g, rows, 1:2]
                    out = out + keep * acc[g, rows, :]
                ml[g, rows, 0:1] = top
                ml[g, rows, 1:2] = mass
                acc[g, rows, :] = out
            return carry

        lax.fori_loop(0, q_tiles, head_group, 0)

    attend(0, own, first=True, diagonal=True)

    m_rows = meta_all.at[me]
    loc = pltpu.make_async_copy(meta_s, m_rows, m_loc)
    loc.start()
    for d in range(1, group):
        remote(meta_s, m_rows, m_send.at[d - 1], m_recv.at[d - 1], lax.rem(me + d, group)).start()

    got(kv.at[0, :, :, other, :], kr_p.at[0])

    @pl.when(core == 1)
    def _():
        attend(0, other)

    for p in range(kv_tiles):
        got(kv.at[1, p, :, own, :], kr_r.at[p])
        if p >= k_tiles:
            remote(kv.at[1, p, :, own, :], kv.at[2, p, :, own, :], k_send.at[7], kr_o.at[p], left).start()
            got(kv.at[3, p, :, own, :], kr_l.at[p])
            to_partner_kv(3, p)
        to_partner_kv(1, p)

    both = pl.ds(0, 2 * tok)
    got(kv.at[3, :, :, other, :], kr_p.at[3])

    @pl.when(chip >= 1)
    def _():
        attend(3, both)

    got(kv.at[1, :, :, other, :], kr_p.at[1])

    @pl.when(right < me)
    def _():
        attend(1, both)

    for p in range(kv_tiles):
        got(kv.at[2, p, :, own, :], kr_o.at[p])
        to_partner_kv(2, p)
    got(kv.at[2, :, :, other, :], kr_p.at[2])

    @pl.when(chip >= 2)
    def _():
        attend(2, both)

    def finish(g, carry):
        for h in range(PER_TILE):
            rows = pl.ds(h * tok, tok)
            o_s[:, pl.ds(pl.multiple_of(g * TILE + h * HEAD, HEAD), HEAD)] = (
                acc[g, rows, :] / ml[g, rows, 1:2]).astype(jnp.bfloat16)
        return carry

    lax.fori_loop(0, q_tiles, finish, 0)

    def rows_of(dev):
        return pl.ds(pl.multiple_of(dev * tok, tok), tok)

    def piece(dev, n):
        col = n * TILE
        if not isinstance(col, int):
            col = pl.multiple_of(col, TILE)
        return h_all.at[rows_of(dev), pl.ds(col, TILE)]

    def o_tile(n, carry):
        slot = lax.rem(kv_tiles + n, SLOTS)
        w_copy(wo, 0, slot).wait()
        y = jnp.dot(o_s[...], wbuf[slot], preferred_element_type=jnp.float32)
        x = xb[:, pl.ds(pl.multiple_of(n * TILE, TILE), TILE)].astype(jnp.float32)
        h_s[n] = (x + y).astype(jnp.bfloat16)
        remote(h_s.at[n], piece(me, n), h_send.at[0], hr_l.at[n], right).start()
        remote(h_s.at[n], piece(me, n), h_send.at[1], hr_r.at[n], left).start()
        remote(h_s.at[n], piece(me, n), h_send.at[2], hr_p.at[0], partner).start()
        pltpu.make_async_copy(h_s.at[n], piece(me, n), x_sem).start()
        return carry

    lax.fori_loop(0, o_tiles, o_tile, 0)

    half = o_tiles // 2
    for n in range(o_tiles):
        got(piece(left, n), hr_l.at[n])
        if n < half:
            remote(piece(left, n), piece(left, n), h_send.at[6], hr_o.at[n], right).start()
        remote(piece(left, n), piece(left, n), h_send.at[5], hr_p.at[3], partner).start()
        got(piece(right, n), hr_r.at[n])
        if n >= half:
            remote(piece(right, n), piece(right, n), h_send.at[7], hr_o.at[n], left).start()
        remote(piece(right, n), piece(right, n), h_send.at[3], hr_p.at[1], partner).start()
    for i in range(half):
        for n in (i, half + i):
            got(piece(opp, n), hr_o.at[n])
            remote(piece(opp, n), piece(opp, n), h_send.at[4], hr_p.at[2], partner).start()

    mine = h_all.at[rows_of(me)]
    got(mine, x_sem)
    for i in range(6):
        got(mine, h_send.at[i])
    half_cols = pl.ds(0, half * TILE)
    for i in (6, 7):
        got(h_all.at[rows_of(me), half_cols], h_send.at[i])
    for r in range(4):
        src = lax.rem(partner + 2 * r, group)
        got(h_all.at[rows_of(src)], hr_p.at[r])
    for i in range(6):
        got(kv.at[0, :, :, own, :], k_send.at[i])
    for i in (6, 7):
        got(kv.at[0, pl.ds(0, k_tiles), :, own, :], k_send.at[i])
    loc.wait()
    for d in range(1, group):
        got(meta_s, m_send.at[d - 1])
        got(meta_all.at[lax.rem(me + group - d, group)], m_recv.at[d - 1])


def dispatch_kernel(n_exp, own_exp, meta_ref, h_ref, hid_hbm, out_ref, hid_sem):
    s = pl.program_id(0)
    e = pl.program_id(1)
    me = lax.axis_index("sp")
    tok, width = h_ref.shape
    hid_copy = pltpu.make_async_copy(h_ref, hid_hbm, hid_sem)

    @pl.when((s == me) & (e == 0))
    def _():
        hid_copy.start()

    expert = me * own_exp + e
    slot = meta_ref[s, pl.ds(expert, 1), :]
    gate = meta_ref[s, pl.ds(n_exp + expert, 1), :]
    row = lax.broadcasted_iota(jnp.int32, (tok, tok), 0).astype(jnp.float32)
    pick = row == slot
    gate_col = jnp.sum(jnp.where(pick, gate, 0.0), axis=1, keepdims=True)
    pick = pick.astype(jnp.float32).astype(jnp.bfloat16)
    for c in range(0, width, TILE):
        got = jnp.dot(pick, h_ref[:, c:c + TILE], preferred_element_type=jnp.float32)
        out_ref[0, :, c:c + TILE] = (got * gate_col).astype(jnp.bfloat16)

    @pl.when((s == me) & (e == own_exp - 1))
    def _():
        hid_copy.wait()


def solution(mesh):
    group = mesh.shape['sp']
    row_spec = P(('dp', 'sp'), None)
    buf_spec = P(('dp', 'sp'), None, None)

    def device_step(x_loc, w_q, w_k, w_v, w_o, ids_loc, probs_loc):
        tok, width = x_loc.shape
        n_exp = probs_loc.shape[1]
        own_exp = n_exp // group
        seq = tok * group
        q_tiles = w_q.shape[1] // TILE
        kv_tiles = 2 * w_k.shape[1] // TILE
        o_tiles = width // TILE
        bf16 = jnp.bfloat16
        any_spec = pl.BlockSpec(memory_space=pl.ANY)
        vmem_spec = pl.BlockSpec(memory_space=pltpu.VMEM)
        dma = pltpu.SemaphoreType.DMA
        h_all, meta_all = pl.pallas_call(
            functools.partial(block_kernel, group, n_exp),
            out_shape=(jax.ShapeDtypeStruct((seq, width), bf16),
                       jax.ShapeDtypeStruct((group, 2 * n_exp, tok), jnp.float32)),
            in_specs=[any_spec] * 5 + [vmem_spec] * 2,
            out_specs=(any_spec, any_spec),
            scratch_shapes=[
                pltpu.VMEM((tok, width), bf16),
                pltpu.VMEM((SLOTS, width, TILE), bf16),
                pltpu.VMEM((4, kv_tiles, PER_TILE, 2 * tok, HEAD), bf16),
                pltpu.VMEM((q_tiles, PER_TILE * tok, HEAD), bf16),
                pltpu.VMEM((q_tiles, PER_TILE * tok, HEAD), jnp.float32),
                pltpu.VMEM((q_tiles, PER_TILE * tok, HEAD), jnp.float32),
                pltpu.VMEM((tok, q_tiles * TILE), bf16),
                pltpu.VMEM((o_tiles, tok, TILE), bf16),
                pltpu.VMEM((2 * n_exp, tok), jnp.float32),
                dma, dma((SLOTS,)),
                dma((8,)), dma((kv_tiles,)), dma((kv_tiles,)), dma((kv_tiles,)), dma((4,)),
                dma((8,)), dma((o_tiles,)), dma((o_tiles,)), dma((o_tiles,)), dma((4,)),
                dma((group - 1,)), dma((group - 1,)), dma,
            ],
            compiler_params=pltpu.CompilerParams(collective_id=0, has_side_effects=True,
                                                 vmem_limit_bytes=VMEM_LIMIT),
            name="block",
        )(x_loc, w_q, w_k, w_v, w_o, ids_loc, probs_loc)

        hidden_out, buf = pl.pallas_call(
            functools.partial(dispatch_kernel, n_exp, own_exp),
            out_shape=(jax.ShapeDtypeStruct((tok, width), bf16),
                       jax.ShapeDtypeStruct((own_exp, seq, width), bf16)),
            grid=(group, own_exp),
            in_specs=[pl.BlockSpec((group, 2 * n_exp, tok), lambda s, e: (0, 0, 0)),
                      pl.BlockSpec((tok, width), lambda s, e: (s, 0))],
            out_specs=(any_spec, pl.BlockSpec((1, tok, width), lambda s, e: (e, s, 0))),
            scratch_shapes=[dma],
            compiler_params=pltpu.CompilerParams(dimension_semantics=("arbitrary", "arbitrary")),
            name="dispatch",
        )(meta_all, h_all)
        return hidden_out, buf

    return jax.shard_map(device_step, mesh=mesh,
                         in_specs=(row_spec, P(), P(), P(), P(), row_spec, row_spec),
                         out_specs=(row_spec, buf_spec), check_vma=False)
```

```python
import functools
import math

import jax
import jax.numpy as jnp
from jax import lax
from jax.experimental import pallas as pl
from jax.experimental.pallas import tpu as pltpu
from jax.sharding import PartitionSpec as P

HEAD = 128
EXP2_SCALE = math.log2(math.e) / math.sqrt(HEAD)
MESH = pl.DeviceIdType.MESH
TILE = 512
SLOTS = 8
PER_TILE = TILE // HEAD
VMEM_LIMIT = 67_000_000
OUT_SLOTS = 10


def block_kernel(group, n_exp, x_hbm, wq, wk, wv, wo, ids_ref, probs_ref, h_all, meta_all,
                 xb, wbuf, kb, vb, q_s, acc, top_s, mass_s, keep_s, s_b, e_b, o_s, h_s, meta_s,
                 x_sem, w_sem, k_send, kr_l, kr_r, kr_o, kr_p, h_send, hr_l, hr_r, hr_o, hr_p, m_send, m_recv, m_loc):
    tok = xb.shape[0]
    chips = group // 2
    q_tiles = wq.shape[1] // TILE
    k_tiles = wk.shape[1] // TILE
    kv_tiles = 2 * k_tiles
    o_tiles = wo.shape[1] // TILE
    me = lax.axis_index("sp")
    core = lax.rem(me, 2)
    chip = lax.div(me, 2)
    right = lax.rem(me + 2, group)
    left = lax.rem(me + group - 2, group)
    partner = me + 1 - 2 * core
    opp = lax.rem(me + 4, group)
    last = chips - 1

    def remote(src, dst, send, recv, dev):
        return pltpu.make_async_remote_copy(src_ref=src, dst_ref=dst, send_sem=send, recv_sem=recv,
                                            device_id={"sp": dev}, device_id_type=MESH)

    def got(ref, sem):
        pltpu.make_async_copy(ref, ref, sem).wait()

    def w_copy(arr, col, slot):
        if not isinstance(col, int):
            col = pl.multiple_of(col, TILE)
        return pltpu.make_async_copy(arr.at[:, pl.ds(col, TILE)], wbuf.at[slot], w_sem.at[slot])

    x_copy = pltpu.make_async_copy(x_hbm, xb, x_sem)
    x_copy.start()
    for p in range(SLOTS):
        if p < k_tiles:
            w_copy(wk, p * TILE, p).start()
        elif p < kv_tiles:
            w_copy(wv, (p - k_tiles) * TILE, p).start()
        else:
            w_copy(wq, (p - kv_tiles) * TILE, p).start()

    barrier = pltpu.get_barrier_semaphore()
    for d in range(1, group):
        pl.semaphore_signal(barrier, inc=1, device_id={"sp": lax.rem(me + d, group)}, device_id_type=MESH)
    x_copy.wait()

    sends_right = chip < last
    sends_left_k = chip == 0
    sends_left_v = chip < 2
    gets_left = chip > 0
    gets_right_k = chip == last
    gets_right_v = (chip == last) | (chip == 0)
    fwd_k = (chip > 0) & (chip < last)
    fwd_v = (chip == last) | (chip == 0)
    gets_opp = chip >= 2

    def k_tile(p, carry):
        w_copy(wk, 0, p).wait()
        y = jnp.dot(xb[...], wbuf[p], preferred_element_type=jnp.float32).astype(jnp.bfloat16)
        for h in range(PER_TILE):
            kb[0, 0, p, h] = y[:, h * HEAD:(h + 1) * HEAD]
        w_copy(wq, (SLOTS - kv_tiles + p) * TILE, p).start()

        @pl.when(p == 0)
        def _():
            pl.semaphore_wait(barrier, group - 1)

        src = kb.at[0, 0, p]

        @pl.when(sends_right)
        def _():
            remote(src, kb.at[3, 0, p], k_send.at[0], kr_l.at[p], right).start()

        @pl.when(sends_left_k)
        def _():
            remote(src, kb.at[1, 0, p], k_send.at[1], kr_r.at[p], left).start()

        @pl.when(core == 0)
        def _():
            remote(src, kb.at[0, 1, p], k_send.at[2], kr_p.at[0], partner).start()

        return carry

    lax.fori_loop(0, k_tiles, k_tile, 0)

    def v_tile(p, carry):
        w_copy(wv, 0, k_tiles + p).wait()
        y = jnp.dot(xb[...], wbuf[k_tiles + p], preferred_element_type=jnp.float32)
        for h in range(PER_TILE):
            vb[0, 0, p, h] = jnp.transpose(y[:, h * HEAD:(h + 1) * HEAD]).astype(jnp.bfloat16)
        w_copy(wq, (SLOTS - k_tiles + p) * TILE, k_tiles + p).start()
        src = vb.at[0, 0, p]

        @pl.when(sends_right)
        def _():
            remote(src, vb.at[3, 0, p], k_send.at[3], kr_l.at[k_tiles + p], right).start()

        @pl.when(sends_left_v)
        def _():
            remote(src, vb.at[1, 0, p], k_send.at[4], kr_r.at[k_tiles + p], left).start()

        @pl.when(core == 0)
        def _():
            remote(src, vb.at[0, 1, p], k_send.at[5], kr_p.at[4], partner).start()

        return carry

    lax.fori_loop(0, k_tiles, v_tile, 0)

    def q_tile(n, carry):
        slot = lax.rem(kv_tiles + n, SLOTS)
        w_copy(wq, 0, slot).wait()
        y = jnp.dot(xb[...], wbuf[slot], preferred_element_type=jnp.float32).astype(jnp.bfloat16)
        for h in range(PER_TILE):
            q_s[n, h] = y[:, h * HEAD:(h + 1) * HEAD]
        w_copy(wo, n * TILE, slot).start()
        return carry

    lax.fori_loop(0, q_tiles, q_tile, 0)

    def k_partner(r, p):
        remote(kb.at[r, 0, p], kb.at[r, 1, p], k_send.at[5 + r], kr_p.at[r], partner).start()

    def v_partner(r, p):
        remote(vb.at[r, 0, p], vb.at[r, 1, p], k_send.at[8 + r], kr_p.at[4 + r], partner).start()

    @pl.when(gets_left)
    def _():
        for p in range(k_tiles):
            got(kb.at[3, 0, p], kr_l.at[p])

            @pl.when(fwd_k)
            def _():
                remote(kb.at[3, 0, p], kb.at[2, 0, p], k_send.at[12], kr_o.at[p], right).start()

            k_partner(3, p)

    expert = lax.broadcasted_iota(jnp.int32, (n_exp, tok), 0)
    hit0 = expert == ids_ref[0:1, :]
    hit1 = expert == ids_ref[1:2, :]
    probs = probs_ref[...]
    p0 = jnp.sum(jnp.where(hit0, probs, 0.0), axis=0, keepdims=True)
    p1 = jnp.sum(jnp.where(hit1, probs, 0.0), axis=0, keepdims=True)
    total = p0 + p1
    hits = hit0 | hit1
    before = (lax.broadcasted_iota(jnp.int32, (tok, tok), 0)
              < lax.broadcasted_iota(jnp.int32, (tok, tok), 1)).astype(jnp.float32).astype(jnp.bfloat16)
    earlier = jnp.dot(hits.astype(jnp.float32).astype(jnp.bfloat16), before, preferred_element_type=jnp.float32)
    meta_s[0:n_exp, :] = jnp.where(hits, earlier, -1.0)
    meta_s[n_exp:2 * n_exp, :] = jnp.where(hit0, p0 / total, jnp.where(hit1, p1 / total, 0.0))

    def attend(r, parts, first=False, diagonal=False):
        keys = parts * tok
        every = pl.ds(0, keys)
        if diagonal:
            key_i = lax.broadcasted_iota(jnp.int32, (tok, tok), 0)
            row_i = lax.broadcasted_iota(jnp.int32, (tok, tok), 1)
            seen = row_i >= key_i

        def score(g, h):
            kp = lax.div(g, PER_TILE)
            kh = lax.rem(g, PER_TILE)
            q = q_s[g, h]
            top = None if first else top_s[g, h]
            old = top
            for o in range(parts):
                s = lax.dot_general(kb[r, o, kp, kh], q, (((1,), (1,)), ((), ())), preferred_element_type=jnp.float32)
                if diagonal and o == 0:
                    s = jnp.where(seen, s, -1e30)
                s_b[h % 2, o] = s
                high = jnp.max(s, axis=0, keepdims=True)
                top = high if top is None else jnp.maximum(top, high)
            top_s[g, h] = top
            if not first:
                keep_s[h] = jnp.exp2((old - top) * EXP2_SCALE)

        def weigh(g, h):
            top = top_s[g, h]
            mass = None
            for o in range(parts):
                e = jnp.exp2((s_b[h % 2, o] - top) * EXP2_SCALE)
                e_b[h % 2, o * tok:(o + 1) * tok, :] = e.astype(jnp.bfloat16)
                part = jnp.sum(e, axis=0, keepdims=True)
                mass = part if mass is None else mass + part
            mass_s[g, h] = mass if first else mass + keep_s[h] * mass_s[g, h]

        def apply(g, h, into):
            kp = lax.div(g, PER_TILE)
            kh = lax.rem(g, PER_TILE)
            v = jnp.concatenate([vb[r, o, kp, kh] for o in range(parts)], axis=1)
            out = jnp.dot(v, e_b[h % 2, every, :], preferred_element_type=jnp.float32)
            acc[into, h] = out if first else out + keep_s[h] * acc[into, h]

        last_h = PER_TILE - 1

        def head_group(g, carry):
            below = jnp.maximum(g - 1, 0)
            into = lax.select(g == 0, q_tiles, g - 1)
            above = jnp.minimum(g + 1, q_tiles - 1)
            for h in range(PER_TILE):
                if h < last_h:
                    score(g, h + 1)
                else:
                    score(above, 0)
                weigh(g, h)
                if h > 0:
                    apply(g, h - 1, g)
                else:
                    apply(below, last_h, into)
            return carry

        score(0, 0)
        lax.fori_loop(0, q_tiles, head_group, 0)
        apply(q_tiles - 1, last_h, q_tiles - 1)

    acc[q_tiles, PER_TILE - 1] = jnp.zeros((HEAD, tok), jnp.float32)
    e_b[(PER_TILE - 1) % 2] = jnp.zeros((2 * tok, tok), jnp.bfloat16)
    keep_s[PER_TILE - 1] = jnp.zeros((1, tok), jnp.float32)

    @pl.when(core == 0)
    def _():
        attend(0, 1, first=True, diagonal=True)

    @pl.when(core == 1)
    def _():
        got(kb.at[0, 1], kr_p.at[0])
        got(vb.at[0, 1], kr_p.at[4])
        attend(0, 2, first=True, diagonal=True)

    m_rows = meta_all.at[me]
    loc = pltpu.make_async_copy(meta_s, m_rows, m_loc)
    loc.start()
    for d in range(1, group):
        remote(meta_s, m_rows, m_send.at[d - 1], m_recv.at[d - 1], lax.rem(me + d, group)).start()

    @pl.when(gets_right_v)
    def _():
        for p in range(k_tiles):
            got(vb.at[1, 0, p], kr_r.at[k_tiles + p])
            remote(vb.at[1, 0, p], vb.at[2, 0, p], k_send.at[13], kr_o.at[k_tiles + p], left).start()

    @pl.when(gets_right_k)
    def _():
        for p in range(k_tiles):
            got(kb.at[1, 0, p], kr_r.at[p])
            k_partner(1, p)
            v_partner(1, p)

    @pl.when(gets_left)
    def _():
        for p in range(k_tiles):
            got(vb.at[3, 0, p], kr_l.at[k_tiles + p])
            v_partner(3, p)
        got(kb.at[3, 1], kr_p.at[3])
        got(vb.at[3, 1], kr_p.at[7])
        attend(3, 2)

    @pl.when(gets_right_k)
    def _():
        got(kb.at[1, 1], kr_p.at[1])
        got(vb.at[1, 1], kr_p.at[5])
        attend(1, 2)

    @pl.when(gets_opp)
    def _():
        for p in range(k_tiles):
            got(kb.at[2, 0, p], kr_o.at[p])
            k_partner(2, p)
            got(vb.at[2, 0, p], kr_o.at[k_tiles + p])
            v_partner(2, p)
        got(kb.at[2, 1], kr_p.at[2])
        got(vb.at[2, 1], kr_p.at[6])
        attend(2, 2)

    def finish(g, carry):
        for h in range(PER_TILE):
            o = jnp.transpose(acc[g, h] * (1.0 / mass_s[g, h]))
            o_s[:, pl.ds(pl.multiple_of(g * TILE + h * HEAD, HEAD), HEAD)] = o.astype(jnp.bfloat16)
        return carry

    lax.fori_loop(0, q_tiles, finish, 0)

    def rows_of(dev):
        return pl.ds(pl.multiple_of(dev * tok, tok), tok)

    def piece(dev, n):
        col = n * TILE
        if not isinstance(col, int):
            col = pl.multiple_of(col, TILE)
        return h_all.at[rows_of(dev), pl.ds(col, TILE)]

    def o_tile(n, carry):
        slot = lax.rem(kv_tiles + n, SLOTS)
        w_copy(wo, 0, slot).wait()
        y = jnp.dot(o_s[...], wbuf[slot], preferred_element_type=jnp.float32)
        x = xb[:, pl.ds(pl.multiple_of(n * TILE, TILE), TILE)].astype(jnp.float32)
        h_s[n] = (x + y).astype(jnp.bfloat16)
        remote(h_s.at[n], piece(me, n), h_send.at[0], hr_l.at[n], right).start()
        remote(h_s.at[n], piece(me, n), h_send.at[1], hr_r.at[n], left).start()
        remote(h_s.at[n], piece(me, n), h_send.at[2], hr_p.at[0], partner).start()
        pltpu.make_async_copy(h_s.at[n], piece(me, n), x_sem).start()
        return carry

    lax.fori_loop(0, o_tiles, o_tile, 0)

    def from_left():
        for n in range(o_tiles):
            got(piece(left, n), hr_l.at[n])
            if n % 2 == 0:
                remote(piece(left, n), piece(left, n), h_send.at[6], hr_o.at[n], right).start()
            remote(piece(left, n), piece(left, n), h_send.at[5], hr_p.at[3], partner).start()

    def from_right():
        for n in range(o_tiles):
            got(piece(right, n), hr_r.at[n])
            if n % 2 == 1:
                remote(piece(right, n), piece(right, n), h_send.at[7], hr_o.at[n], left).start()
            remote(piece(right, n), piece(right, n), h_send.at[3], hr_p.at[1], partner).start()

    early_right = (chip == 0) | (chip == last)

    @pl.when(early_right)
    def _():
        from_right()
        from_left()

    @pl.when(jnp.logical_not(early_right))
    def _():
        from_left()
        from_right()

    for n in range(o_tiles):
        got(piece(opp, n), hr_o.at[n])
        remote(piece(opp, n), piece(opp, n), h_send.at[4], hr_p.at[2], partner).start()

    mine = h_all.at[rows_of(me)]
    got(mine, x_sem)
    for i in range(6):
        got(mine, h_send.at[i])
    for i in (6, 7):
        got(h_all.at[rows_of(me), pl.ds(0, o_tiles // 2 * TILE)], h_send.at[i])
    for r in range(chips):
        got(h_all.at[rows_of(lax.rem(partner + 2 * r, group))], hr_p.at[r])
    k_own = kb.at[0, 0]
    v_own = vb.at[0, 0]
    for when, waits in ((sends_right, ((k_own, 0), (v_own, 3))), (sends_left_k, ((k_own, 1),)), (sends_left_v, ((v_own, 4),)),
                        (core == 0, ((k_own, 2), (v_own, 5))), (gets_left, ((k_own, 8), (v_own, 11))),
                        (gets_right_k, ((k_own, 6), (v_own, 9))), (gets_opp, ((k_own, 7), (v_own, 10))),
                        (fwd_k, ((k_own, 12),)), (fwd_v, ((v_own, 13),))):
        @pl.when(when)
        def _(waits=waits):
            for ref, i in waits:
                got(ref, k_send.at[i])

    loc.wait()
    for d in range(1, group):
        got(meta_s, m_send.at[d - 1])
        got(meta_all.at[lax.rem(me + group - d, group)], m_recv.at[d - 1])


def dispatch_kernel(n_exp, own_exp, meta_ref, h_hbm, hid_hbm, buf_hbm, hb, ob, h_sem, o_sem, hid_sem):
    group, tok, width = hb.shape
    slots = ob.shape[0]
    me = lax.axis_index("sp")
    steps = group * own_exp
    row = lax.broadcasted_iota(jnp.int32, (tok, tok), 0).astype(jnp.float32)

    def h_copy(s):
        return pltpu.make_async_copy(h_hbm.at[pl.ds(s * tok, tok)], hb.at[s], h_sem.at[s])

    def o_copy(i):
        s = lax.div(i, own_exp)
        return pltpu.make_async_copy(ob.at[lax.rem(i, slots)],
                                     buf_hbm.at[lax.rem(i, own_exp), pl.ds(pl.multiple_of(s * tok, tok), tok)],
                                     o_sem.at[lax.rem(i, slots)])

    for s in range(group):
        h_copy(s).start()

    def step(i, carry):
        s = lax.div(i, own_exp)
        e = lax.rem(i, own_exp)

        @pl.when(e == 0)
        def _():
            pltpu.make_async_copy(hb.at[s], hb.at[s], h_sem.at[s]).wait()

            @pl.when(s == me)
            def _():
                pltpu.make_async_copy(hb.at[s], hid_hbm, hid_sem).start()

        @pl.when(i >= slots)
        def _():
            o_copy(i - slots).wait()

        expert = me * own_exp + e
        slot = meta_ref[s, pl.ds(expert, 1), :]
        gate = meta_ref[s, pl.ds(n_exp + expert, 1), :]
        pick = row == slot
        gate_col = jnp.sum(jnp.where(pick, gate, 0.0), axis=1, keepdims=True)
        pick = pick.astype(jnp.float32).astype(jnp.bfloat16)
        o = lax.rem(i, slots)
        for c in range(0, width, TILE):
            rows = jnp.dot(pick, hb[s, :, c:c + TILE], preferred_element_type=jnp.float32)
            ob[o, :, c:c + TILE] = (rows * gate_col).astype(jnp.bfloat16)
        o_copy(i).start()
        return carry

    lax.fori_loop(0, steps, step, 0)
    for i in range(steps - slots, steps):
        o_copy(i).wait()
    pltpu.make_async_copy(hb.at[0], hid_hbm, hid_sem).wait()


def solution(mesh):
    group = mesh.shape['sp']
    row_spec = P(('dp', 'sp'), None)
    buf_spec = P(('dp', 'sp'), None, None)

    def device_step(x_loc, w_q, w_k, w_v, w_o, ids_loc, probs_loc):
        tok, width = x_loc.shape
        n_exp = probs_loc.shape[1]
        own_exp = n_exp // group
        seq = tok * group
        q_tiles = w_q.shape[1] // TILE
        k_tiles = w_k.shape[1] // TILE
        chips = group // 2
        o_tiles = width // TILE
        bf16 = jnp.bfloat16
        any_spec = pl.BlockSpec(memory_space=pl.ANY)
        vmem_spec = pl.BlockSpec(memory_space=pltpu.VMEM)
        dma = pltpu.SemaphoreType.DMA
        h_all, meta_all = pl.pallas_call(
            functools.partial(block_kernel, group, n_exp),
            out_shape=(jax.ShapeDtypeStruct((seq, width), bf16),
                       jax.ShapeDtypeStruct((group, 2 * n_exp, tok), jnp.float32)),
            in_specs=[any_spec] * 5 + [vmem_spec] * 2,
            out_specs=(any_spec, any_spec),
            scratch_shapes=[
                pltpu.VMEM((tok, width), bf16),
                pltpu.VMEM((SLOTS, width, TILE), bf16),
                pltpu.VMEM((chips, 2, k_tiles, PER_TILE, tok, HEAD), bf16),
                pltpu.VMEM((chips, 2, k_tiles, PER_TILE, HEAD, tok), bf16),
                pltpu.VMEM((q_tiles, PER_TILE, tok, HEAD), bf16),
                pltpu.VMEM((q_tiles + 1, PER_TILE, HEAD, tok), jnp.float32),
                pltpu.VMEM((q_tiles, PER_TILE, 1, tok), jnp.float32),
                pltpu.VMEM((q_tiles, PER_TILE, 1, tok), jnp.float32),
                pltpu.VMEM((PER_TILE, 1, tok), jnp.float32),
                pltpu.VMEM((2, 2, tok, tok), jnp.float32),
                pltpu.VMEM((2, 2 * tok, tok), bf16),
                pltpu.VMEM((tok, q_tiles * TILE), bf16),
                pltpu.VMEM((o_tiles, tok, TILE), bf16),
                pltpu.VMEM((2 * n_exp, tok), jnp.float32),
                dma, dma((SLOTS,)),
                dma((14,)), dma((2 * k_tiles,)), dma((2 * k_tiles,)), dma((2 * k_tiles,)), dma((2 * chips,)),
                dma((8,)), dma((o_tiles,)), dma((o_tiles,)), dma((o_tiles,)), dma((chips,)),
                dma((group - 1,)), dma((group - 1,)), dma,
            ],
            compiler_params=pltpu.CompilerParams(collective_id=0, has_side_effects=True,
                                                 vmem_limit_bytes=VMEM_LIMIT),
            name="block",
        )(x_loc, w_q, w_k, w_v, w_o, ids_loc.T, probs_loc.T)

        hidden_out, buf = pl.pallas_call(
            functools.partial(dispatch_kernel, n_exp, own_exp),
            out_shape=(jax.ShapeDtypeStruct((tok, width), bf16),
                       jax.ShapeDtypeStruct((own_exp, seq, width), bf16)),
            in_specs=[vmem_spec, any_spec],
            out_specs=(any_spec, any_spec),
            scratch_shapes=[pltpu.VMEM((group, tok, width), bf16), pltpu.VMEM((OUT_SLOTS, tok, width), bf16),
                            dma((group,)), dma((OUT_SLOTS,)), dma],
            compiler_params=pltpu.CompilerParams(vmem_limit_bytes=VMEM_LIMIT),
            name="dispatch",
        )(meta_all, h_all)
        return hidden_out, buf

    return jax.shard_map(device_step, mesh=mesh,
                         in_specs=(row_spec, P(), P(), P(), P(), row_spec, row_spec),
                         out_specs=(row_spec, buf_spec), check_vma=False)
```

```python
import functools
import math

import jax
import jax.numpy as jnp
from jax import lax
from jax.experimental import pallas as pl
from jax.experimental.pallas import tpu as pltpu
from jax.sharding import PartitionSpec as P

HEAD = 128
EXP2_SCALE = math.log2(math.e) / math.sqrt(HEAD)
MESH = pl.DeviceIdType.MESH
TILE = 512
SLOTS = 8
PER_TILE = TILE // HEAD
SEND_TILES = 2
VMEM_LIMIT = 67_000_000
OUT_SLOTS = 10


def block_kernel(group, n_exp, x_hbm, wq, wk, wv, wo, ids_ref, probs_ref, h_all, meta_all,
                 xb, wbuf, kb, vb, q_s, acc, top_s, mass_s, keep_s, s_b, e_b, o_s, h_s, land, meta_s,
                 x_sem, w_sem, k_send, kr_l, kr_r, kr_o, kr_p, h_send, hr_l, hr_r, hr_o, hr_p, h_loc, m_send, m_recv, m_loc):
    tok = xb.shape[0]
    chips = group // 2
    q_tiles = wq.shape[1] // TILE
    k_tiles = wk.shape[1] // TILE
    kv_tiles = 2 * k_tiles
    o_tiles = wo.shape[1] // TILE
    me = lax.axis_index("sp")
    core = lax.rem(me, 2)
    chip = lax.div(me, 2)
    right = lax.rem(me + 2, group)
    left = lax.rem(me + group - 2, group)
    partner = me + 1 - 2 * core
    opp = lax.rem(me + 4, group)
    last = chips - 1

    def remote(src, dst, send, recv, dev):
        return pltpu.make_async_remote_copy(src_ref=src, dst_ref=dst, send_sem=send, recv_sem=recv,
                                            device_id={"sp": dev}, device_id_type=MESH)

    def got(ref, sem):
        pltpu.make_async_copy(ref, ref, sem).wait()

    def w_copy(arr, col, slot):
        if not isinstance(col, int):
            col = pl.multiple_of(col, TILE)
        return pltpu.make_async_copy(arr.at[:, pl.ds(col, TILE)], wbuf.at[slot], w_sem.at[slot])

    x_copy = pltpu.make_async_copy(x_hbm, xb, x_sem)
    x_copy.start()
    for p in range(SLOTS):
        if p < k_tiles:
            w_copy(wk, p * TILE, p).start()
        elif p < kv_tiles:
            w_copy(wv, (p - k_tiles) * TILE, p).start()
        else:
            w_copy(wq, (p - kv_tiles) * TILE, p).start()

    barrier = pltpu.get_barrier_semaphore()
    for d in range(1, group):
        pl.semaphore_signal(barrier, inc=1, device_id={"sp": lax.rem(me + d, group)}, device_id_type=MESH)
    x_copy.wait()

    sends_right = chip < last
    sends_left_k = chip == 0
    sends_left_v = chip < 2
    gets_left = chip > 0
    gets_right_k = chip == last
    gets_right_v = (chip == last) | (chip == 0)
    fwd_k = (chip > 0) & (chip < last)
    fwd_v = (chip == last) | (chip == 0)
    gets_opp = chip >= 2

    def k_tile(p, carry):
        w_copy(wk, 0, p).wait()
        y = jnp.dot(xb[...], wbuf[p], preferred_element_type=jnp.float32).astype(jnp.bfloat16)
        for h in range(PER_TILE):
            kb[0, 0, p, h] = y[:, h * HEAD:(h + 1) * HEAD]
        w_copy(wq, (SLOTS - kv_tiles + p) * TILE, p).start()

        @pl.when(p == 0)
        def _():
            pl.semaphore_wait(barrier, group - 1)

        src = kb.at[0, 0, p]

        @pl.when(sends_right)
        def _():
            remote(src, kb.at[3, 0, p], k_send.at[0], kr_l.at[p], right).start()

        @pl.when(sends_left_k)
        def _():
            remote(src, kb.at[1, 0, p], k_send.at[1], kr_r.at[p], left).start()

        @pl.when(core == 0)
        def _():
            remote(src, kb.at[0, 1, p], k_send.at[2], kr_p.at[0], partner).start()

        return carry

    lax.fori_loop(0, k_tiles, k_tile, 0)

    def v_tile(p, carry):
        w_copy(wv, 0, k_tiles + p).wait()
        y = jnp.dot(xb[...], wbuf[k_tiles + p], preferred_element_type=jnp.float32)
        for h in range(PER_TILE):
            vb[0, 0, p, h] = jnp.transpose(y[:, h * HEAD:(h + 1) * HEAD]).astype(jnp.bfloat16)
        w_copy(wq, (SLOTS - k_tiles + p) * TILE, k_tiles + p).start()
        src = vb.at[0, 0, p]

        @pl.when(sends_right)
        def _():
            remote(src, vb.at[3, 0, p], k_send.at[3], kr_l.at[k_tiles + p], right).start()

        @pl.when(sends_left_v)
        def _():
            remote(src, vb.at[1, 0, p], k_send.at[4], kr_r.at[k_tiles + p], left).start()

        @pl.when(core == 0)
        def _():
            remote(src, vb.at[0, 1, p], k_send.at[5], kr_p.at[4], partner).start()

        return carry

    lax.fori_loop(0, k_tiles, v_tile, 0)

    def q_tile(n, carry):
        slot = lax.rem(kv_tiles + n, SLOTS)
        w_copy(wq, 0, slot).wait()
        y = jnp.dot(xb[...], wbuf[slot], preferred_element_type=jnp.float32).astype(jnp.bfloat16)
        for h in range(PER_TILE):
            q_s[n, h] = y[:, h * HEAD:(h + 1) * HEAD]
        w_copy(wo, n * TILE, slot).start()
        return carry

    lax.fori_loop(0, q_tiles, q_tile, 0)

    def k_partner(r, p):
        remote(kb.at[r, 0, p], kb.at[r, 1, p], k_send.at[5 + r], kr_p.at[r], partner).start()

    def v_partner(r, p):
        remote(vb.at[r, 0, p], vb.at[r, 1, p], k_send.at[8 + r], kr_p.at[4 + r], partner).start()

    @pl.when(gets_left)
    def _():
        for p in range(k_tiles):
            got(kb.at[3, 0, p], kr_l.at[p])

            @pl.when(fwd_k)
            def _():
                remote(kb.at[3, 0, p], kb.at[2, 0, p], k_send.at[12], kr_o.at[p], right).start()

            k_partner(3, p)

    expert = lax.broadcasted_iota(jnp.int32, (n_exp, tok), 0)
    hit0 = expert == ids_ref[0:1, :]
    hit1 = expert == ids_ref[1:2, :]
    probs = probs_ref[...]
    p0 = jnp.sum(jnp.where(hit0, probs, 0.0), axis=0, keepdims=True)
    p1 = jnp.sum(jnp.where(hit1, probs, 0.0), axis=0, keepdims=True)
    total = p0 + p1
    hits = hit0 | hit1
    before = (lax.broadcasted_iota(jnp.int32, (tok, tok), 0)
              < lax.broadcasted_iota(jnp.int32, (tok, tok), 1)).astype(jnp.float32).astype(jnp.bfloat16)
    earlier = jnp.dot(hits.astype(jnp.float32).astype(jnp.bfloat16), before, preferred_element_type=jnp.float32)
    meta_s[0:n_exp, :] = jnp.where(hits, earlier, -1.0)
    meta_s[n_exp:2 * n_exp, :] = jnp.where(hit0, p0 / total, jnp.where(hit1, p1 / total, 0.0))

    def attend(r, parts, first=False, diagonal=False):
        keys = parts * tok
        every = pl.ds(0, keys)
        if diagonal:
            key_i = lax.broadcasted_iota(jnp.int32, (tok, tok), 0)
            row_i = lax.broadcasted_iota(jnp.int32, (tok, tok), 1)
            seen = row_i >= key_i

        def score(g, h):
            kp = lax.div(g, PER_TILE)
            kh = lax.rem(g, PER_TILE)
            q = q_s[g, h]
            top = None if first else top_s[g, h]
            old = top
            for o in range(parts):
                s = lax.dot_general(kb[r, o, kp, kh], q, (((1,), (1,)), ((), ())), preferred_element_type=jnp.float32)
                if diagonal and o == 0:
                    s = jnp.where(seen, s, -1e30)
                s_b[h % 2, o] = s
                high = jnp.max(s, axis=0, keepdims=True)
                top = high if top is None else jnp.maximum(top, high)
            top_s[g, h] = top
            if not first:
                keep_s[h] = jnp.exp2((old - top) * EXP2_SCALE)

        def weigh(g, h):
            top = top_s[g, h]
            mass = None
            for o in range(parts):
                e = jnp.exp2((s_b[h % 2, o] - top) * EXP2_SCALE)
                e_b[h % 2, o * tok:(o + 1) * tok, :] = e.astype(jnp.bfloat16)
                part = jnp.sum(e, axis=0, keepdims=True)
                mass = part if mass is None else mass + part
            mass_s[g, h] = mass if first else mass + keep_s[h] * mass_s[g, h]

        def apply(g, h, into):
            kp = lax.div(g, PER_TILE)
            kh = lax.rem(g, PER_TILE)
            v = jnp.concatenate([vb[r, o, kp, kh] for o in range(parts)], axis=1)
            out = jnp.dot(v, e_b[h % 2, every, :], preferred_element_type=jnp.float32)
            acc[into, h] = out if first else out + keep_s[h] * acc[into, h]

        last_h = PER_TILE - 1

        def head_group(g, carry):
            below = jnp.maximum(g - 1, 0)
            into = lax.select(g == 0, q_tiles, g - 1)
            above = jnp.minimum(g + 1, q_tiles - 1)
            for h in range(PER_TILE):
                if h < last_h:
                    score(g, h + 1)
                else:
                    score(above, 0)
                weigh(g, h)
                if h > 0:
                    apply(g, h - 1, g)
                else:
                    apply(below, last_h, into)
            return carry

        score(0, 0)
        lax.fori_loop(0, q_tiles, head_group, 0)
        apply(q_tiles - 1, last_h, q_tiles - 1)

    acc[q_tiles, PER_TILE - 1] = jnp.zeros((HEAD, tok), jnp.float32)
    e_b[(PER_TILE - 1) % 2] = jnp.zeros((2 * tok, tok), jnp.bfloat16)
    keep_s[PER_TILE - 1] = jnp.zeros((1, tok), jnp.float32)

    @pl.when(core == 0)
    def _():
        attend(0, 1, first=True, diagonal=True)

    @pl.when(core == 1)
    def _():
        got(kb.at[0, 1], kr_p.at[0])
        got(vb.at[0, 1], kr_p.at[4])
        attend(0, 2, first=True, diagonal=True)

    m_rows = meta_all.at[me]
    loc = pltpu.make_async_copy(meta_s, m_rows, m_loc)
    loc.start()
    for d in range(1, group):
        remote(meta_s, m_rows, m_send.at[d - 1], m_recv.at[d - 1], lax.rem(me + d, group)).start()

    @pl.when(gets_right_v)
    def _():
        for p in range(k_tiles):
            got(vb.at[1, 0, p], kr_r.at[k_tiles + p])
            remote(vb.at[1, 0, p], vb.at[2, 0, p], k_send.at[13], kr_o.at[k_tiles + p], left).start()

    @pl.when(gets_right_k)
    def _():
        for p in range(k_tiles):
            got(kb.at[1, 0, p], kr_r.at[p])
            k_partner(1, p)
            v_partner(1, p)

    @pl.when(gets_left)
    def _():
        for p in range(k_tiles):
            got(vb.at[3, 0, p], kr_l.at[k_tiles + p])
            v_partner(3, p)
        got(kb.at[3, 1], kr_p.at[3])
        got(vb.at[3, 1], kr_p.at[7])
        attend(3, 2)

    @pl.when(gets_right_k)
    def _():
        got(kb.at[1, 1], kr_p.at[1])
        got(vb.at[1, 1], kr_p.at[5])
        attend(1, 2)

    @pl.when(gets_opp)
    def _():
        for p in range(k_tiles):
            got(kb.at[2, 0, p], kr_o.at[p])
            k_partner(2, p)
            got(vb.at[2, 0, p], kr_o.at[k_tiles + p])
            v_partner(2, p)
        got(kb.at[2, 1], kr_p.at[2])
        got(vb.at[2, 1], kr_p.at[6])
        attend(2, 2)

    def finish(g, carry):
        for h in range(PER_TILE):
            o = jnp.transpose(acc[g, h] * (1.0 / mass_s[g, h]))
            o_s[:, pl.ds(pl.multiple_of(g * TILE + h * HEAD, HEAD), HEAD)] = o.astype(jnp.bfloat16)
        return carry

    lax.fori_loop(0, q_tiles, finish, 0)

    def rows_of(dev):
        return pl.ds(pl.multiple_of(dev * tok, tok), tok)

    def piece(dev, n):
        col = n * cols
        if not isinstance(col, int):
            col = pl.multiple_of(col, cols)
        return h_all.at[rows_of(dev), pl.ds(col, cols)]

    cols = SEND_TILES * TILE
    pieces = o_tiles // SEND_TILES

    def keep(ref, dev, r, n):
        pltpu.make_async_copy(ref, piece(dev, n), h_loc.at[r]).start()
        remote(ref, piece(dev, n), h_send.at[2 + r], hr_p.at[r], partner).start()

    def o_piece(n, carry):
        for t in range(SEND_TILES):
            tile = n * SEND_TILES + t
            slot = lax.rem(kv_tiles + tile, SLOTS)
            w_copy(wo, 0, slot).wait()
            y = jnp.dot(o_s[...], wbuf[slot], preferred_element_type=jnp.float32)
            x = xb[:, pl.ds(pl.multiple_of(tile * TILE, TILE), TILE)].astype(jnp.float32)
            h_s[n, :, t * TILE:(t + 1) * TILE] = (x + y).astype(jnp.bfloat16)
        remote(h_s.at[n], land.at[0, n], h_send.at[0], hr_l.at[n], right).start()
        remote(h_s.at[n], land.at[1, n], h_send.at[1], hr_r.at[n], left).start()
        keep(h_s.at[n], me, 0, n)
        return carry

    lax.fori_loop(0, pieces, o_piece, 0)

    def from_left():
        for n in range(pieces):
            got(land.at[0, n], hr_l.at[n])
            if n % 2 == 0:
                remote(land.at[0, n], land.at[2, n], h_send.at[6], hr_o.at[n], right).start()
            keep(land.at[0, n], left, 3, n)

    def from_right():
        for n in range(pieces):
            got(land.at[1, n], hr_r.at[n])
            if n % 2 == 1:
                remote(land.at[1, n], land.at[2, n], h_send.at[7], hr_o.at[n], left).start()
            keep(land.at[1, n], right, 1, n)

    early_right = (chip == 0) | (chip == last)

    @pl.when(early_right)
    def _():
        from_right()
        from_left()

    @pl.when(jnp.logical_not(early_right))
    def _():
        from_left()
        from_right()

    for n in range(pieces):
        got(land.at[2, n], hr_o.at[n])
        keep(land.at[2, n], opp, 2, n)

    mine = h_all.at[rows_of(me)]
    for i in range(6):
        got(mine, h_send.at[i])
    for i in (6, 7):
        got(h_all.at[rows_of(me), pl.ds(0, o_tiles // 2 * TILE)], h_send.at[i])
    for r in range(chips):
        got(h_all.at[rows_of(lax.rem(me + 2 * r, group))], h_loc.at[r])
    for r in range(chips):
        got(h_all.at[rows_of(lax.rem(partner + 2 * r, group))], hr_p.at[r])
    k_own = kb.at[0, 0]
    v_own = vb.at[0, 0]
    for when, waits in ((sends_right, ((k_own, 0), (v_own, 3))), (sends_left_k, ((k_own, 1),)), (sends_left_v, ((v_own, 4),)),
                        (core == 0, ((k_own, 2), (v_own, 5))), (gets_left, ((k_own, 8), (v_own, 11))),
                        (gets_right_k, ((k_own, 6), (v_own, 9))), (gets_opp, ((k_own, 7), (v_own, 10))),
                        (fwd_k, ((k_own, 12),)), (fwd_v, ((v_own, 13),))):
        @pl.when(when)
        def _(waits=waits):
            for ref, i in waits:
                got(ref, k_send.at[i])

    loc.wait()
    for d in range(1, group):
        got(meta_s, m_send.at[d - 1])
        got(meta_all.at[lax.rem(me + group - d, group)], m_recv.at[d - 1])


def dispatch_kernel(n_exp, own_exp, meta_ref, h_hbm, hid_hbm, buf_hbm, hb, ob, h_sem, o_sem, hid_sem):
    group, tok, width = hb.shape
    slots = ob.shape[0]
    me = lax.axis_index("sp")
    steps = group * own_exp
    row = lax.broadcasted_iota(jnp.int32, (tok, tok), 0).astype(jnp.float32)

    def h_copy(s):
        return pltpu.make_async_copy(h_hbm.at[pl.ds(s * tok, tok)], hb.at[s], h_sem.at[s])

    def o_copy(i):
        s = lax.div(i, own_exp)
        return pltpu.make_async_copy(ob.at[lax.rem(i, slots)],
                                     buf_hbm.at[lax.rem(i, own_exp), pl.ds(pl.multiple_of(s * tok, tok), tok)],
                                     o_sem.at[lax.rem(i, slots)])

    for s in range(group):
        h_copy(s).start()

    def step(i, carry):
        s = lax.div(i, own_exp)
        e = lax.rem(i, own_exp)

        @pl.when(e == 0)
        def _():
            pltpu.make_async_copy(hb.at[s], hb.at[s], h_sem.at[s]).wait()

            @pl.when(s == me)
            def _():
                pltpu.make_async_copy(hb.at[s], hid_hbm, hid_sem).start()

        @pl.when(i >= slots)
        def _():
            o_copy(i - slots).wait()

        expert = me * own_exp + e
        slot = meta_ref[s, pl.ds(expert, 1), :]
        gate = meta_ref[s, pl.ds(n_exp + expert, 1), :]
        pick = row == slot
        gate_col = jnp.sum(jnp.where(pick, gate, 0.0), axis=1, keepdims=True)
        pick = pick.astype(jnp.float32).astype(jnp.bfloat16)
        o = lax.rem(i, slots)
        for c in range(0, width, TILE):
            rows = jnp.dot(pick, hb[s, :, c:c + TILE], preferred_element_type=jnp.float32)
            ob[o, :, c:c + TILE] = (rows * gate_col).astype(jnp.bfloat16)
        o_copy(i).start()
        return carry

    lax.fori_loop(0, steps, step, 0)
    for i in range(steps - slots, steps):
        o_copy(i).wait()
    pltpu.make_async_copy(hb.at[0], hid_hbm, hid_sem).wait()


def solution(mesh):
    group = mesh.shape['sp']
    row_spec = P(('dp', 'sp'), None)
    buf_spec = P(('dp', 'sp'), None, None)

    def device_step(x_loc, w_q, w_k, w_v, w_o, ids_loc, probs_loc):
        tok, width = x_loc.shape
        n_exp = probs_loc.shape[1]
        own_exp = n_exp // group
        seq = tok * group
        q_tiles = w_q.shape[1] // TILE
        k_tiles = w_k.shape[1] // TILE
        chips = group // 2
        pieces = width // (SEND_TILES * TILE)
        bf16 = jnp.bfloat16
        any_spec = pl.BlockSpec(memory_space=pl.ANY)
        vmem_spec = pl.BlockSpec(memory_space=pltpu.VMEM)
        dma = pltpu.SemaphoreType.DMA
        h_all, meta_all = pl.pallas_call(
            functools.partial(block_kernel, group, n_exp),
            out_shape=(jax.ShapeDtypeStruct((seq, width), bf16),
                       jax.ShapeDtypeStruct((group, 2 * n_exp, tok), jnp.float32)),
            in_specs=[any_spec] * 5 + [vmem_spec] * 2,
            out_specs=(any_spec, any_spec),
            scratch_shapes=[
                pltpu.VMEM((tok, width), bf16),
                pltpu.VMEM((SLOTS, width, TILE), bf16),
                pltpu.VMEM((chips, 2, k_tiles, PER_TILE, tok, HEAD), bf16),
                pltpu.VMEM((chips, 2, k_tiles, PER_TILE, HEAD, tok), bf16),
                pltpu.VMEM((q_tiles, PER_TILE, tok, HEAD), bf16),
                pltpu.VMEM((q_tiles + 1, PER_TILE, HEAD, tok), jnp.float32),
                pltpu.VMEM((q_tiles, PER_TILE, 1, tok), jnp.float32),
                pltpu.VMEM((q_tiles, PER_TILE, 1, tok), jnp.float32),
                pltpu.VMEM((PER_TILE, 1, tok), jnp.float32),
                pltpu.VMEM((2, 2, tok, tok), jnp.float32),
                pltpu.VMEM((2, 2 * tok, tok), bf16),
                pltpu.VMEM((tok, q_tiles * TILE), bf16),
                pltpu.VMEM((pieces, tok, SEND_TILES * TILE), bf16),
                pltpu.VMEM((3, pieces, tok, SEND_TILES * TILE), bf16),
                pltpu.VMEM((2 * n_exp, tok), jnp.float32),
                dma, dma((SLOTS,)),
                dma((14,)), dma((2 * k_tiles,)), dma((2 * k_tiles,)), dma((2 * k_tiles,)), dma((2 * chips,)),
                dma((8,)), dma((pieces,)), dma((pieces,)), dma((pieces,)), dma((chips,)), dma((chips,)),
                dma((group - 1,)), dma((group - 1,)), dma,
            ],
            compiler_params=pltpu.CompilerParams(collective_id=0, has_side_effects=True,
                                                 vmem_limit_bytes=VMEM_LIMIT),
            name="block",
        )(x_loc, w_q, w_k, w_v, w_o, ids_loc.T, probs_loc.T)

        hidden_out, buf = pl.pallas_call(
            functools.partial(dispatch_kernel, n_exp, own_exp),
            out_shape=(jax.ShapeDtypeStruct((tok, width), bf16),
                       jax.ShapeDtypeStruct((own_exp, seq, width), bf16)),
            in_specs=[vmem_spec, any_spec],
            out_specs=(any_spec, any_spec),
            scratch_shapes=[pltpu.VMEM((group, tok, width), bf16), pltpu.VMEM((OUT_SLOTS, tok, width), bf16),
                            dma((group,)), dma((OUT_SLOTS,)), dma],
            compiler_params=pltpu.CompilerParams(vmem_limit_bytes=VMEM_LIMIT),
            name="dispatch",
        )(meta_all, h_all)
        return hidden_out, buf

    return jax.shard_map(device_step, mesh=mesh,
                         in_specs=(row_spec, P(), P(), P(), P(), row_spec, row_spec),
                         out_specs=(row_spec, buf_spec), check_vma=False)
```

```python
import functools
import math

import jax
import jax.numpy as jnp
from jax import lax
from jax.experimental import pallas as pl
from jax.experimental.pallas import tpu as pltpu
from jax.sharding import PartitionSpec as P

HEAD = 128
EXP2_SCALE = math.log2(math.e) / math.sqrt(HEAD)
MESH = pl.DeviceIdType.MESH
TILE = 512
SLOTS = 8
PER_TILE = TILE // HEAD
AHEAD = 3
VMEM_LIMIT = 67_000_000
VIA_NEXT = ((0, 2, 3, 5, 7), (0, 3, 6), (1, 4, 6), (0, 1, 3, 4, 6, 7))
OUT_SLOTS = 10


def block_kernel(group, n_exp, x_hbm, wq, wk, wv, wo, ids_ref, probs_ref, h_all, meta_all,
                 xb, wbuf, kb, vb, q_s, acc, top_s, mass_s, keep_s, s_b, e_b, o_s, h_s, meta_s,
                 x_sem, w_sem, k_send, kr_l, kr_r, kr_o, kr_p, h_send, hr_l, hr_r, hr_o, hr_p, m_send, m_recv, m_loc):
    tok = xb.shape[0]
    chips = group // 2
    q_tiles = wq.shape[1] // TILE
    k_tiles = wk.shape[1] // TILE
    kv_tiles = 2 * k_tiles
    o_tiles = wo.shape[1] // TILE
    me = lax.axis_index("sp")
    core = lax.rem(me, 2)
    chip = lax.div(me, 2)
    right = lax.rem(me + 2, group)
    left = lax.rem(me + group - 2, group)
    partner = me + 1 - 2 * core
    opp = lax.rem(me + 4, group)
    last = chips - 1

    def remote(src, dst, send, recv, dev):
        return pltpu.make_async_remote_copy(src_ref=src, dst_ref=dst, send_sem=send, recv_sem=recv,
                                            device_id={"sp": dev}, device_id_type=MESH)

    def got(ref, sem):
        pltpu.make_async_copy(ref, ref, sem).wait()

    def w_copy(arr, col, slot):
        if not isinstance(col, int):
            col = pl.multiple_of(col, TILE)
        return pltpu.make_async_copy(arr.at[:, pl.ds(col, TILE)], wbuf.at[slot], w_sem.at[slot])

    x_copy = pltpu.make_async_copy(x_hbm, xb, x_sem)
    x_copy.start()
    w_copy(wk, 0, 0).start()

    barrier = pltpu.get_barrier_semaphore()
    for d in range(1, group):
        pl.semaphore_signal(barrier, inc=1, device_id={"sp": lax.rem(me + d, group)}, device_id_type=MESH)
    x_copy.wait()
    w_copy(wk, TILE, 1).start()

    sends_right = chip < last
    sends_left_k = chip == 0
    sends_left_v = chip < 2
    gets_left = chip > 0
    gets_right_k = chip == last
    gets_right_v = (chip == last) | (chip == 0)
    fwd_k = (chip > 0) & (chip < last)
    fwd_v = (chip == last) | (chip == 0)
    gets_opp = chip >= 2

    def k_tile(p, carry):
        w_copy(wk, 0, p).wait()
        w_copy(wv, p * TILE, k_tiles + p).start()

        @pl.when(p == k_tiles - 1)
        def _():
            w_copy(wq, 0, kv_tiles).start()

        y = jnp.dot(xb[...], wbuf[p], preferred_element_type=jnp.float32).astype(jnp.bfloat16)
        for h in range(PER_TILE):
            kb[0, 0, p, h] = y[:, h * HEAD:(h + 1) * HEAD]

        @pl.when(p == 0)
        def _():
            pl.semaphore_wait(barrier, group - 1)

        src = kb.at[0, 0, p]

        @pl.when(sends_right)
        def _():
            remote(src, kb.at[3, 0, p], k_send.at[0], kr_l.at[p], right).start()

        @pl.when(sends_left_k)
        def _():
            remote(src, kb.at[1, 0, p], k_send.at[1], kr_r.at[p], left).start()

        @pl.when(core == 0)
        def _():
            remote(src, kb.at[0, 1, p], k_send.at[2], kr_p.at[0], partner).start()

        return carry

    lax.fori_loop(0, k_tiles, k_tile, 0)

    def v_tile(p, carry):
        w_copy(wv, 0, k_tiles + p).wait()
        w_copy(wq, (1 + p) * TILE, kv_tiles + 1 + p).start()
        y = jnp.dot(xb[...], wbuf[k_tiles + p], preferred_element_type=jnp.float32)
        for h in range(PER_TILE):
            vb[0, 0, p, h] = jnp.transpose(y[:, h * HEAD:(h + 1) * HEAD]).astype(jnp.bfloat16)
        src = vb.at[0, 0, p]

        @pl.when(sends_right)
        def _():
            remote(src, vb.at[3, 0, p], k_send.at[3], kr_l.at[k_tiles + p], right).start()

        @pl.when(sends_left_v)
        def _():
            remote(src, vb.at[1, 0, p], k_send.at[4], kr_r.at[k_tiles + p], left).start()

        @pl.when(core == 0)
        def _():
            remote(src, vb.at[0, 1, p], k_send.at[5], kr_p.at[4], partner).start()

        return carry

    lax.fori_loop(0, k_tiles, v_tile, 0)

    def q_tile(n, carry):
        slot = lax.rem(kv_tiles + n, SLOTS)
        w_copy(wq, 0, slot).wait()
        ahead = lax.rem(kv_tiles + AHEAD + n, SLOTS)

        @pl.when(n + AHEAD < q_tiles)
        def _():
            w_copy(wq, (n + AHEAD) * TILE, ahead).start()

        @pl.when(n + AHEAD >= q_tiles)
        def _():
            w_copy(wo, (n + AHEAD - q_tiles) * TILE, ahead).start()

        y = jnp.dot(xb[...], wbuf[slot], preferred_element_type=jnp.float32).astype(jnp.bfloat16)
        for h in range(PER_TILE):
            q_s[n, h] = y[:, h * HEAD:(h + 1) * HEAD]
        return carry

    lax.fori_loop(0, q_tiles, q_tile, 0)
    for n in range(AHEAD, o_tiles):
        w_copy(wo, n * TILE, (kv_tiles + q_tiles + n) % SLOTS).start()

    def k_partner(r, p):
        remote(kb.at[r, 0, p], kb.at[r, 1, p], k_send.at[5 + r], kr_p.at[r], partner).start()

    def v_partner(r, p):
        remote(vb.at[r, 0, p], vb.at[r, 1, p], k_send.at[8 + r], kr_p.at[4 + r], partner).start()

    @pl.when(gets_left)
    def _():
        for p in range(k_tiles):
            got(kb.at[3, 0, p], kr_l.at[p])

            @pl.when(fwd_k)
            def _():
                remote(kb.at[3, 0, p], kb.at[2, 0, p], k_send.at[12], kr_o.at[p], right).start()

            k_partner(3, p)

    expert = lax.broadcasted_iota(jnp.int32, (n_exp, tok), 0)
    hit0 = expert == ids_ref[0:1, :]
    hit1 = expert == ids_ref[1:2, :]
    probs = probs_ref[...]
    p0 = jnp.sum(jnp.where(hit0, probs, 0.0), axis=0, keepdims=True)
    p1 = jnp.sum(jnp.where(hit1, probs, 0.0), axis=0, keepdims=True)
    total = p0 + p1
    hits = hit0 | hit1
    before = (lax.broadcasted_iota(jnp.int32, (tok, tok), 0)
              < lax.broadcasted_iota(jnp.int32, (tok, tok), 1)).astype(jnp.float32).astype(jnp.bfloat16)
    earlier = jnp.dot(hits.astype(jnp.float32).astype(jnp.bfloat16), before, preferred_element_type=jnp.float32)
    meta_s[0:n_exp, :] = jnp.where(hits, earlier, -1.0)
    meta_s[n_exp:2 * n_exp, :] = jnp.where(hit0, p0 / total, jnp.where(hit1, p1 / total, 0.0))

    def attend(r, parts, lo=0, hi=None, first=False, diagonal=False):
        hi = q_tiles if hi is None else hi
        keys = parts * tok
        every = pl.ds(0, keys)
        if diagonal:
            key_i = lax.broadcasted_iota(jnp.int32, (tok, tok), 0)
            row_i = lax.broadcasted_iota(jnp.int32, (tok, tok), 1)
            seen = row_i >= key_i

        def score(g, h):
            kp = lax.div(g, PER_TILE)
            kh = lax.rem(g, PER_TILE)
            q = q_s[g, h]
            top = None if first else top_s[g, h]
            old = top
            for o in range(parts):
                s = lax.dot_general(kb[r, o, kp, kh], q, (((1,), (1,)), ((), ())), preferred_element_type=jnp.float32)
                if diagonal and o == 0:
                    s = jnp.where(seen, s, -1e30)
                s_b[h % 2, o] = s
                high = jnp.max(s, axis=0, keepdims=True)
                top = high if top is None else jnp.maximum(top, high)
            top_s[g, h] = top
            if not first:
                keep_s[h] = jnp.exp2((old - top) * EXP2_SCALE)

        def weigh(g, h):
            top = top_s[g, h]
            mass = None
            for o in range(parts):
                e = jnp.exp2((s_b[h % 2, o] - top) * EXP2_SCALE)
                e_b[h % 2, o * tok:(o + 1) * tok, :] = e.astype(jnp.bfloat16)
                part = jnp.sum(e, axis=0, keepdims=True)
                mass = part if mass is None else mass + part
            mass_s[g, h] = mass if first else mass + keep_s[h] * mass_s[g, h]

        def apply(g, h, into):
            kp = lax.div(g, PER_TILE)
            kh = lax.rem(g, PER_TILE)
            v = jnp.concatenate([vb[r, o, kp, kh] for o in range(parts)], axis=1)
            out = jnp.dot(v, e_b[h % 2, every, :], preferred_element_type=jnp.float32)
            acc[into, h] = out if first else out + keep_s[h] * acc[into, h]

        last_h = PER_TILE - 1

        def head_group(g, carry):
            below = jnp.maximum(g - 1, lo)
            into = lax.select(g == lo, q_tiles, g - 1)
            above = jnp.minimum(g + 1, hi - 1)
            for h in range(PER_TILE):
                if h < last_h:
                    score(g, h + 1)
                else:
                    score(above, 0)
                weigh(g, h)
                if h > 0:
                    apply(g, h - 1, g)
                else:
                    apply(below, last_h, into)
            return carry

        score(lo, 0)
        lax.fori_loop(lo, hi, head_group, 0)
        apply(hi - 1, last_h, hi - 1)

    acc[q_tiles, PER_TILE - 1] = jnp.zeros((HEAD, tok), jnp.float32)
    e_b[(PER_TILE - 1) % 2] = jnp.zeros((2 * tok, tok), jnp.bfloat16)
    keep_s[PER_TILE - 1] = jnp.zeros((1, tok), jnp.float32)

    @pl.when(core == 0)
    def _():
        attend(0, 1, first=True, diagonal=True)

    @pl.when(core == 1)
    def _():
        got(kb.at[0, 1], kr_p.at[0])
        got(vb.at[0, 1], kr_p.at[4])
        attend(0, 2, first=True, diagonal=True)

    m_rows = meta_all.at[me]
    loc = pltpu.make_async_copy(meta_s, m_rows, m_loc)
    loc.start()
    for d in range(1, group):
        remote(meta_s, m_rows, m_send.at[d - 1], m_recv.at[d - 1], lax.rem(me + d, group)).start()

    @pl.when(gets_right_v)
    def _():
        for p in range(k_tiles):
            got(vb.at[1, 0, p], kr_r.at[k_tiles + p])
            remote(vb.at[1, 0, p], vb.at[2, 0, p], k_send.at[13], kr_o.at[k_tiles + p], left).start()

    @pl.when(gets_right_k)
    def _():
        for p in range(k_tiles):
            got(kb.at[1, 0, p], kr_r.at[p])
            k_partner(1, p)
            v_partner(1, p)

    @pl.when(gets_left)
    def _():
        for p in range(k_tiles):
            got(vb.at[3, 0, p], kr_l.at[k_tiles + p])
            v_partner(3, p)
        got(kb.at[3, 1], kr_p.at[3])
        got(vb.at[3, 1], kr_p.at[7])
        attend(3, 2)

    def take_opp():
        for p in range(k_tiles):
            got(kb.at[2, 0, p], kr_o.at[p])
            k_partner(2, p)
            got(vb.at[2, 0, p], kr_o.at[k_tiles + p])
            v_partner(2, p)

    @pl.when(gets_right_k)
    def _():
        got(kb.at[1, 1], kr_p.at[1])
        got(vb.at[1, 1], kr_p.at[5])
        attend(1, 2, hi=q_tiles // 2)
        take_opp()
        attend(1, 2, lo=q_tiles // 2)

    @pl.when(gets_opp)
    def _():
        @pl.when(jnp.logical_not(gets_right_k))
        def _():
            take_opp()

        got(kb.at[2, 1], kr_p.at[2])
        got(vb.at[2, 1], kr_p.at[6])
        attend(2, 2)

    def finish(g, carry):
        for h in range(PER_TILE):
            o = jnp.transpose(acc[g, h] * (1.0 / mass_s[g, h]))
            o_s[:, pl.ds(pl.multiple_of(g * TILE + h * HEAD, HEAD), HEAD)] = o.astype(jnp.bfloat16)
        return carry

    lax.fori_loop(0, q_tiles, finish, 0)

    def rows_of(dev):
        return pl.ds(pl.multiple_of(dev * tok, tok), tok)

    def piece(dev, n):
        col = n * TILE
        if not isinstance(col, int):
            col = pl.multiple_of(col, TILE)
        return h_all.at[rows_of(dev), pl.ds(col, TILE)]

    def o_tile(n, carry):
        slot = lax.rem(kv_tiles + q_tiles + n, SLOTS)
        w_copy(wo, 0, slot).wait()
        y = jnp.dot(o_s[...], wbuf[slot], preferred_element_type=jnp.float32)
        x = xb[:, pl.ds(pl.multiple_of(n * TILE, TILE), TILE)].astype(jnp.float32)
        h_s[n] = (x + y).astype(jnp.bfloat16)
        remote(h_s.at[n], piece(me, n), h_send.at[0], hr_l.at[n], right).start()
        remote(h_s.at[n], piece(me, n), h_send.at[1], hr_r.at[n], left).start()
        remote(h_s.at[n], piece(me, n), h_send.at[2], hr_p.at[0], partner).start()
        pltpu.make_async_copy(h_s.at[n], piece(me, n), x_sem).start()
        return carry

    lax.fori_loop(0, o_tiles, o_tile, 0)

    def of_chips(which):
        hit = jnp.bool_(False)
        for c in which:
            hit = hit | (chip == c)
        return hit

    on_right = [[n in VIA_NEXT[(c - 1) % chips] for n in range(o_tiles)] for c in range(chips)]
    on_left = [[n not in VIA_NEXT[(c + 1) % chips] for n in range(o_tiles)] for c in range(chips)]

    def from_left():
        for n in range(o_tiles):
            got(piece(left, n), hr_l.at[n])

            @pl.when(of_chips([c for c in range(chips) if on_right[c][n]]))
            def _():
                remote(piece(left, n), piece(left, n), h_send.at[6], hr_o.at[n], right).start()

            remote(piece(left, n), piece(left, n), h_send.at[5], hr_p.at[3], partner).start()

    def from_right():
        for n in range(o_tiles):
            got(piece(right, n), hr_r.at[n])

            @pl.when(of_chips([c for c in range(chips) if on_left[c][n]]))
            def _():
                remote(piece(right, n), piece(right, n), h_send.at[7], hr_o.at[n], left).start()

            remote(piece(right, n), piece(right, n), h_send.at[3], hr_p.at[1], partner).start()

    early_right = (chip == 0) | (chip == last)

    @pl.when(early_right)
    def _():
        from_right()
        from_left()

    @pl.when(jnp.logical_not(early_right))
    def _():
        from_left()
        from_right()

    for n in range(o_tiles):
        got(piece(opp, n), hr_o.at[n])
        remote(piece(opp, n), piece(opp, n), h_send.at[4], hr_p.at[2], partner).start()

    mine = h_all.at[rows_of(me)]
    got(mine, x_sem)
    for i in range(6):
        got(mine, h_send.at[i])
    for c in range(chips):
        @pl.when(chip == c)
        def _():
            for i, on in ((6, on_right[c]), (7, on_left[c])):
                if sum(on):
                    got(h_all.at[rows_of(me), pl.ds(0, sum(on) * TILE)], h_send.at[i])
    for r in range(chips):
        got(h_all.at[rows_of(lax.rem(partner + 2 * r, group))], hr_p.at[r])
    k_own = kb.at[0, 0]
    v_own = vb.at[0, 0]
    for when, waits in ((sends_right, ((k_own, 0), (v_own, 3))), (sends_left_k, ((k_own, 1),)), (sends_left_v, ((v_own, 4),)),
                        (core == 0, ((k_own, 2), (v_own, 5))), (gets_left, ((k_own, 8), (v_own, 11))),
                        (gets_right_k, ((k_own, 6), (v_own, 9))), (gets_opp, ((k_own, 7), (v_own, 10))),
                        (fwd_k, ((k_own, 12),)), (fwd_v, ((v_own, 13),))):
        @pl.when(when)
        def _(waits=waits):
            for ref, i in waits:
                got(ref, k_send.at[i])

    loc.wait()
    for d in range(1, group):
        got(meta_s, m_send.at[d - 1])
        got(meta_all.at[lax.rem(me + group - d, group)], m_recv.at[d - 1])


def dispatch_kernel(n_exp, own_exp, meta_ref, h_hbm, hid_hbm, buf_hbm, hb, ob, h_sem, o_sem, hid_sem):
    group, tok, width = hb.shape
    slots = ob.shape[0]
    me = lax.axis_index("sp")
    steps = group * own_exp
    row = lax.broadcasted_iota(jnp.int32, (tok, tok), 0).astype(jnp.float32)

    def h_copy(s):
        return pltpu.make_async_copy(h_hbm.at[pl.ds(s * tok, tok)], hb.at[s], h_sem.at[s])

    def o_copy(i):
        s = lax.div(i, own_exp)
        return pltpu.make_async_copy(ob.at[lax.rem(i, slots)],
                                     buf_hbm.at[lax.rem(i, own_exp), pl.ds(pl.multiple_of(s * tok, tok), tok)],
                                     o_sem.at[lax.rem(i, slots)])

    for s in range(group):
        h_copy(s).start()

    def step(i, carry):
        s = lax.div(i, own_exp)
        e = lax.rem(i, own_exp)

        @pl.when(e == 0)
        def _():
            pltpu.make_async_copy(hb.at[s], hb.at[s], h_sem.at[s]).wait()

            @pl.when(s == me)
            def _():
                pltpu.make_async_copy(hb.at[s], hid_hbm, hid_sem).start()

        @pl.when(i >= slots)
        def _():
            o_copy(i - slots).wait()

        expert = me * own_exp + e
        slot = meta_ref[s, pl.ds(expert, 1), :]
        gate = meta_ref[s, pl.ds(n_exp + expert, 1), :]
        pick = row == slot
        gate_col = jnp.sum(jnp.where(pick, gate, 0.0), axis=1, keepdims=True)
        pick = pick.astype(jnp.float32).astype(jnp.bfloat16)
        o = lax.rem(i, slots)
        for c in range(0, width, TILE):
            rows = jnp.dot(pick, hb[s, :, c:c + TILE], preferred_element_type=jnp.float32)
            ob[o, :, c:c + TILE] = (rows * gate_col).astype(jnp.bfloat16)
        o_copy(i).start()
        return carry

    lax.fori_loop(0, steps, step, 0)
    for i in range(steps - slots, steps):
        o_copy(i).wait()
    pltpu.make_async_copy(hb.at[0], hid_hbm, hid_sem).wait()


def solution(mesh):
    group = mesh.shape['sp']
    row_spec = P(('dp', 'sp'), None)
    buf_spec = P(('dp', 'sp'), None, None)

    def device_step(x_loc, w_q, w_k, w_v, w_o, ids_loc, probs_loc):
        tok, width = x_loc.shape
        n_exp = probs_loc.shape[1]
        own_exp = n_exp // group
        seq = tok * group
        q_tiles = w_q.shape[1] // TILE
        k_tiles = w_k.shape[1] // TILE
        chips = group // 2
        o_tiles = width // TILE
        bf16 = jnp.bfloat16
        any_spec = pl.BlockSpec(memory_space=pl.ANY)
        vmem_spec = pl.BlockSpec(memory_space=pltpu.VMEM)
        dma = pltpu.SemaphoreType.DMA
        h_all, meta_all = pl.pallas_call(
            functools.partial(block_kernel, group, n_exp),
            out_shape=(jax.ShapeDtypeStruct((seq, width), bf16),
                       jax.ShapeDtypeStruct((group, 2 * n_exp, tok), jnp.float32)),
            in_specs=[any_spec] * 5 + [vmem_spec] * 2,
            out_specs=(any_spec, any_spec),
            scratch_shapes=[
                pltpu.VMEM((tok, width), bf16),
                pltpu.VMEM((SLOTS, width, TILE), bf16),
                pltpu.VMEM((chips, 2, k_tiles, PER_TILE, tok, HEAD), bf16),
                pltpu.VMEM((chips, 2, k_tiles, PER_TILE, HEAD, tok), bf16),
                pltpu.VMEM((q_tiles, PER_TILE, tok, HEAD), bf16),
                pltpu.VMEM((q_tiles + 1, PER_TILE, HEAD, tok), jnp.float32),
                pltpu.VMEM((q_tiles, PER_TILE, 1, tok), jnp.float32),
                pltpu.VMEM((q_tiles, PER_TILE, 1, tok), jnp.float32),
                pltpu.VMEM((PER_TILE, 1, tok), jnp.float32),
                pltpu.VMEM((2, 2, tok, tok), jnp.float32),
                pltpu.VMEM((2, 2 * tok, tok), bf16),
                pltpu.VMEM((tok, q_tiles * TILE), bf16),
                pltpu.VMEM((o_tiles, tok, TILE), bf16),
                pltpu.VMEM((2 * n_exp, tok), jnp.float32),
                dma, dma((SLOTS,)),
                dma((14,)), dma((2 * k_tiles,)), dma((2 * k_tiles,)), dma((2 * k_tiles,)), dma((2 * chips,)),
                dma((8,)), dma((o_tiles,)), dma((o_tiles,)), dma((o_tiles,)), dma((chips,)),
                dma((group - 1,)), dma((group - 1,)), dma,
            ],
            compiler_params=pltpu.CompilerParams(collective_id=0, has_side_effects=True,
                                                 vmem_limit_bytes=VMEM_LIMIT),
            name="block",
        )(x_loc, w_q, w_k, w_v, w_o, ids_loc.T, probs_loc.T)

        hidden_out, buf = pl.pallas_call(
            functools.partial(dispatch_kernel, n_exp, own_exp),
            out_shape=(jax.ShapeDtypeStruct((tok, width), bf16),
                       jax.ShapeDtypeStruct((own_exp, seq, width), bf16)),
            in_specs=[vmem_spec, any_spec],
            out_specs=(any_spec, any_spec),
            scratch_shapes=[pltpu.VMEM((group, tok, width), bf16), pltpu.VMEM((OUT_SLOTS, tok, width), bf16),
                            dma((group,)), dma((OUT_SLOTS,)), dma],
            compiler_params=pltpu.CompilerParams(vmem_limit_bytes=VMEM_LIMIT),
            name="dispatch",
        )(meta_all, h_all)
        return hidden_out, buf

    return jax.shard_map(device_step, mesh=mesh,
                         in_specs=(row_spec, P(), P(), P(), P(), row_spec, row_spec),
                         out_specs=(row_spec, buf_spec), check_vma=False)
```

```python
import functools
import math

import jax
import jax.numpy as jnp
from jax import lax
from jax.experimental import pallas as pl
from jax.experimental.pallas import tpu as pltpu
from jax.sharding import PartitionSpec as P

HEAD = 128
EXP2_SCALE = math.log2(math.e) / math.sqrt(HEAD)
MESH = pl.DeviceIdType.MESH
TILE = 512
SLOTS = 8
PER_TILE = TILE // HEAD
AHEAD = 3
VMEM_LIMIT = 67_000_000
VIA_NEXT = ((0, 2, 3, 5, 7), (0, 3, 6), (1, 4, 6), (0, 1, 3, 4, 6, 7))
OUT_SLOTS = 10


def block_kernel(group, n_exp, x_hbm, wq, wk, wv, wo, ids_ref, probs_ref, h_all, meta_all,
                 xb, wbuf, kb, vb, q_s, acc, top_s, mass_s, keep_s, s_b, e_b, o_s, h_s, meta_s,
                 x_sem, w_sem, k_send, kr_l, kr_r, kr_o, kr_p, h_send, hr_l, hr_r, hr_o, hr_p, m_send, m_recv, m_loc):
    tok = xb.shape[0]
    chips = group // 2
    q_tiles = wq.shape[1] // TILE
    k_tiles = wk.shape[1] // TILE
    kv_tiles = 2 * k_tiles
    o_tiles = wo.shape[1] // TILE
    me = lax.axis_index("sp")
    core = lax.rem(me, 2)
    chip = lax.div(me, 2)
    right = lax.rem(me + 2, group)
    left = lax.rem(me + group - 2, group)
    partner = me + 1 - 2 * core
    opp = lax.rem(me + 4, group)
    last = chips - 1

    def remote(src, dst, send, recv, dev):
        return pltpu.make_async_remote_copy(src_ref=src, dst_ref=dst, send_sem=send, recv_sem=recv,
                                            device_id={"sp": dev}, device_id_type=MESH)

    def got(ref, sem):
        pltpu.make_async_copy(ref, ref, sem).wait()

    def w_copy(arr, col, slot):
        if not isinstance(col, int):
            col = pl.multiple_of(col, TILE)
        return pltpu.make_async_copy(arr.at[:, pl.ds(col, TILE)], wbuf.at[slot], w_sem.at[slot])

    x_copy = pltpu.make_async_copy(x_hbm, xb, x_sem)
    x_copy.start()
    w_copy(wk, 0, 0).start()

    barrier = pltpu.get_barrier_semaphore()
    for d in range(1, group):
        pl.semaphore_signal(barrier, inc=1, device_id={"sp": lax.rem(me + d, group)}, device_id_type=MESH)
    x_copy.wait()
    w_copy(wk, TILE, 1).start()

    sends_right = chip < last
    sends_left_k = chip == 0
    sends_left_v = chip < 2
    gets_left = chip > 0
    gets_right_k = chip == last
    gets_right_v = (chip == last) | (chip == 0)
    fwd_k = (chip > 0) & (chip < last)
    fwd_v = (chip == last) | (chip == 0)
    gets_opp = chip >= 2

    def k_tile(p, carry):
        w_copy(wk, 0, p).wait()
        w_copy(wv, p * TILE, k_tiles + p).start()

        @pl.when(p == k_tiles - 1)
        def _():
            w_copy(wq, 0, kv_tiles).start()

        y = jnp.dot(xb[...], wbuf[p], preferred_element_type=jnp.float32).astype(jnp.bfloat16)
        for h in range(PER_TILE):
            kb[0, 0, p, h] = y[:, h * HEAD:(h + 1) * HEAD]

        @pl.when(p == 0)
        def _():
            pl.semaphore_wait(barrier, group - 1)

        src = kb.at[0, 0, p]

        @pl.when(sends_right)
        def _():
            remote(src, kb.at[3, 0, p], k_send.at[0], kr_l.at[p], right).start()

        @pl.when(sends_left_k)
        def _():
            remote(src, kb.at[1, 0, p], k_send.at[1], kr_r.at[p], left).start()

        @pl.when(core == 0)
        def _():
            remote(src, kb.at[0, 1, p], k_send.at[2], kr_p.at[0], partner).start()

        return carry

    with jax.named_scope("kproj"):
        lax.fori_loop(0, k_tiles, k_tile, 0)

    def v_tile(p, carry):
        w_copy(wv, 0, k_tiles + p).wait()
        w_copy(wq, (1 + p) * TILE, kv_tiles + 1 + p).start()
        y = jnp.dot(xb[...], wbuf[k_tiles + p], preferred_element_type=jnp.float32)
        for h in range(PER_TILE):
            vb[0, 0, p, h] = jnp.transpose(y[:, h * HEAD:(h + 1) * HEAD]).astype(jnp.bfloat16)
        src = vb.at[0, 0, p]

        @pl.when(sends_right)
        def _():
            remote(src, vb.at[3, 0, p], k_send.at[3], kr_l.at[k_tiles + p], right).start()

        @pl.when(sends_left_v)
        def _():
            remote(src, vb.at[1, 0, p], k_send.at[4], kr_r.at[k_tiles + p], left).start()

        @pl.when(core == 0)
        def _():
            remote(src, vb.at[0, 1, p], k_send.at[5], kr_p.at[4], partner).start()

        return carry

    with jax.named_scope("vproj"):
        lax.fori_loop(0, k_tiles, v_tile, 0)

    def q_tile(n, carry):
        slot = lax.rem(kv_tiles + n, SLOTS)
        w_copy(wq, 0, slot).wait()
        ahead = lax.rem(kv_tiles + AHEAD + n, SLOTS)

        @pl.when(n + AHEAD < q_tiles)
        def _():
            w_copy(wq, (n + AHEAD) * TILE, ahead).start()

        @pl.when(n + AHEAD >= q_tiles)
        def _():
            w_copy(wo, (n + AHEAD - q_tiles) * TILE, ahead).start()

        y = jnp.dot(xb[...], wbuf[slot], preferred_element_type=jnp.float32).astype(jnp.bfloat16)
        for h in range(PER_TILE):
            q_s[n, h] = y[:, h * HEAD:(h + 1) * HEAD]
        return carry

    with jax.named_scope("qproj"):
        lax.fori_loop(0, q_tiles, q_tile, 0)
    for n in range(AHEAD, o_tiles):
        w_copy(wo, n * TILE, (kv_tiles + q_tiles + n) % SLOTS).start()

    def k_partner(r, p):
        remote(kb.at[r, 0, p], kb.at[r, 1, p], k_send.at[5 + r], kr_p.at[r], partner).start()

    def v_partner(r, p):
        remote(vb.at[r, 0, p], vb.at[r, 1, p], k_send.at[8 + r], kr_p.at[4 + r], partner).start()

    @pl.when(gets_left)
    def _():
        for p in range(k_tiles):
            got(kb.at[3, 0, p], kr_l.at[p])

            @pl.when(fwd_k)
            def _():
                remote(kb.at[3, 0, p], kb.at[2, 0, p], k_send.at[12], kr_o.at[p], right).start()

            k_partner(3, p)

    expert = lax.broadcasted_iota(jnp.int32, (n_exp, tok), 0)
    hit0 = expert == ids_ref[0:1, :]
    hit1 = expert == ids_ref[1:2, :]
    probs = probs_ref[...]
    p0 = jnp.sum(jnp.where(hit0, probs, 0.0), axis=0, keepdims=True)
    p1 = jnp.sum(jnp.where(hit1, probs, 0.0), axis=0, keepdims=True)
    total = p0 + p1
    hits = hit0 | hit1
    before = (lax.broadcasted_iota(jnp.int32, (tok, tok), 0)
              < lax.broadcasted_iota(jnp.int32, (tok, tok), 1)).astype(jnp.float32).astype(jnp.bfloat16)
    earlier = jnp.dot(hits.astype(jnp.float32).astype(jnp.bfloat16), before, preferred_element_type=jnp.float32)
    meta_s[0:n_exp, :] = jnp.where(hits, earlier, -1.0)
    meta_s[n_exp:2 * n_exp, :] = jnp.where(hit0, p0 / total, jnp.where(hit1, p1 / total, 0.0))

    def attend(r, parts, lo=0, hi=None, first=False, diagonal=False):
        hi = q_tiles if hi is None else hi
        spare = q_tiles
        keys = parts * tok
        if diagonal:
            key_i = lax.broadcasted_iota(jnp.int32, (tok, tok), 0)
            row_i = lax.broadcasted_iota(jnp.int32, (tok, tok), 1)
            seen = row_i >= key_i

        def score(g, into, h, side):
            kp = lax.div(g, PER_TILE)
            kh = lax.rem(g, PER_TILE)
            q = q_s[g, h]
            top = None if first else top_s[g, h]
            old = top
            for o in range(parts):
                s = lax.dot_general(kb[r, o, kp, kh], q, (((1,), (1,)), ((), ())), preferred_element_type=jnp.float32)
                if diagonal and o == 0:
                    s = jnp.where(seen, s, -1e30)
                s_b[side, h, o] = s
                high = jnp.max(s, axis=0, keepdims=True)
                top = high if top is None else jnp.maximum(top, high)
            top_s[into, h] = top
            if not first:
                keep_s[into, h] = jnp.exp2((old - top) * EXP2_SCALE)

        def weigh(g, h, side):
            top = top_s[g, h]
            mass = None
            for o in range(parts):
                e = jnp.exp2((s_b[side, h, o] - top) * EXP2_SCALE)
                e_b[side, h, o * tok:(o + 1) * tok, :] = e.astype(jnp.bfloat16)
                part = jnp.sum(e, axis=0, keepdims=True)
                mass = part if mass is None else mass + part
            mass_s[g, h] = mass if first else mass + keep_s[g, h] * mass_s[g, h]

        def apply(g, into, h, side):
            kp = lax.div(g, PER_TILE)
            kh = lax.rem(g, PER_TILE)
            v = jnp.concatenate([vb[r, o, kp, kh] for o in range(parts)], axis=1)
            out = jnp.dot(v, e_b[side, h, 0:keys, :], preferred_element_type=jnp.float32)
            acc[into, h] = out if first else out + keep_s[into, h] * acc[into, h]

        def head_groups(i, carry):
            g = lo + 2 * i
            below = jnp.maximum(g - 1, lo)
            below_into = lax.select(g == lo, spare, g - 1)
            above = jnp.minimum(g + 2, hi - 1)
            above_into = lax.select(g == hi - 2, spare, g + 2)
            for h in range(PER_TILE):
                weigh(g, h, 0)
                score(g + 1, g + 1, h, 1)
                apply(below, below_into, h, 1)
            for h in range(PER_TILE):
                weigh(g + 1, h, 1)
                score(above, above_into, h, 0)
                apply(g, g, h, 0)
            return carry

        for h in range(PER_TILE):
            score(lo, lo, h, 0)
        lax.fori_loop(0, (hi - lo) // 2, head_groups, 0)
        for h in range(PER_TILE):
            apply(hi - 1, hi - 1, h, 1)

    for h in range(PER_TILE):
        e_b[1, h] = jnp.zeros((2 * tok, tok), jnp.bfloat16)
        acc[q_tiles, h] = jnp.zeros((HEAD, tok), jnp.float32)
        keep_s[q_tiles, h] = jnp.zeros((1, tok), jnp.float32)

    @pl.when(core == 0)
    def _():
        with jax.named_scope("att_own1"):
            attend(0, 1, first=True, diagonal=True)

    @pl.when(core == 1)
    def _():
        got(kb.at[0, 1], kr_p.at[0])
        got(vb.at[0, 1], kr_p.at[4])
        with jax.named_scope("att_own2"):
            attend(0, 2, first=True, diagonal=True)

    m_rows = meta_all.at[me]
    loc = pltpu.make_async_copy(meta_s, m_rows, m_loc)
    loc.start()
    for d in range(1, group):
        remote(meta_s, m_rows, m_send.at[d - 1], m_recv.at[d - 1], lax.rem(me + d, group)).start()

    @pl.when(gets_right_v)
    def _():
        for p in range(k_tiles):
            got(vb.at[1, 0, p], kr_r.at[k_tiles + p])
            remote(vb.at[1, 0, p], vb.at[2, 0, p], k_send.at[13], kr_o.at[k_tiles + p], left).start()

    @pl.when(gets_right_k)
    def _():
        for p in range(k_tiles):
            got(kb.at[1, 0, p], kr_r.at[p])
            k_partner(1, p)
            v_partner(1, p)

    @pl.when(gets_left)
    def _():
        for p in range(k_tiles):
            got(vb.at[3, 0, p], kr_l.at[k_tiles + p])
            v_partner(3, p)
        got(kb.at[3, 1], kr_p.at[3])
        got(vb.at[3, 1], kr_p.at[7])
        with jax.named_scope("att_left"):
            attend(3, 2)

    def take_opp():
        for p in range(k_tiles):
            got(kb.at[2, 0, p], kr_o.at[p])
            k_partner(2, p)
            got(vb.at[2, 0, p], kr_o.at[k_tiles + p])
            v_partner(2, p)

    @pl.when(gets_right_k)
    def _():
        got(kb.at[1, 1], kr_p.at[1])
        got(vb.at[1, 1], kr_p.at[5])
        with jax.named_scope("att_right_a"):
            attend(1, 2, hi=q_tiles // 2)
        take_opp()
        with jax.named_scope("att_right_b"):
            attend(1, 2, lo=q_tiles // 2)

    @pl.when(gets_opp)
    def _():
        @pl.when(jnp.logical_not(gets_right_k))
        def _():
            take_opp()

        got(kb.at[2, 1], kr_p.at[2])
        got(vb.at[2, 1], kr_p.at[6])
        with jax.named_scope("att_opp"):
            attend(2, 2)

    def finish(g, carry):
        for h in range(PER_TILE):
            o = jnp.transpose(acc[g, h] * (1.0 / mass_s[g, h]))
            o_s[:, pl.ds(pl.multiple_of(g * TILE + h * HEAD, HEAD), HEAD)] = o.astype(jnp.bfloat16)
        return carry

    with jax.named_scope("finish"):
        lax.fori_loop(0, q_tiles, finish, 0)

    def rows_of(dev):
        return pl.ds(pl.multiple_of(dev * tok, tok), tok)

    def piece(dev, n):
        col = n * TILE
        if not isinstance(col, int):
            col = pl.multiple_of(col, TILE)
        return h_all.at[rows_of(dev), pl.ds(col, TILE)]

    def o_tile(n, carry):
        slot = lax.rem(kv_tiles + q_tiles + n, SLOTS)
        w_copy(wo, 0, slot).wait()
        y = jnp.dot(o_s[...], wbuf[slot], preferred_element_type=jnp.float32)
        x = xb[:, pl.ds(pl.multiple_of(n * TILE, TILE), TILE)].astype(jnp.float32)
        h_s[n] = (x + y).astype(jnp.bfloat16)
        remote(h_s.at[n], piece(me, n), h_send.at[0], hr_l.at[n], right).start()
        remote(h_s.at[n], piece(me, n), h_send.at[1], hr_r.at[n], left).start()
        remote(h_s.at[n], piece(me, n), h_send.at[2], hr_p.at[0], partner).start()
        pltpu.make_async_copy(h_s.at[n], piece(me, n), x_sem).start()
        return carry

    with jax.named_scope("oproj"):
        lax.fori_loop(0, o_tiles, o_tile, 0)

    def of_chips(which):
        hit = jnp.bool_(False)
        for c in which:
            hit = hit | (chip == c)
        return hit

    on_right = [[n in VIA_NEXT[(c - 1) % chips] for n in range(o_tiles)] for c in range(chips)]
    on_left = [[n not in VIA_NEXT[(c + 1) % chips] for n in range(o_tiles)] for c in range(chips)]

    def from_left():
        for n in range(o_tiles):
            with jax.named_scope("w_left%d" % n):
                got(piece(left, n), hr_l.at[n])

            @pl.when(of_chips([c for c in range(chips) if on_right[c][n]]))
            def _():
                remote(piece(left, n), piece(left, n), h_send.at[6], hr_o.at[n], right).start()

            remote(piece(left, n), piece(left, n), h_send.at[5], hr_p.at[3], partner).start()

    def from_right():
        for n in range(o_tiles):
            with jax.named_scope("w_right%d" % n):
                got(piece(right, n), hr_r.at[n])

            @pl.when(of_chips([c for c in range(chips) if on_left[c][n]]))
            def _():
                remote(piece(right, n), piece(right, n), h_send.at[7], hr_o.at[n], left).start()

            remote(piece(right, n), piece(right, n), h_send.at[3], hr_p.at[1], partner).start()

    early_right = (chip == 0) | (chip == last)

    @pl.when(early_right)
    def _():
        from_right()
        from_left()

    @pl.when(jnp.logical_not(early_right))
    def _():
        from_left()
        from_right()

    for n in range(o_tiles):
        with jax.named_scope("w_opp%d" % n):
            got(piece(opp, n), hr_o.at[n])
        remote(piece(opp, n), piece(opp, n), h_send.at[4], hr_p.at[2], partner).start()

    mine = h_all.at[rows_of(me)]
    got(mine, x_sem)
    for i in range(6):
        got(mine, h_send.at[i])
    for c in range(chips):
        @pl.when(chip == c)
        def _():
            for i, on in ((6, on_right[c]), (7, on_left[c])):
                if sum(on):
                    got(h_all.at[rows_of(me), pl.ds(0, sum(on) * TILE)], h_send.at[i])
    for r in range(chips):
        got(h_all.at[rows_of(lax.rem(partner + 2 * r, group))], hr_p.at[r])
    k_own = kb.at[0, 0]
    v_own = vb.at[0, 0]
    for when, waits in ((sends_right, ((k_own, 0), (v_own, 3))), (sends_left_k, ((k_own, 1),)), (sends_left_v, ((v_own, 4),)),
                        (core == 0, ((k_own, 2), (v_own, 5))), (gets_left, ((k_own, 8), (v_own, 11))),
                        (gets_right_k, ((k_own, 6), (v_own, 9))), (gets_opp, ((k_own, 7), (v_own, 10))),
                        (fwd_k, ((k_own, 12),)), (fwd_v, ((v_own, 13),))):
        @pl.when(when)
        def _(waits=waits):
            for ref, i in waits:
                got(ref, k_send.at[i])

    loc.wait()
    for d in range(1, group):
        got(meta_s, m_send.at[d - 1])
        got(meta_all.at[lax.rem(me + group - d, group)], m_recv.at[d - 1])


def dispatch_kernel(n_exp, own_exp, meta_ref, h_hbm, hid_hbm, buf_hbm, hb, ob, h_sem, o_sem, hid_sem):
    group, tok, width = hb.shape
    slots = ob.shape[0]
    me = lax.axis_index("sp")
    steps = group * own_exp
    row = lax.broadcasted_iota(jnp.int32, (tok, tok), 0).astype(jnp.float32)

    def h_copy(s):
        return pltpu.make_async_copy(h_hbm.at[pl.ds(s * tok, tok)], hb.at[s], h_sem.at[s])

    def o_copy(i):
        s = lax.div(i, own_exp)
        return pltpu.make_async_copy(ob.at[lax.rem(i, slots)],
                                     buf_hbm.at[lax.rem(i, own_exp), pl.ds(pl.multiple_of(s * tok, tok), tok)],
                                     o_sem.at[lax.rem(i, slots)])

    for s in range(group):
        h_copy(s).start()

    def step(i, carry):
        s = lax.div(i, own_exp)
        e = lax.rem(i, own_exp)

        @pl.when(e == 0)
        def _():
            pltpu.make_async_copy(hb.at[s], hb.at[s], h_sem.at[s]).wait()

            @pl.when(s == me)
            def _():
                pltpu.make_async_copy(hb.at[s], hid_hbm, hid_sem).start()

        @pl.when(i >= slots)
        def _():
            o_copy(i - slots).wait()

        expert = me * own_exp + e
        slot = meta_ref[s, pl.ds(expert, 1), :]
        gate = meta_ref[s, pl.ds(n_exp + expert, 1), :]
        pick = row == slot
        gate_col = jnp.sum(jnp.where(pick, gate, 0.0), axis=1, keepdims=True)
        pick = pick.astype(jnp.float32).astype(jnp.bfloat16)
        o = lax.rem(i, slots)
        for c in range(0, width, TILE):
            rows = jnp.dot(pick, hb[s, :, c:c + TILE], preferred_element_type=jnp.float32)
            ob[o, :, c:c + TILE] = (rows * gate_col).astype(jnp.bfloat16)
        o_copy(i).start()
        return carry

    lax.fori_loop(0, steps, step, 0)
    for i in range(steps - slots, steps):
        o_copy(i).wait()
    pltpu.make_async_copy(hb.at[0], hid_hbm, hid_sem).wait()


def solution(mesh):
    group = mesh.shape['sp']
    row_spec = P(('dp', 'sp'), None)
    buf_spec = P(('dp', 'sp'), None, None)

    def device_step(x_loc, w_q, w_k, w_v, w_o, ids_loc, probs_loc):
        tok, width = x_loc.shape
        n_exp = probs_loc.shape[1]
        own_exp = n_exp // group
        seq = tok * group
        q_tiles = w_q.shape[1] // TILE
        k_tiles = w_k.shape[1] // TILE
        chips = group // 2
        o_tiles = width // TILE
        bf16 = jnp.bfloat16
        any_spec = pl.BlockSpec(memory_space=pl.ANY)
        vmem_spec = pl.BlockSpec(memory_space=pltpu.VMEM)
        dma = pltpu.SemaphoreType.DMA
        h_all, meta_all = pl.pallas_call(
            functools.partial(block_kernel, group, n_exp),
            out_shape=(jax.ShapeDtypeStruct((seq, width), bf16),
                       jax.ShapeDtypeStruct((group, 2 * n_exp, tok), jnp.float32)),
            in_specs=[any_spec] * 5 + [vmem_spec] * 2,
            out_specs=(any_spec, any_spec),
            scratch_shapes=[
                pltpu.VMEM((tok, width), bf16),
                pltpu.VMEM((SLOTS, width, TILE), bf16),
                pltpu.VMEM((chips, 2, k_tiles, PER_TILE, tok, HEAD), bf16),
                pltpu.VMEM((chips, 2, k_tiles, PER_TILE, HEAD, tok), bf16),
                pltpu.VMEM((q_tiles, PER_TILE, tok, HEAD), bf16),
                pltpu.VMEM((q_tiles + 1, PER_TILE, HEAD, tok), jnp.float32),
                pltpu.VMEM((q_tiles + 1, PER_TILE, 1, tok), jnp.float32),
                pltpu.VMEM((q_tiles + 1, PER_TILE, 1, tok), jnp.float32),
                pltpu.VMEM((q_tiles + 1, PER_TILE, 1, tok), jnp.float32),
                pltpu.VMEM((2, PER_TILE, 2, tok, tok), jnp.float32),
                pltpu.VMEM((2, PER_TILE, 2 * tok, tok), bf16),
                pltpu.VMEM((tok, q_tiles * TILE), bf16),
                pltpu.VMEM((o_tiles, tok, TILE), bf16),
                pltpu.VMEM((2 * n_exp, tok), jnp.float32),
                dma, dma((SLOTS,)),
                dma((14,)), dma((2 * k_tiles,)), dma((2 * k_tiles,)), dma((2 * k_tiles,)), dma((2 * chips,)),
                dma((8,)), dma((o_tiles,)), dma((o_tiles,)), dma((o_tiles,)), dma((chips,)),
                dma((group - 1,)), dma((group - 1,)), dma,
            ],
            compiler_params=pltpu.CompilerParams(collective_id=0, has_side_effects=True,
                                                 vmem_limit_bytes=VMEM_LIMIT),
            name="block",
        )(x_loc, w_q, w_k, w_v, w_o, ids_loc.T, probs_loc.T)

        hidden_out, buf = pl.pallas_call(
            functools.partial(dispatch_kernel, n_exp, own_exp),
            out_shape=(jax.ShapeDtypeStruct((tok, width), bf16),
                       jax.ShapeDtypeStruct((own_exp, seq, width), bf16)),
            in_specs=[vmem_spec, any_spec],
            out_specs=(any_spec, any_spec),
            scratch_shapes=[pltpu.VMEM((group, tok, width), bf16), pltpu.VMEM((OUT_SLOTS, tok, width), bf16),
                            dma((group,)), dma((OUT_SLOTS,)), dma],
            compiler_params=pltpu.CompilerParams(vmem_limit_bytes=VMEM_LIMIT),
            name="dispatch",
        )(meta_all, h_all)
        return hidden_out, buf

    return jax.shard_map(device_step, mesh=mesh,
                         in_specs=(row_spec, P(), P(), P(), P(), row_spec, row_spec),
                         out_specs=(row_spec, buf_spec), check_vma=False)
```

```python
import functools
import math

import jax
import jax.numpy as jnp
from jax import lax
from jax.experimental import pallas as pl
from jax.experimental.pallas import tpu as pltpu
from jax.sharding import PartitionSpec as P

HEAD = 128
EXP2_SCALE = math.log2(math.e) / math.sqrt(HEAD)
MESH = pl.DeviceIdType.MESH
TILE = 512
SLOTS = 8
PER_TILE = TILE // HEAD
AHEAD = 3
VMEM_LIMIT = 67_000_000
VIA_NEXT = ((0, 2, 3, 5, 7), (0, 3, 6), (1, 4, 6), (0, 1, 3, 4, 6, 7))
LAG = 3
H_AHEAD = 2
OUT_SLOTS = 10


def block_kernel(group, n_exp, x_hbm, wq, wk, wv, wo, ids_ref, probs_ref, h_all, meta_all,
                 xb, wbuf, kb, vb, q_s, acc, top_s, mass_s, keep_s, s_b, e_b, o_s, h_s, meta_s,
                 x_sem, w_sem, k_send, kr_l, kr_r, kr_o, kr_p, h_send, hr_l, hr_r, hr_o, hr_p, m_send, m_recv, m_loc):
    tok = xb.shape[0]
    chips = group // 2
    q_tiles = wq.shape[1] // TILE
    k_tiles = wk.shape[1] // TILE
    kv_tiles = 2 * k_tiles
    o_tiles = wo.shape[1] // TILE
    me = lax.axis_index("sp")
    core = lax.rem(me, 2)
    chip = lax.div(me, 2)
    right = lax.rem(me + 2, group)
    left = lax.rem(me + group - 2, group)
    partner = me + 1 - 2 * core
    opp = lax.rem(me + 4, group)
    last = chips - 1

    def remote(src, dst, send, recv, dev):
        return pltpu.make_async_remote_copy(src_ref=src, dst_ref=dst, send_sem=send, recv_sem=recv,
                                            device_id={"sp": dev}, device_id_type=MESH)

    def got(ref, sem):
        pltpu.make_async_copy(ref, ref, sem).wait()

    def w_copy(arr, col, slot):
        if not isinstance(col, int):
            col = pl.multiple_of(col, TILE)
        return pltpu.make_async_copy(arr.at[:, pl.ds(col, TILE)], wbuf.at[slot], w_sem.at[slot])

    x_copy = pltpu.make_async_copy(x_hbm, xb, x_sem)
    x_copy.start()
    w_copy(wk, 0, 0).start()

    barrier = pltpu.get_barrier_semaphore()
    for d in range(1, group):
        pl.semaphore_signal(barrier, inc=1, device_id={"sp": lax.rem(me + d, group)}, device_id_type=MESH)
    x_copy.wait()
    w_copy(wk, TILE, 1).start()

    sends_right = chip < last
    sends_left_k = chip == 0
    sends_left_v = chip < 2
    gets_left = chip > 0
    gets_right_k = chip == last
    gets_right_v = (chip == last) | (chip == 0)
    fwd_k = (chip > 0) & (chip < last)
    fwd_v = (chip == last) | (chip == 0)
    gets_opp = chip >= 2

    def k_tile(p, carry):
        w_copy(wk, 0, p).wait()
        w_copy(wv, p * TILE, k_tiles + p).start()

        @pl.when(p == k_tiles - 1)
        def _():
            w_copy(wq, 0, kv_tiles).start()

        y = jnp.dot(xb[...], wbuf[p], preferred_element_type=jnp.float32).astype(jnp.bfloat16)
        for h in range(PER_TILE):
            kb[0, 0, p, h] = y[:, h * HEAD:(h + 1) * HEAD]

        @pl.when(p == 0)
        def _():
            pl.semaphore_wait(barrier, group - 1)

        src = kb.at[0, 0, p]

        @pl.when(sends_right)
        def _():
            remote(src, kb.at[3, 0, p], k_send.at[0], kr_l.at[p], right).start()

        @pl.when(sends_left_k)
        def _():
            remote(src, kb.at[1, 0, p], k_send.at[1], kr_r.at[p], left).start()

        @pl.when(core == 0)
        def _():
            remote(src, kb.at[0, 1, p], k_send.at[2], kr_p.at[0], partner).start()

        return carry

    with jax.named_scope("kproj"):
        lax.fori_loop(0, k_tiles, k_tile, 0)

    def v_tile(p, carry):
        w_copy(wv, 0, k_tiles + p).wait()
        w_copy(wq, (1 + p) * TILE, kv_tiles + 1 + p).start()
        y = jnp.dot(xb[...], wbuf[k_tiles + p], preferred_element_type=jnp.float32)
        for h in range(PER_TILE):
            vb[0, 0, p, h] = jnp.transpose(y[:, h * HEAD:(h + 1) * HEAD]).astype(jnp.bfloat16)
        src = vb.at[0, 0, p]

        @pl.when(sends_right)
        def _():
            remote(src, vb.at[3, 0, p], k_send.at[3], kr_l.at[k_tiles + p], right).start()

        @pl.when(sends_left_v)
        def _():
            remote(src, vb.at[1, 0, p], k_send.at[4], kr_r.at[k_tiles + p], left).start()

        @pl.when(core == 0)
        def _():
            remote(src, vb.at[0, 1, p], k_send.at[5], kr_p.at[4], partner).start()

        return carry

    with jax.named_scope("vproj"):
        lax.fori_loop(0, k_tiles, v_tile, 0)

    def q_tile(n, carry):
        slot = lax.rem(kv_tiles + n, SLOTS)
        w_copy(wq, 0, slot).wait()
        ahead = lax.rem(kv_tiles + AHEAD + n, SLOTS)

        @pl.when(n + AHEAD < q_tiles)
        def _():
            w_copy(wq, (n + AHEAD) * TILE, ahead).start()

        @pl.when(n + AHEAD >= q_tiles)
        def _():
            w_copy(wo, (n + AHEAD - q_tiles) * TILE, ahead).start()

        y = jnp.dot(xb[...], wbuf[slot], preferred_element_type=jnp.float32).astype(jnp.bfloat16)
        for h in range(PER_TILE):
            q_s[n, h] = y[:, h * HEAD:(h + 1) * HEAD]
        return carry

    with jax.named_scope("qproj"):
        lax.fori_loop(0, q_tiles, q_tile, 0)
    for n in range(AHEAD, o_tiles):
        w_copy(wo, n * TILE, (kv_tiles + q_tiles + n) % SLOTS).start()

    def k_partner(r, p):
        remote(kb.at[r, 0, p], kb.at[r, 1, p], k_send.at[5 + r], kr_p.at[r], partner).start()

    def v_partner(r, p):
        remote(vb.at[r, 0, p], vb.at[r, 1, p], k_send.at[8 + r], kr_p.at[4 + r], partner).start()

    @pl.when(gets_left)
    def _():
        for p in range(k_tiles):
            got(kb.at[3, 0, p], kr_l.at[p])

            @pl.when(fwd_k)
            def _():
                remote(kb.at[3, 0, p], kb.at[2, 0, p], k_send.at[12], kr_o.at[p], right).start()

            k_partner(3, p)

    expert = lax.broadcasted_iota(jnp.int32, (n_exp, tok), 0)
    hit0 = expert == ids_ref[0:1, :]
    hit1 = expert == ids_ref[1:2, :]
    probs = probs_ref[...]
    p0 = jnp.sum(jnp.where(hit0, probs, 0.0), axis=0, keepdims=True)
    p1 = jnp.sum(jnp.where(hit1, probs, 0.0), axis=0, keepdims=True)
    total = p0 + p1
    hits = hit0 | hit1
    before = (lax.broadcasted_iota(jnp.int32, (tok, tok), 0)
              < lax.broadcasted_iota(jnp.int32, (tok, tok), 1)).astype(jnp.float32).astype(jnp.bfloat16)
    earlier = jnp.dot(hits.astype(jnp.float32).astype(jnp.bfloat16), before, preferred_element_type=jnp.float32)
    meta_s[0:n_exp, :] = jnp.where(hits, earlier, -1.0)
    meta_s[n_exp:2 * n_exp, :] = jnp.where(hit0, p0 / total, jnp.where(hit1, p1 / total, 0.0))

    def attend(r, parts, lo=0, hi=None, first=False, diagonal=False):
        hi = q_tiles if hi is None else hi
        spare = q_tiles
        keys = parts * tok
        if diagonal:
            key_i = lax.broadcasted_iota(jnp.int32, (tok, tok), 0)
            row_i = lax.broadcasted_iota(jnp.int32, (tok, tok), 1)
            seen = row_i >= key_i

        def score(g, into, h, side):
            kp = lax.div(g, PER_TILE)
            kh = lax.rem(g, PER_TILE)
            q = q_s[g, h]
            top = None if first else top_s[g, h]
            old = top
            for o in range(parts):
                s = lax.dot_general(kb[r, o, kp, kh], q, (((1,), (1,)), ((), ())), preferred_element_type=jnp.float32)
                if diagonal and o == 0:
                    s = jnp.where(seen, s, -1e30)
                s_b[side, h, o] = s
                high = jnp.max(s, axis=0, keepdims=True)
                top = high if top is None else jnp.maximum(top, high)
            top_s[into, h] = top
            if not first:
                keep_s[into, h] = jnp.exp2((old - top) * EXP2_SCALE)

        def weigh(g, h, side):
            top = top_s[g, h]
            mass = None
            for o in range(parts):
                e = jnp.exp2((s_b[side, h, o] - top) * EXP2_SCALE)
                e_b[side, h, o * tok:(o + 1) * tok, :] = e.astype(jnp.bfloat16)
                part = jnp.sum(e, axis=0, keepdims=True)
                mass = part if mass is None else mass + part
            mass_s[g, h] = mass if first else mass + keep_s[g, h] * mass_s[g, h]

        def apply(g, into, h, side):
            kp = lax.div(g, PER_TILE)
            kh = lax.rem(g, PER_TILE)
            v = jnp.concatenate([vb[r, o, kp, kh] for o in range(parts)], axis=1)
            out = jnp.dot(v, e_b[side, h, 0:keys, :], preferred_element_type=jnp.float32)
            acc[into, h] = out if first else out + keep_s[into, h] * acc[into, h]

        def head_groups(i, carry):
            g = lo + 2 * i
            below = jnp.maximum(g - 1, lo)
            below_into = lax.select(g == lo, spare, g - 1)
            above = jnp.minimum(g + 2, hi - 1)
            above_into = lax.select(g == hi - 2, spare, g + 2)
            for h in range(PER_TILE):
                weigh(g, h, 0)
                score(g + 1, g + 1, h, 1)
                apply(below, below_into, h, 1)
            for h in range(PER_TILE):
                weigh(g + 1, h, 1)
                score(above, above_into, h, 0)
                apply(g, g, h, 0)
            return carry

        for h in range(PER_TILE):
            score(lo, lo, h, 0)
        lax.fori_loop(0, (hi - lo) // 2, head_groups, 0)
        for h in range(PER_TILE):
            apply(hi - 1, hi - 1, h, 1)

    for h in range(PER_TILE):
        e_b[1, h] = jnp.zeros((2 * tok, tok), jnp.bfloat16)
        acc[q_tiles, h] = jnp.zeros((HEAD, tok), jnp.float32)
        keep_s[q_tiles, h] = jnp.zeros((1, tok), jnp.float32)

    @pl.when(core == 0)
    def _():
        with jax.named_scope("att_own1"):
            attend(0, 1, first=True, diagonal=True)

    @pl.when(core == 1)
    def _():
        got(kb.at[0, 1], kr_p.at[0])
        got(vb.at[0, 1], kr_p.at[4])
        with jax.named_scope("att_own2"):
            attend(0, 2, first=True, diagonal=True)

    m_rows = meta_all.at[me]
    loc = pltpu.make_async_copy(meta_s, m_rows, m_loc)
    loc.start()
    for d in range(1, group):
        remote(meta_s, m_rows, m_send.at[d - 1], m_recv.at[d - 1], lax.rem(me + d, group)).start()

    @pl.when(gets_right_v)
    def _():
        for p in range(k_tiles):
            got(vb.at[1, 0, p], kr_r.at[k_tiles + p])
            remote(vb.at[1, 0, p], vb.at[2, 0, p], k_send.at[13], kr_o.at[k_tiles + p], left).start()

    @pl.when(gets_right_k)
    def _():
        for p in range(k_tiles):
            got(kb.at[1, 0, p], kr_r.at[p])
            k_partner(1, p)
            v_partner(1, p)

    @pl.when(gets_left)
    def _():
        for p in range(k_tiles):
            got(vb.at[3, 0, p], kr_l.at[k_tiles + p])
            v_partner(3, p)
        got(kb.at[3, 1], kr_p.at[3])
        got(vb.at[3, 1], kr_p.at[7])
        with jax.named_scope("att_left"):
            attend(3, 2)

    def take_opp():
        for p in range(k_tiles):
            got(kb.at[2, 0, p], kr_o.at[p])
            k_partner(2, p)
            got(vb.at[2, 0, p], kr_o.at[k_tiles + p])
            v_partner(2, p)

    @pl.when(gets_right_k)
    def _():
        got(kb.at[1, 1], kr_p.at[1])
        got(vb.at[1, 1], kr_p.at[5])
        with jax.named_scope("att_right_a"):
            attend(1, 2, hi=q_tiles // 2)
        take_opp()
        with jax.named_scope("att_right_b"):
            attend(1, 2, lo=q_tiles // 2)

    @pl.when(gets_opp)
    def _():
        @pl.when(jnp.logical_not(gets_right_k))
        def _():
            take_opp()

        got(kb.at[2, 1], kr_p.at[2])
        got(vb.at[2, 1], kr_p.at[6])
        with jax.named_scope("att_opp"):
            attend(2, 2)

    def finish(g, carry):
        for h in range(PER_TILE):
            o = jnp.transpose(acc[g, h] * (1.0 / mass_s[g, h]))
            o_s[:, pl.ds(pl.multiple_of(g * TILE + h * HEAD, HEAD), HEAD)] = o.astype(jnp.bfloat16)
        return carry

    with jax.named_scope("finish"):
        lax.fori_loop(0, q_tiles, finish, 0)

    def rows_of(dev):
        return pl.ds(pl.multiple_of(dev * tok, tok), tok)

    def piece(dev, n):
        col = n * TILE
        if not isinstance(col, int):
            col = pl.multiple_of(col, TILE)
        return h_all.at[rows_of(dev), pl.ds(col, TILE)]

    def to_left(n):
        remote(h_s.at[n], piece(me, n), h_send.at[1], hr_r.at[n], left).start()

    def o_tile(n, carry):
        slot = lax.rem(kv_tiles + q_tiles + n, SLOTS)
        w_copy(wo, 0, slot).wait()
        y = jnp.dot(o_s[...], wbuf[slot], preferred_element_type=jnp.float32)
        x = xb[:, pl.ds(pl.multiple_of(n * TILE, TILE), TILE)].astype(jnp.float32)
        h_s[n] = (x + y).astype(jnp.bfloat16)
        remote(h_s.at[n], piece(me, n), h_send.at[0], hr_l.at[n], right).start()

        @pl.when(chip > 0)
        def _():
            to_left(n)

        remote(h_s.at[n], piece(me, n), h_send.at[2], hr_p.at[0], partner).start()
        pltpu.make_async_copy(h_s.at[n], piece(me, n), x_sem).start()
        return carry

    with jax.named_scope("oproj"):
        lax.fori_loop(0, o_tiles, o_tile, 0)

    @pl.when(chip == 0)
    def _():
        got(vb.at[0, 0], k_send.at[13])
        for n in range(o_tiles):
            to_left(n)


    def of_chips(which):
        hit = jnp.bool_(False)
        for c in which:
            hit = hit | (chip == c)
        return hit

    on_right = [[n in VIA_NEXT[(c - 1) % chips] for n in range(o_tiles)] for c in range(chips)]
    on_left = [[n not in VIA_NEXT[(c + 1) % chips] for n in range(o_tiles)] for c in range(chips)]

    def from_left(n):
        with jax.named_scope("w_left%d" % n):
            got(piece(left, n), hr_l.at[n])

        @pl.when(of_chips([c for c in range(chips) if on_right[c][n]]))
        def _():
            remote(piece(left, n), piece(left, n), h_send.at[6], hr_o.at[n], right).start()

        remote(piece(left, n), piece(left, n), h_send.at[5], hr_p.at[3], partner).start()

    def from_right(n):
        with jax.named_scope("w_right%d" % n):
            got(piece(right, n), hr_r.at[n])

        @pl.when(of_chips([c for c in range(chips) if on_left[c][n]]))
        def _():
            remote(piece(right, n), piece(right, n), h_send.at[7], hr_o.at[n], left).start()

        remote(piece(right, n), piece(right, n), h_send.at[3], hr_p.at[1], partner).start()

    def in_turn(early, late):
        for n in range(o_tiles + LAG):
            if n < o_tiles:
                early(n)
            if n >= LAG:
                late(n - LAG)

    early_right = (chip == 0) | (chip == last)

    @pl.when(early_right)
    def _():
        in_turn(from_right, from_left)

    @pl.when(jnp.logical_not(early_right))
    def _():
        in_turn(from_left, from_right)

    for n in range(o_tiles):
        with jax.named_scope("w_opp%d" % n):
            got(piece(opp, n), hr_o.at[n])
        remote(piece(opp, n), piece(opp, n), h_send.at[4], hr_p.at[2], partner).start()

    mine = h_all.at[rows_of(me)]
    got(mine, x_sem)
    for i in range(6):
        got(mine, h_send.at[i])
    for c in range(chips):
        @pl.when(chip == c)
        def _():
            for i, on in ((6, on_right[c]), (7, on_left[c])):
                if sum(on):
                    got(h_all.at[rows_of(me), pl.ds(0, sum(on) * TILE)], h_send.at[i])
    for r in range(chips):
        got(h_all.at[rows_of(lax.rem(partner + 2 * r, group))], hr_p.at[r])
    k_own = kb.at[0, 0]
    v_own = vb.at[0, 0]
    for when, waits in ((sends_right, ((k_own, 0), (v_own, 3))), (sends_left_k, ((k_own, 1),)), (sends_left_v, ((v_own, 4),)),
                        (core == 0, ((k_own, 2), (v_own, 5))), (gets_left, ((k_own, 8), (v_own, 11))),
                        (gets_right_k, ((k_own, 6), (v_own, 9))), (gets_opp, ((k_own, 7), (v_own, 10))),
                        (fwd_k, ((k_own, 12),)), (chip == last, ((v_own, 13),))):
        @pl.when(when)
        def _(waits=waits):
            for ref, i in waits:
                got(ref, k_send.at[i])

    loc.wait()
    for d in range(1, group):
        got(meta_s, m_send.at[d - 1])
        got(meta_all.at[lax.rem(me + group - d, group)], m_recv.at[d - 1])


def dispatch_kernel(n_exp, own_exp, meta_ref, h_hbm, hid_hbm, buf_hbm, hb, ob, h_sem, o_sem, hid_sem):
    group, tok, width = hb.shape
    slots = ob.shape[0]
    me = lax.axis_index("sp")
    steps = group * own_exp
    row = lax.broadcasted_iota(jnp.int32, (tok, tok), 0).astype(jnp.float32)

    def h_copy(s):
        return pltpu.make_async_copy(h_hbm.at[pl.ds(pl.multiple_of(s * tok, tok) if not isinstance(s, int) else s * tok, tok)], hb.at[s], h_sem.at[s])

    def o_copy(i):
        s = lax.div(i, own_exp)
        return pltpu.make_async_copy(ob.at[lax.rem(i, slots)],
                                     buf_hbm.at[lax.rem(i, own_exp), pl.ds(pl.multiple_of(s * tok, tok), tok)],
                                     o_sem.at[lax.rem(i, slots)])

    for s in range(H_AHEAD):
        h_copy(s).start()

    def step(i, carry):
        s = lax.div(i, own_exp)
        e = lax.rem(i, own_exp)

        @pl.when(e == 0)
        def _():
            pltpu.make_async_copy(hb.at[s], hb.at[s], h_sem.at[s]).wait()

            @pl.when(s + H_AHEAD < group)
            def _():
                h_copy(s + H_AHEAD).start()

            @pl.when(s == me)
            def _():
                pltpu.make_async_copy(hb.at[s], hid_hbm, hid_sem).start()

        @pl.when(i >= slots)
        def _():
            o_copy(i - slots).wait()

        expert = me * own_exp + e
        slot = meta_ref[s, pl.ds(expert, 1), :]
        gate = meta_ref[s, pl.ds(n_exp + expert, 1), :]
        pick = row == slot
        gate_col = jnp.sum(jnp.where(pick, gate, 0.0), axis=1, keepdims=True)
        pick = pick.astype(jnp.float32).astype(jnp.bfloat16)
        o = lax.rem(i, slots)
        for c in range(0, width, TILE):
            rows = jnp.dot(pick, hb[s, :, c:c + TILE], preferred_element_type=jnp.float32)
            ob[o, :, c:c + TILE] = (rows * gate_col).astype(jnp.bfloat16)
        o_copy(i).start()
        return carry

    lax.fori_loop(0, steps, step, 0)
    for i in range(steps - slots, steps):
        o_copy(i).wait()
    pltpu.make_async_copy(hb.at[0], hid_hbm, hid_sem).wait()


def solution(mesh):
    group = mesh.shape['sp']
    row_spec = P(('dp', 'sp'), None)
    buf_spec = P(('dp', 'sp'), None, None)

    def device_step(x_loc, w_q, w_k, w_v, w_o, ids_loc, probs_loc):
        tok, width = x_loc.shape
        n_exp = probs_loc.shape[1]
        own_exp = n_exp // group
        seq = tok * group
        q_tiles = w_q.shape[1] // TILE
        k_tiles = w_k.shape[1] // TILE
        chips = group // 2
        o_tiles = width // TILE
        bf16 = jnp.bfloat16
        any_spec = pl.BlockSpec(memory_space=pl.ANY)
        vmem_spec = pl.BlockSpec(memory_space=pltpu.VMEM)
        dma = pltpu.SemaphoreType.DMA
        h_all, meta_all = pl.pallas_call(
            functools.partial(block_kernel, group, n_exp),
            out_shape=(jax.ShapeDtypeStruct((seq, width), bf16),
                       jax.ShapeDtypeStruct((group, 2 * n_exp, tok), jnp.float32)),
            in_specs=[any_spec] * 5 + [vmem_spec] * 2,
            out_specs=(any_spec, any_spec),
            scratch_shapes=[
                pltpu.VMEM((tok, width), bf16),
                pltpu.VMEM((SLOTS, width, TILE), bf16),
                pltpu.VMEM((chips, 2, k_tiles, PER_TILE, tok, HEAD), bf16),
                pltpu.VMEM((chips, 2, k_tiles, PER_TILE, HEAD, tok), bf16),
                pltpu.VMEM((q_tiles, PER_TILE, tok, HEAD), bf16),
                pltpu.VMEM((q_tiles + 1, PER_TILE, HEAD, tok), jnp.float32),
                pltpu.VMEM((q_tiles + 1, PER_TILE, 1, tok), jnp.float32),
                pltpu.VMEM((q_tiles + 1, PER_TILE, 1, tok), jnp.float32),
                pltpu.VMEM((q_tiles + 1, PER_TILE, 1, tok), jnp.float32),
                pltpu.VMEM((2, PER_TILE, 2, tok, tok), jnp.float32),
                pltpu.VMEM((2, PER_TILE, 2 * tok, tok), bf16),
                pltpu.VMEM((tok, q_tiles * TILE), bf16),
                pltpu.VMEM((o_tiles, tok, TILE), bf16),
                pltpu.VMEM((2 * n_exp, tok), jnp.float32),
                dma, dma((SLOTS,)),
                dma((14,)), dma((2 * k_tiles,)), dma((2 * k_tiles,)), dma((2 * k_tiles,)), dma((2 * chips,)),
                dma((8,)), dma((o_tiles,)), dma((o_tiles,)), dma((o_tiles,)), dma((chips,)),
                dma((group - 1,)), dma((group - 1,)), dma,
            ],
            compiler_params=pltpu.CompilerParams(collective_id=0, has_side_effects=True,
                                                 vmem_limit_bytes=VMEM_LIMIT),
            name="block",
        )(x_loc, w_q, w_k, w_v, w_o, ids_loc.T, probs_loc.T)

        hidden_out, buf = pl.pallas_call(
            functools.partial(dispatch_kernel, n_exp, own_exp),
            out_shape=(jax.ShapeDtypeStruct((tok, width), bf16),
                       jax.ShapeDtypeStruct((own_exp, seq, width), bf16)),
            in_specs=[vmem_spec, any_spec],
            out_specs=(any_spec, any_spec),
            scratch_shapes=[pltpu.VMEM((group, tok, width), bf16), pltpu.VMEM((OUT_SLOTS, tok, width), bf16),
                            dma((group,)), dma((OUT_SLOTS,)), dma],
            compiler_params=pltpu.CompilerParams(vmem_limit_bytes=VMEM_LIMIT),
            name="dispatch",
        )(meta_all, h_all)
        return hidden_out, buf

    return jax.shard_map(device_step, mesh=mesh,
                         in_specs=(row_spec, P(), P(), P(), P(), row_spec, row_spec),
                         out_specs=(row_spec, buf_spec), check_vma=False)
```

```python
import functools
import math

import jax
import jax.numpy as jnp
from jax import lax
from jax.experimental import pallas as pl
from jax.experimental.pallas import tpu as pltpu
from jax.sharding import PartitionSpec as P

HEAD = 128
EXP2_SCALE = math.log2(math.e) / math.sqrt(HEAD)
MESH = pl.DeviceIdType.MESH
TILE = 512
SLOTS = 8
PER_TILE = TILE // HEAD
AHEAD = 3
VMEM_LIMIT = 67_000_000
VIA_NEXT = ((0, 1, 3, 4, 6, 7, 9, 10, 12, 13, 15), (0, 3, 6, 9, 12, 15), (2, 5, 8, 11, 14), (0, 1, 2, 4, 5, 6, 8, 9, 10, 12, 13, 14))
LAG = 3
H_AHEAD = 2
OUT_SLOTS = 10


def block_kernel(group, n_exp, x_hbm, wq, wk, wv, wo, ids_ref, probs_ref, h_all, meta_all,
                 xb, wbuf, kb, vb, q_s, acc, top_s, mass_s, keep_s, s_b, e_b, o_s, h_s, meta_s,
                 x_sem, w_sem, k_send, kr_l, kr_r, kr_o, kr_p, h_send, hr_l, hr_r, hr_o, hr_p, m_send, m_recv, m_loc):
    tok = xb.shape[0]
    chips = group // 2
    q_tiles = wq.shape[1] // TILE
    k_tiles = wk.shape[1] // TILE
    kv_tiles = 2 * k_tiles
    o_tiles = wo.shape[1] // TILE
    me = lax.axis_index("sp")
    core = lax.rem(me, 2)
    chip = lax.div(me, 2)
    right = lax.rem(me + 2, group)
    left = lax.rem(me + group - 2, group)
    partner = me + 1 - 2 * core
    opp = lax.rem(me + 4, group)
    last = chips - 1

    def remote(src, dst, send, recv, dev):
        return pltpu.make_async_remote_copy(src_ref=src, dst_ref=dst, send_sem=send, recv_sem=recv,
                                            device_id={"sp": dev}, device_id_type=MESH)

    def got(ref, sem):
        pltpu.make_async_copy(ref, ref, sem).wait()

    def w_copy(arr, col, slot):
        if not isinstance(col, int):
            col = pl.multiple_of(col, TILE)
        return pltpu.make_async_copy(arr.at[:, pl.ds(col, TILE)], wbuf.at[slot], w_sem.at[slot])

    x_copy = pltpu.make_async_copy(x_hbm, xb, x_sem)
    x_copy.start()
    w_copy(wk, 0, 0).start()

    barrier = pltpu.get_barrier_semaphore()
    for d in range(1, group):
        pl.semaphore_signal(barrier, inc=1, device_id={"sp": lax.rem(me + d, group)}, device_id_type=MESH)
    x_copy.wait()
    w_copy(wk, TILE, 1).start()

    sends_right = chip < last
    sends_left_k = chip == 0
    sends_left_v = chip < 2
    gets_left = chip > 0
    gets_right_k = chip == last
    fwd_k = (chip > 0) & (chip < last)
    gets_opp = chip >= 2

    def k_tile(p, carry):
        w_copy(wk, 0, p).wait()
        w_copy(wv, p * TILE, k_tiles + p).start()

        @pl.when(p == k_tiles - 1)
        def _():
            w_copy(wq, 0, kv_tiles).start()

        y = jnp.dot(xb[...], wbuf[p], preferred_element_type=jnp.float32).astype(jnp.bfloat16)
        for h in range(PER_TILE):
            kb[0, 0, p, h] = y[:, h * HEAD:(h + 1) * HEAD]

        @pl.when(p == 0)
        def _():
            pl.semaphore_wait(barrier, group - 1)

        src = kb.at[0, 0, p]

        @pl.when(sends_right)
        def _():
            remote(src, kb.at[3, 0, p], k_send.at[0], kr_l.at[p], right).start()

        @pl.when(sends_left_k)
        def _():
            remote(src, kb.at[1, 0, p], k_send.at[1], kr_r.at[p], left).start()

        @pl.when(core == 0)
        def _():
            remote(src, kb.at[0, 1, p], k_send.at[2], kr_p.at[0], partner).start()

        return carry

    with jax.named_scope("kproj"):
        lax.fori_loop(0, k_tiles, k_tile, 0)

    def v_tile(p, carry):
        w_copy(wv, 0, k_tiles + p).wait()
        w_copy(wq, (1 + p) * TILE, kv_tiles + 1 + p).start()
        y = jnp.dot(xb[...], wbuf[k_tiles + p], preferred_element_type=jnp.float32)
        for h in range(PER_TILE):
            vb[0, 0, p, h] = jnp.transpose(y[:, h * HEAD:(h + 1) * HEAD]).astype(jnp.bfloat16)
        src = vb.at[0, 0, p]

        @pl.when(sends_right)
        def _():
            remote(src, vb.at[3, 0, p], k_send.at[3], kr_l.at[k_tiles + p], right).start()

        @pl.when(sends_left_v)
        def _():
            remote(src, vb.at[1, 0, p], k_send.at[4], kr_r.at[k_tiles + p], left).start()

        @pl.when(core == 0)
        def _():
            remote(src, vb.at[0, 1, p], k_send.at[5], kr_p.at[4], partner).start()

        return carry

    with jax.named_scope("vproj"):
        lax.fori_loop(0, k_tiles, v_tile, 0)

    def q_tile(n, carry):
        slot = lax.rem(kv_tiles + n, SLOTS)
        w_copy(wq, 0, slot).wait()
        ahead = lax.rem(kv_tiles + AHEAD + n, SLOTS)

        @pl.when(n + AHEAD < q_tiles)
        def _():
            w_copy(wq, (n + AHEAD) * TILE, ahead).start()

        @pl.when(n + AHEAD >= q_tiles)
        def _():
            w_copy(wo, (n + AHEAD - q_tiles) * TILE, ahead).start()

        y = jnp.dot(xb[...], wbuf[slot], preferred_element_type=jnp.float32).astype(jnp.bfloat16)
        for h in range(PER_TILE):
            q_s[n, h] = y[:, h * HEAD:(h + 1) * HEAD]
        return carry

    with jax.named_scope("qproj"):
        lax.fori_loop(0, q_tiles, q_tile, 0)
    for n in range(AHEAD, o_tiles):
        w_copy(wo, n * TILE, (kv_tiles + q_tiles + n) % SLOTS).start()

    def k_partner(r, p):
        remote(kb.at[r, 0, p], kb.at[r, 1, p], k_send.at[5 + r], kr_p.at[r], partner).start()

    def v_partner(r, p):
        remote(vb.at[r, 0, p], vb.at[r, 1, p], k_send.at[8 + r], kr_p.at[4 + r], partner).start()

    @pl.when(gets_left)
    def _():
        for p in range(k_tiles):
            got(kb.at[3, 0, p], kr_l.at[p])

            @pl.when(fwd_k)
            def _():
                remote(kb.at[3, 0, p], kb.at[2, 0, p], k_send.at[12], kr_o.at[p], right).start()

            k_partner(3, p)

    expert = lax.broadcasted_iota(jnp.int32, (n_exp, tok), 0)
    hit0 = expert == ids_ref[0:1, :]
    hit1 = expert == ids_ref[1:2, :]
    probs = probs_ref[...]
    p0 = jnp.sum(jnp.where(hit0, probs, 0.0), axis=0, keepdims=True)
    p1 = jnp.sum(jnp.where(hit1, probs, 0.0), axis=0, keepdims=True)
    total = p0 + p1
    hits = hit0 | hit1
    before = (lax.broadcasted_iota(jnp.int32, (tok, tok), 0)
              < lax.broadcasted_iota(jnp.int32, (tok, tok), 1)).astype(jnp.float32).astype(jnp.bfloat16)
    earlier = jnp.dot(hits.astype(jnp.float32).astype(jnp.bfloat16), before, preferred_element_type=jnp.float32)
    meta_s[0:n_exp, :] = jnp.where(hits, earlier, -1.0)
    meta_s[n_exp:2 * n_exp, :] = jnp.where(hit0, p0 / total, jnp.where(hit1, p1 / total, 0.0))

    def attend(r, parts, lo=0, hi=None, first=False, diagonal=False):
        hi = q_tiles if hi is None else hi
        spare = q_tiles
        keys = parts * tok
        if diagonal:
            key_i = lax.broadcasted_iota(jnp.int32, (tok, tok), 0)
            row_i = lax.broadcasted_iota(jnp.int32, (tok, tok), 1)
            seen = row_i >= key_i

        def score(g, into, h, side):
            kp = lax.div(g, PER_TILE)
            kh = lax.rem(g, PER_TILE)
            q = q_s[g, h]
            top = None if first else top_s[g, h]
            old = top
            for o in range(parts):
                s = lax.dot_general(kb[r, o, kp, kh], q, (((1,), (1,)), ((), ())), preferred_element_type=jnp.float32)
                if diagonal and o == 0:
                    s = jnp.where(seen, s, -1e30)
                s_b[side, h, o] = s
                high = jnp.max(s, axis=0, keepdims=True)
                top = high if top is None else jnp.maximum(top, high)
            top_s[into, h] = top
            if not first:
                keep_s[into, h] = jnp.exp2((old - top) * EXP2_SCALE)

        def weigh(g, h, side):
            top = top_s[g, h]
            mass = None
            for o in range(parts):
                e = jnp.exp2((s_b[side, h, o] - top) * EXP2_SCALE)
                e_b[side, h, o * tok:(o + 1) * tok, :] = e.astype(jnp.bfloat16)
                part = jnp.sum(e, axis=0, keepdims=True)
                mass = part if mass is None else mass + part
            mass_s[g, h] = mass if first else mass + keep_s[g, h] * mass_s[g, h]

        def apply(g, into, h, side):
            kp = lax.div(g, PER_TILE)
            kh = lax.rem(g, PER_TILE)
            v = jnp.concatenate([vb[r, o, kp, kh] for o in range(parts)], axis=1)
            out = jnp.dot(v, e_b[side, h, 0:keys, :], preferred_element_type=jnp.float32)
            acc[into, h] = out if first else out + keep_s[into, h] * acc[into, h]

        def head_groups(i, carry):
            g = lo + 2 * i
            below = jnp.maximum(g - 1, lo)
            below_into = lax.select(g == lo, spare, g - 1)
            above = jnp.minimum(g + 2, hi - 1)
            above_into = lax.select(g == hi - 2, spare, g + 2)
            for h in range(PER_TILE):
                weigh(g, h, 0)
                score(g + 1, g + 1, h, 1)
                apply(below, below_into, h, 1)
            for h in range(PER_TILE):
                weigh(g + 1, h, 1)
                score(above, above_into, h, 0)
                apply(g, g, h, 0)
            return carry

        for h in range(PER_TILE):
            score(lo, lo, h, 0)
        lax.fori_loop(0, (hi - lo) // 2, head_groups, 0)
        for h in range(PER_TILE):
            apply(hi - 1, hi - 1, h, 1)

    for h in range(PER_TILE):
        e_b[1, h] = jnp.zeros((2 * tok, tok), jnp.bfloat16)
        acc[q_tiles, h] = jnp.zeros((HEAD, tok), jnp.float32)
        keep_s[q_tiles, h] = jnp.zeros((1, tok), jnp.float32)

    @pl.when(core == 0)
    def _():
        with jax.named_scope("att_own1"):
            attend(0, 1, first=True, diagonal=True)

    @pl.when(core == 1)
    def _():
        got(kb.at[0, 1], kr_p.at[0])
        got(vb.at[0, 1], kr_p.at[4])
        with jax.named_scope("att_own2"):
            attend(0, 2, first=True, diagonal=True)

    m_rows = meta_all.at[me]
    loc = pltpu.make_async_copy(meta_s, m_rows, m_loc)
    loc.start()
    for d in range(1, group):
        remote(meta_s, m_rows, m_send.at[d - 1], m_recv.at[d - 1], lax.rem(me + d, group)).start()

    def values_on_left():
        for p in range(k_tiles):
            got(vb.at[1, 0, p], kr_r.at[k_tiles + p])
            remote(vb.at[1, 0, p], vb.at[2, 0, p], k_send.at[13], kr_o.at[k_tiles + p], left).start()

    @pl.when(chip == last)
    def _():
        values_on_left()

    @pl.when(gets_right_k)
    def _():
        for p in range(k_tiles):
            got(kb.at[1, 0, p], kr_r.at[p])
            k_partner(1, p)
            v_partner(1, p)

    @pl.when(gets_left)
    def _():
        for p in range(k_tiles):
            got(vb.at[3, 0, p], kr_l.at[k_tiles + p])
            v_partner(3, p)
        got(kb.at[3, 1], kr_p.at[3])
        got(vb.at[3, 1], kr_p.at[7])
        with jax.named_scope("att_left"):
            attend(3, 2)

    def take_opp():
        for p in range(k_tiles):
            got(kb.at[2, 0, p], kr_o.at[p])
            k_partner(2, p)
            got(vb.at[2, 0, p], kr_o.at[k_tiles + p])
            v_partner(2, p)

    @pl.when(gets_right_k)
    def _():
        got(kb.at[1, 1], kr_p.at[1])
        got(vb.at[1, 1], kr_p.at[5])
        with jax.named_scope("att_right_a"):
            attend(1, 2, hi=q_tiles - 2)
        take_opp()
        with jax.named_scope("att_right_b"):
            attend(1, 2, lo=q_tiles - 2)

    @pl.when(gets_opp)
    def _():
        @pl.when(jnp.logical_not(gets_right_k))
        def _():
            take_opp()

        got(kb.at[2, 1], kr_p.at[2])
        got(vb.at[2, 1], kr_p.at[6])
        with jax.named_scope("att_opp"):
            attend(2, 2)

    def finish(g, carry):
        for h in range(PER_TILE):
            o = jnp.transpose(acc[g, h] * (1.0 / mass_s[g, h]))
            o_s[:, pl.ds(pl.multiple_of(g * TILE + h * HEAD, HEAD), HEAD)] = o.astype(jnp.bfloat16)
        return carry

    with jax.named_scope("finish"):
        lax.fori_loop(0, q_tiles, finish, 0)

    @pl.when(chip == 0)
    def _():
        got(kb.at[0, 0], k_send.at[1])
        got(vb.at[0, 0], k_send.at[4])
        values_on_left()

    def rows_of(dev):
        return pl.ds(pl.multiple_of(dev * tok, tok), tok)

    def piece(dev, n):
        col = n * TILE
        if not isinstance(col, int):
            col = pl.multiple_of(col, TILE)
        return h_all.at[rows_of(dev), pl.ds(col, TILE)]

    def to_left(n):
        remote(h_s.at[n], piece(me, n), h_send.at[1], hr_r.at[n], left).start()

    def o_tile(n, carry):
        slot = lax.rem(kv_tiles + q_tiles + n, SLOTS)
        w_copy(wo, 0, slot).wait()
        y = jnp.dot(o_s[...], wbuf[slot], preferred_element_type=jnp.float32)
        x = xb[:, pl.ds(pl.multiple_of(n * TILE, TILE), TILE)].astype(jnp.float32)
        h_s[n] = (x + y).astype(jnp.bfloat16)
        remote(h_s.at[n], piece(me, n), h_send.at[0], hr_l.at[n], right).start()

        @pl.when(chip > 0)
        def _():
            to_left(n)

        remote(h_s.at[n], piece(me, n), h_send.at[2], hr_p.at[0], partner).start()
        pltpu.make_async_copy(h_s.at[n], piece(me, n), x_sem).start()
        return carry

    with jax.named_scope("oproj"):
        lax.fori_loop(0, o_tiles, o_tile, 0)

    @pl.when(chip == 0)
    def _():
        got(vb.at[0, 0], k_send.at[13])
        for n in range(o_tiles):
            to_left(n)


    def of_chips(which):
        hit = jnp.bool_(False)
        for c in which:
            hit = hit | (chip == c)
        return hit

    halves = 2 * o_tiles
    on_right = [[m in VIA_NEXT[(c - 1) % chips] for m in range(halves)] for c in range(chips)]
    on_left = [[m not in VIA_NEXT[(c + 1) % chips] for m in range(halves)] for c in range(chips)]

    def half_piece(dev, m):
        return h_all.at[rows_of(dev), pl.ds(m * (TILE // 2), TILE // 2)]

    def from_left(n):
        with jax.named_scope("w_left%d" % n):
            got(piece(left, n), hr_l.at[n])
        for m in (2 * n, 2 * n + 1):
            @pl.when(of_chips([c for c in range(chips) if on_right[c][m]]))
            def _(m=m):
                remote(half_piece(left, m), half_piece(left, m), h_send.at[6], hr_o.at[m], right).start()

        remote(piece(left, n), piece(left, n), h_send.at[5], hr_p.at[3], partner).start()

    def from_right(n):
        with jax.named_scope("w_right%d" % n):
            got(piece(right, n), hr_r.at[n])
        for m in (2 * n, 2 * n + 1):
            @pl.when(of_chips([c for c in range(chips) if on_left[c][m]]))
            def _(m=m):
                remote(half_piece(right, m), half_piece(right, m), h_send.at[7], hr_o.at[m], left).start()

        remote(piece(right, n), piece(right, n), h_send.at[3], hr_p.at[1], partner).start()

    def in_turn(early, late):
        for n in range(o_tiles + LAG):
            if n < o_tiles:
                early(n)
            if n >= LAG:
                late(n - LAG)

    early_right = (chip == 0) | (chip == last)

    @pl.when(early_right)
    def _():
        in_turn(from_right, from_left)

    @pl.when(jnp.logical_not(early_right))
    def _():
        in_turn(from_left, from_right)

    for n in range(halves):
        with jax.named_scope("w_opp%d" % n):
            got(half_piece(opp, n), hr_o.at[n])
        remote(half_piece(opp, n), half_piece(opp, n), h_send.at[4], hr_p.at[2], partner).start()

    mine = h_all.at[rows_of(me)]
    got(mine, x_sem)
    for i in range(6):
        got(mine, h_send.at[i])
    for c in range(chips):
        @pl.when(chip == c)
        def _():
            for i, on in ((6, on_right[c]), (7, on_left[c])):
                if sum(on):
                    got(h_all.at[rows_of(me), pl.ds(0, sum(on) * (TILE // 2))], h_send.at[i])
    for r in range(chips):
        got(h_all.at[rows_of(lax.rem(partner + 2 * r, group))], hr_p.at[r])
    k_own = kb.at[0, 0]
    v_own = vb.at[0, 0]
    for when, waits in ((sends_right, ((k_own, 0), (v_own, 3))), (chip == 1, ((v_own, 4),)),
                        (core == 0, ((k_own, 2), (v_own, 5))), (gets_left, ((k_own, 8), (v_own, 11))),
                        (gets_right_k, ((k_own, 6), (v_own, 9))), (gets_opp, ((k_own, 7), (v_own, 10))),
                        (fwd_k, ((k_own, 12),)), (chip == last, ((v_own, 13),))):
        @pl.when(when)
        def _(waits=waits):
            for ref, i in waits:
                got(ref, k_send.at[i])

    loc.wait()
    for d in range(1, group):
        got(meta_s, m_send.at[d - 1])
        got(meta_all.at[lax.rem(me + group - d, group)], m_recv.at[d - 1])


def dispatch_kernel(n_exp, own_exp, meta_ref, h_hbm, hid_hbm, buf_hbm, hb, ob, h_sem, o_sem, hid_sem):
    group, tok, width = hb.shape
    slots = ob.shape[0]
    me = lax.axis_index("sp")
    steps = group * own_exp
    row = lax.broadcasted_iota(jnp.int32, (tok, tok), 0).astype(jnp.float32)

    def h_copy(s):
        return pltpu.make_async_copy(h_hbm.at[pl.ds(pl.multiple_of(s * tok, tok) if not isinstance(s, int) else s * tok, tok)], hb.at[s], h_sem.at[s])

    def o_copy(i):
        s = lax.div(i, own_exp)
        return pltpu.make_async_copy(ob.at[lax.rem(i, slots)],
                                     buf_hbm.at[lax.rem(i, own_exp), pl.ds(pl.multiple_of(s * tok, tok), tok)],
                                     o_sem.at[lax.rem(i, slots)])

    for s in range(H_AHEAD):
        h_copy(s).start()

    def step(i, carry):
        s = lax.div(i, own_exp)
        e = lax.rem(i, own_exp)

        @pl.when(e == 0)
        def _():
            pltpu.make_async_copy(hb.at[s], hb.at[s], h_sem.at[s]).wait()

            for more in range(H_AHEAD):
                @pl.when(H_AHEAD * (s + 1) + more < group)
                def _(more=more):
                    h_copy(H_AHEAD * (s + 1) + more).start()

            @pl.when(s == me)
            def _():
                pltpu.make_async_copy(hb.at[s], hid_hbm, hid_sem).start()

        @pl.when(i >= slots)
        def _():
            o_copy(i - slots).wait()

        expert = me * own_exp + e
        slot = meta_ref[s, pl.ds(expert, 1), :]
        gate = meta_ref[s, pl.ds(n_exp + expert, 1), :]
        pick = row == slot
        gate_col = jnp.sum(jnp.where(pick, gate, 0.0), axis=1, keepdims=True)
        pick = pick.astype(jnp.float32).astype(jnp.bfloat16)
        o = lax.rem(i, slots)
        for c in range(0, width, TILE):
            rows = jnp.dot(pick, hb[s, :, c:c + TILE], preferred_element_type=jnp.float32)
            ob[o, :, c:c + TILE] = (rows * gate_col).astype(jnp.bfloat16)
        o_copy(i).start()
        return carry

    lax.fori_loop(0, steps, step, 0)
    for i in range(steps - slots, steps):
        o_copy(i).wait()
    pltpu.make_async_copy(hb.at[0], hid_hbm, hid_sem).wait()


def solution(mesh):
    group = mesh.shape['sp']
    row_spec = P(('dp', 'sp'), None)
    buf_spec = P(('dp', 'sp'), None, None)

    def device_step(x_loc, w_q, w_k, w_v, w_o, ids_loc, probs_loc):
        tok, width = x_loc.shape
        n_exp = probs_loc.shape[1]
        own_exp = n_exp // group
        seq = tok * group
        q_tiles = w_q.shape[1] // TILE
        k_tiles = w_k.shape[1] // TILE
        chips = group // 2
        o_tiles = width // TILE
        bf16 = jnp.bfloat16
        any_spec = pl.BlockSpec(memory_space=pl.ANY)
        vmem_spec = pl.BlockSpec(memory_space=pltpu.VMEM)
        dma = pltpu.SemaphoreType.DMA
        h_all, meta_all = pl.pallas_call(
            functools.partial(block_kernel, group, n_exp),
            out_shape=(jax.ShapeDtypeStruct((seq, width), bf16),
                       jax.ShapeDtypeStruct((group, 2 * n_exp, tok), jnp.float32)),
            in_specs=[any_spec] * 5 + [vmem_spec] * 2,
            out_specs=(any_spec, any_spec),
            scratch_shapes=[
                pltpu.VMEM((tok, width), bf16),
                pltpu.VMEM((SLOTS, width, TILE), bf16),
                pltpu.VMEM((chips, 2, k_tiles, PER_TILE, tok, HEAD), bf16),
                pltpu.VMEM((chips, 2, k_tiles, PER_TILE, HEAD, tok), bf16),
                pltpu.VMEM((q_tiles, PER_TILE, tok, HEAD), bf16),
                pltpu.VMEM((q_tiles + 1, PER_TILE, HEAD, tok), jnp.float32),
                pltpu.VMEM((q_tiles + 1, PER_TILE, 1, tok), jnp.float32),
                pltpu.VMEM((q_tiles + 1, PER_TILE, 1, tok), jnp.float32),
                pltpu.VMEM((q_tiles + 1, PER_TILE, 1, tok), jnp.float32),
                pltpu.VMEM((2, PER_TILE, 2, tok, tok), jnp.float32),
                pltpu.VMEM((2, PER_TILE, 2 * tok, tok), bf16),
                pltpu.VMEM((tok, q_tiles * TILE), bf16),
                pltpu.VMEM((o_tiles, tok, TILE), bf16),
                pltpu.VMEM((2 * n_exp, tok), jnp.float32),
                dma, dma((SLOTS,)),
                dma((14,)), dma((2 * k_tiles,)), dma((2 * k_tiles,)), dma((2 * k_tiles,)), dma((2 * chips,)),
                dma((8,)), dma((o_tiles,)), dma((o_tiles,)), dma((2 * o_tiles,)), dma((chips,)),
                dma((group - 1,)), dma((group - 1,)), dma,
            ],
            compiler_params=pltpu.CompilerParams(collective_id=0, has_side_effects=True,
                                                 vmem_limit_bytes=VMEM_LIMIT),
            name="block",
        )(x_loc, w_q, w_k, w_v, w_o, ids_loc.T, probs_loc.T)

        hidden_out, buf = pl.pallas_call(
            functools.partial(dispatch_kernel, n_exp, own_exp),
            out_shape=(jax.ShapeDtypeStruct((tok, width), bf16),
                       jax.ShapeDtypeStruct((own_exp, seq, width), bf16)),
            in_specs=[vmem_spec, any_spec],
            out_specs=(any_spec, any_spec),
            scratch_shapes=[pltpu.VMEM((group, tok, width), bf16), pltpu.VMEM((OUT_SLOTS, tok, width), bf16),
                            dma((group,)), dma((OUT_SLOTS,)), dma],
            compiler_params=pltpu.CompilerParams(vmem_limit_bytes=VMEM_LIMIT),
            name="dispatch",
        )(meta_all, h_all)
        return hidden_out, buf

    return jax.shard_map(device_step, mesh=mesh,
                         in_specs=(row_spec, P(), P(), P(), P(), row_spec, row_spec),
                         out_specs=(row_spec, buf_spec), check_vma=False)
```

```python
import functools
import math

import jax
import jax.numpy as jnp
from jax import lax
from jax.experimental import pallas as pl
from jax.experimental.pallas import tpu as pltpu
from jax.sharding import PartitionSpec as P

HEAD = 128
EXP2_SCALE = math.log2(math.e) / math.sqrt(HEAD)
MESH = pl.DeviceIdType.MESH
TILE = 512
SLOTS = 8
PER_TILE = TILE // HEAD
AHEAD = 3
VMEM_LIMIT = 67_000_000
VIA_NEXT = ((0, 1, 3, 4, 6, 7, 9, 10, 12, 13, 15), (0, 3, 6, 9, 12, 15), (2, 5, 8, 11, 14), (0, 1, 2, 4, 5, 6, 8, 9, 10, 12, 13, 14))
LAG = 3
OUT_SLOTS = 5
COLS = 512


def block_kernel(group, n_exp, x_hbm, wq, wk, wv, wo, ids_ref, probs_ref, h_all, meta_all,
                 xb, wbuf, kb, vb, q_s, acc, top_s, mass_s, keep_s, s_b, e_b, o_s, h_s, meta_s,
                 x_sem, w_sem, k_send, kr_l, kr_r, kr_o, kr_p, h_send, hr_l, hr_r, hr_o, hr_p, m_send, m_recv, m_loc):
    tok = xb.shape[0]
    chips = group // 2
    q_tiles = wq.shape[1] // TILE
    k_tiles = wk.shape[1] // TILE
    kv_tiles = 2 * k_tiles
    o_tiles = wo.shape[1] // TILE
    me = lax.axis_index("sp")
    core = lax.rem(me, 2)
    chip = lax.div(me, 2)
    right = lax.rem(me + 2, group)
    left = lax.rem(me + group - 2, group)
    partner = me + 1 - 2 * core
    opp = lax.rem(me + 4, group)
    last = chips - 1

    def remote(src, dst, send, recv, dev):
        return pltpu.make_async_remote_copy(src_ref=src, dst_ref=dst, send_sem=send, recv_sem=recv,
                                            device_id={"sp": dev}, device_id_type=MESH)

    def got(ref, sem):
        pltpu.make_async_copy(ref, ref, sem).wait()

    def w_copy(arr, col, slot):
        if not isinstance(col, int):
            col = pl.multiple_of(col, TILE)
        return pltpu.make_async_copy(arr.at[:, pl.ds(col, TILE)], wbuf.at[slot], w_sem.at[slot])

    x_copy = pltpu.make_async_copy(x_hbm, xb, x_sem)
    x_copy.start()
    w_copy(wk, 0, 0).start()

    barrier = pltpu.get_barrier_semaphore()
    for d in range(1, group):
        pl.semaphore_signal(barrier, inc=1, device_id={"sp": lax.rem(me + d, group)}, device_id_type=MESH)
    x_copy.wait()
    w_copy(wk, TILE, 1).start()

    sends_right = chip < last
    sends_left_k = chip == 0
    sends_left_v = chip < 2
    gets_left = chip > 0
    gets_right_k = chip == last
    fwd_k = (chip > 0) & (chip < last)
    gets_opp = chip >= 2

    def k_tile(p, carry):
        w_copy(wk, 0, p).wait()
        w_copy(wv, p * TILE, k_tiles + p).start()

        @pl.when(p == k_tiles - 1)
        def _():
            w_copy(wq, 0, kv_tiles).start()

        y = jnp.dot(xb[...], wbuf[p], preferred_element_type=jnp.float32).astype(jnp.bfloat16)
        for h in range(PER_TILE):
            kb[0, 0, p, h] = y[:, h * HEAD:(h + 1) * HEAD]

        @pl.when(p == 0)
        def _():
            pl.semaphore_wait(barrier, group - 1)

        src = kb.at[0, 0, p]

        @pl.when(sends_right)
        def _():
            remote(src, kb.at[3, 0, p], k_send.at[0], kr_l.at[p], right).start()

        @pl.when(sends_left_k)
        def _():
            remote(src, kb.at[1, 0, p], k_send.at[1], kr_r.at[p], left).start()

        @pl.when(core == 0)
        def _():
            remote(src, kb.at[0, 1, p], k_send.at[2], kr_p.at[0], partner).start()

        return carry

    lax.fori_loop(0, k_tiles, k_tile, 0)

    def v_tile(p, carry):
        w_copy(wv, 0, k_tiles + p).wait()
        w_copy(wq, (1 + p) * TILE, kv_tiles + 1 + p).start()
        y = jnp.dot(xb[...], wbuf[k_tiles + p], preferred_element_type=jnp.float32)
        for h in range(PER_TILE):
            vb[0, 0, p, h] = jnp.transpose(y[:, h * HEAD:(h + 1) * HEAD]).astype(jnp.bfloat16)
        src = vb.at[0, 0, p]

        @pl.when(sends_right)
        def _():
            remote(src, vb.at[3, 0, p], k_send.at[3], kr_l.at[k_tiles + p], right).start()

        @pl.when(sends_left_v)
        def _():
            remote(src, vb.at[1, 0, p], k_send.at[4], kr_r.at[k_tiles + p], left).start()

        @pl.when(core == 0)
        def _():
            remote(src, vb.at[0, 1, p], k_send.at[5], kr_p.at[4], partner).start()

        return carry

    lax.fori_loop(0, k_tiles, v_tile, 0)

    def q_tile(n, carry):
        slot = lax.rem(kv_tiles + n, SLOTS)
        w_copy(wq, 0, slot).wait()
        ahead = lax.rem(kv_tiles + AHEAD + n, SLOTS)

        @pl.when(n + AHEAD < q_tiles)
        def _():
            w_copy(wq, (n + AHEAD) * TILE, ahead).start()

        @pl.when(n + AHEAD >= q_tiles)
        def _():
            w_copy(wo, (n + AHEAD - q_tiles) * TILE, ahead).start()

        y = jnp.dot(xb[...], wbuf[slot], preferred_element_type=jnp.float32).astype(jnp.bfloat16)
        for h in range(PER_TILE):
            q_s[n, h] = y[:, h * HEAD:(h + 1) * HEAD]
        return carry

    lax.fori_loop(0, q_tiles, q_tile, 0)
    for n in range(AHEAD, o_tiles):
        w_copy(wo, n * TILE, (kv_tiles + q_tiles + n) % SLOTS).start()

    def k_partner(r, p):
        remote(kb.at[r, 0, p], kb.at[r, 1, p], k_send.at[5 + r], kr_p.at[r], partner).start()

    def v_partner(r, p):
        remote(vb.at[r, 0, p], vb.at[r, 1, p], k_send.at[8 + r], kr_p.at[4 + r], partner).start()

    @pl.when(gets_left)
    def _():
        for p in range(k_tiles):
            got(kb.at[3, 0, p], kr_l.at[p])

            @pl.when(fwd_k)
            def _():
                remote(kb.at[3, 0, p], kb.at[2, 0, p], k_send.at[12], kr_o.at[p], right).start()

            k_partner(3, p)

    expert = lax.broadcasted_iota(jnp.int32, (n_exp, tok), 0)
    hit0 = expert == ids_ref[0:1, :]
    hit1 = expert == ids_ref[1:2, :]
    probs = probs_ref[...]
    p0 = jnp.sum(jnp.where(hit0, probs, 0.0), axis=0, keepdims=True)
    p1 = jnp.sum(jnp.where(hit1, probs, 0.0), axis=0, keepdims=True)
    total = p0 + p1
    hits = hit0 | hit1
    before = (lax.broadcasted_iota(jnp.int32, (tok, tok), 0)
              < lax.broadcasted_iota(jnp.int32, (tok, tok), 1)).astype(jnp.float32).astype(jnp.bfloat16)
    earlier = jnp.dot(hits.astype(jnp.float32).astype(jnp.bfloat16), before, preferred_element_type=jnp.float32)
    meta_s[0:n_exp, :] = jnp.where(hits, earlier, -1.0)
    meta_s[n_exp:2 * n_exp, :] = jnp.where(hit0, p0 / total, jnp.where(hit1, p1 / total, 0.0))

    def attend(r, parts, lo=0, hi=None, first=False, diagonal=False):
        hi = q_tiles if hi is None else hi
        spare = q_tiles
        keys = parts * tok
        if diagonal:
            key_i = lax.broadcasted_iota(jnp.int32, (tok, tok), 0)
            row_i = lax.broadcasted_iota(jnp.int32, (tok, tok), 1)
            seen = row_i >= key_i

        def score(g, into, h, side):
            kp = lax.div(g, PER_TILE)
            kh = lax.rem(g, PER_TILE)
            q = q_s[g, h]
            top = None if first else top_s[g, h]
            old = top
            for o in range(parts):
                s = lax.dot_general(kb[r, o, kp, kh], q, (((1,), (1,)), ((), ())), preferred_element_type=jnp.float32)
                if diagonal and o == 0:
                    s = jnp.where(seen, s, -1e30)
                s_b[side, h, o] = s
                high = jnp.max(s, axis=0, keepdims=True)
                top = high if top is None else jnp.maximum(top, high)
            top_s[into, h] = top
            if not first:
                keep_s[into, h] = jnp.exp2((old - top) * EXP2_SCALE)

        def weigh(g, h, side):
            top = top_s[g, h]
            mass = None
            for o in range(parts):
                e = jnp.exp2((s_b[side, h, o] - top) * EXP2_SCALE)
                e_b[side, h, o * tok:(o + 1) * tok, :] = e.astype(jnp.bfloat16)
                part = jnp.sum(e, axis=0, keepdims=True)
                mass = part if mass is None else mass + part
            mass_s[g, h] = mass if first else mass + keep_s[g, h] * mass_s[g, h]

        def apply(g, into, h, side):
            kp = lax.div(g, PER_TILE)
            kh = lax.rem(g, PER_TILE)
            v = jnp.concatenate([vb[r, o, kp, kh] for o in range(parts)], axis=1)
            out = jnp.dot(v, e_b[side, h, 0:keys, :], preferred_element_type=jnp.float32)
            acc[into, h] = out if first else out + keep_s[into, h] * acc[into, h]

        def head_groups(i, carry):
            g = lo + 2 * i
            below = jnp.maximum(g - 1, lo)
            below_into = lax.select(g == lo, spare, g - 1)
            above = jnp.minimum(g + 2, hi - 1)
            above_into = lax.select(g == hi - 2, spare, g + 2)
            for h in range(PER_TILE):
                weigh(g, h, 0)
                score(g + 1, g + 1, h, 1)
                apply(below, below_into, h, 1)
            for h in range(PER_TILE):
                weigh(g + 1, h, 1)
                score(above, above_into, h, 0)
                apply(g, g, h, 0)
            return carry

        for h in range(PER_TILE):
            score(lo, lo, h, 0)
        lax.fori_loop(0, (hi - lo) // 2, head_groups, 0)
        for h in range(PER_TILE):
            apply(hi - 1, hi - 1, h, 1)

    for h in range(PER_TILE):
        e_b[1, h] = jnp.zeros((2 * tok, tok), jnp.bfloat16)
        acc[q_tiles, h] = jnp.zeros((HEAD, tok), jnp.float32)
        keep_s[q_tiles, h] = jnp.zeros((1, tok), jnp.float32)

    @pl.when(core == 0)
    def _():
        attend(0, 1, first=True, diagonal=True)

    @pl.when(core == 1)
    def _():
        got(kb.at[0, 1], kr_p.at[0])
        got(vb.at[0, 1], kr_p.at[4])
        attend(0, 2, first=True, diagonal=True)

    m_rows = meta_all.at[me]
    loc = pltpu.make_async_copy(meta_s, m_rows, m_loc)
    loc.start()
    for d in range(1, group):
        remote(meta_s, m_rows, m_send.at[d - 1], m_recv.at[d - 1], lax.rem(me + d, group)).start()

    def values_on_left():
        for p in range(k_tiles):
            got(vb.at[1, 0, p], kr_r.at[k_tiles + p])
            remote(vb.at[1, 0, p], vb.at[2, 0, p], k_send.at[13], kr_o.at[k_tiles + p], left).start()

    @pl.when(chip == last)
    def _():
        values_on_left()

    @pl.when(gets_left)
    def _():
        for p in range(k_tiles):
            got(vb.at[3, 0, p], kr_l.at[k_tiles + p])
            v_partner(3, p)

        @pl.when(gets_right_k)
        def _():
            for p in range(k_tiles):
                got(kb.at[1, 0, p], kr_r.at[p])
                k_partner(1, p)
                v_partner(1, p)

        got(kb.at[3, 1], kr_p.at[3])
        got(vb.at[3, 1], kr_p.at[7])
        attend(3, 2)

    def take_opp():
        for p in range(k_tiles):
            got(kb.at[2, 0, p], kr_o.at[p])
            k_partner(2, p)
            got(vb.at[2, 0, p], kr_o.at[k_tiles + p])
            v_partner(2, p)

    @pl.when(gets_right_k)
    def _():
        got(kb.at[1, 1], kr_p.at[1])
        got(vb.at[1, 1], kr_p.at[5])
        attend(1, 2, hi=q_tiles - 2)
        take_opp()
        attend(1, 2, lo=q_tiles - 2)

    @pl.when(gets_opp)
    def _():
        @pl.when(jnp.logical_not(gets_right_k))
        def _():
            take_opp()

        got(kb.at[2, 1], kr_p.at[2])
        got(vb.at[2, 1], kr_p.at[6])
        attend(2, 2)

    def finish(g, carry):
        for h in range(PER_TILE):
            o = jnp.transpose(acc[g, h] * (1.0 / mass_s[g, h]))
            o_s[:, pl.ds(pl.multiple_of(g * TILE + h * HEAD, HEAD), HEAD)] = o.astype(jnp.bfloat16)
        return carry

    lax.fori_loop(0, q_tiles, finish, 0)

    @pl.when(chip == 0)
    def _():
        got(kb.at[0, 0], k_send.at[1])
        got(vb.at[0, 0], k_send.at[4])
        values_on_left()

    def rows_of(dev):
        return pl.ds(pl.multiple_of(dev * tok, tok), tok)

    def piece(dev, n):
        col = n * TILE
        if not isinstance(col, int):
            col = pl.multiple_of(col, TILE)
        return h_all.at[rows_of(dev), pl.ds(col, TILE)]

    def to_left(n):
        remote(h_s.at[n], piece(me, n), h_send.at[1], hr_r.at[n], left).start()

    def o_tile(n, carry):
        slot = lax.rem(kv_tiles + q_tiles + n, SLOTS)
        w_copy(wo, 0, slot).wait()
        y = jnp.dot(o_s[...], wbuf[slot], preferred_element_type=jnp.float32)
        x = xb[:, pl.ds(pl.multiple_of(n * TILE, TILE), TILE)].astype(jnp.float32)
        h_s[n] = (x + y).astype(jnp.bfloat16)
        remote(h_s.at[n], piece(me, n), h_send.at[0], hr_l.at[n], right).start()

        @pl.when(chip > 0)
        def _():
            to_left(n)

        remote(h_s.at[n], piece(me, n), h_send.at[2], hr_p.at[0], partner).start()
        pltpu.make_async_copy(h_s.at[n], piece(me, n), x_sem).start()
        return carry

    lax.fori_loop(0, o_tiles, o_tile, 0)

    @pl.when(chip == 0)
    def _():
        got(vb.at[0, 0], k_send.at[13])
        for n in range(o_tiles):
            to_left(n)


    def of_chips(which):
        hit = jnp.bool_(False)
        for c in which:
            hit = hit | (chip == c)
        return hit

    halves = 2 * o_tiles
    on_right = [[m in VIA_NEXT[(c - 1) % chips] for m in range(halves)] for c in range(chips)]
    on_left = [[m not in VIA_NEXT[(c + 1) % chips] for m in range(halves)] for c in range(chips)]

    def half_piece(dev, m):
        return h_all.at[rows_of(dev), pl.ds(m * (TILE // 2), TILE // 2)]

    def from_left(n):
        got(piece(left, n), hr_l.at[n])
        for m in (2 * n, 2 * n + 1):
            @pl.when(of_chips([c for c in range(chips) if on_right[c][m]]))
            def _(m=m):
                remote(half_piece(left, m), half_piece(left, m), h_send.at[6], hr_o.at[m], right).start()

        remote(piece(left, n), piece(left, n), h_send.at[5], hr_p.at[3], partner).start()

    def from_right(n):
        got(piece(right, n), hr_r.at[n])
        for m in (2 * n, 2 * n + 1):
            @pl.when(of_chips([c for c in range(chips) if on_left[c][m]]))
            def _(m=m):
                remote(half_piece(right, m), half_piece(right, m), h_send.at[7], hr_o.at[m], left).start()

        remote(piece(right, n), piece(right, n), h_send.at[3], hr_p.at[1], partner).start()

    def in_turn(early, late):
        for n in range(o_tiles + LAG):
            if n < o_tiles:
                early(n)
            if n >= LAG:
                late(n - LAG)

    early_right = (chip == 0) | (chip == last)

    @pl.when(early_right)
    def _():
        in_turn(from_right, from_left)

    @pl.when(jnp.logical_not(early_right))
    def _():
        in_turn(from_left, from_right)

    for n in range(halves):
        got(half_piece(opp, n), hr_o.at[n])
        remote(half_piece(opp, n), half_piece(opp, n), h_send.at[4], hr_p.at[2], partner).start()

    mine = h_all.at[rows_of(me)]
    got(mine, x_sem)
    for i in range(6):
        got(mine, h_send.at[i])
    for c in range(chips):
        @pl.when(chip == c)
        def _():
            for i, on in ((6, on_right[c]), (7, on_left[c])):
                if sum(on):
                    got(h_all.at[rows_of(me), pl.ds(0, sum(on) * (TILE // 2))], h_send.at[i])
    for r in range(chips):
        got(h_all.at[rows_of(lax.rem(partner + 2 * r, group))], hr_p.at[r])
    k_own = kb.at[0, 0]
    v_own = vb.at[0, 0]
    for when, waits in ((sends_right, ((k_own, 0), (v_own, 3))), (chip == 1, ((v_own, 4),)),
                        (core == 0, ((k_own, 2), (v_own, 5))), (gets_left, ((k_own, 8), (v_own, 11))),
                        (gets_right_k, ((k_own, 6), (v_own, 9))), (gets_opp, ((k_own, 7), (v_own, 10))),
                        (fwd_k, ((k_own, 12),)), (chip == last, ((v_own, 13),))):
        @pl.when(when)
        def _(waits=waits):
            for ref, i in waits:
                got(ref, k_send.at[i])

    loc.wait()
    for d in range(1, group):
        got(meta_s, m_send.at[d - 1])
        got(meta_all.at[lax.rem(me + group - d, group)], m_recv.at[d - 1])


def dispatch_kernel(n_exp, own_exp, meta_ref, h_hbm, hid_hbm, buf_hbm, hb, ob, h_sem, o_sem, hid_sem):
    group, tok, width = hb.shape
    slots = ob.shape[0]
    me = lax.axis_index("sp")
    row = lax.broadcasted_iota(jnp.int32, (tok, tok), 0).astype(jnp.float32)

    def o_copy(s):
        rows = pl.ds(s * tok if isinstance(s, int) else pl.multiple_of(s * tok, tok), tok)
        return pltpu.make_async_copy(ob.at[lax.rem(s, slots)], buf_hbm.at[:, rows], o_sem.at[lax.rem(s, slots)])

    for s in range(group):
        pltpu.make_async_copy(h_hbm.at[pl.ds(s * tok, tok)], hb.at[s], h_sem.at[s]).start()

    def source(s, carry):
        pltpu.make_async_copy(hb.at[s], hb.at[s], h_sem.at[s]).wait()

        @pl.when(s == me)
        def _():
            pltpu.make_async_copy(hb.at[s], hid_hbm, hid_sem).start()

        @pl.when(s >= slots)
        def _():
            o_copy(s - slots).wait()

        picks, gates = [], []
        for e in range(own_exp):
            expert = me * own_exp + e
            pick = row == meta_ref[s, pl.ds(expert, 1), :]
            gates.append(jnp.sum(jnp.where(pick, meta_ref[s, pl.ds(n_exp + expert, 1), :], 0.0), axis=1, keepdims=True))
            picks.append(pick.astype(jnp.float32).astype(jnp.bfloat16))
        o = lax.rem(s, slots)
        for c in range(0, width, COLS):
            for e in range(own_exp):
                rows = jnp.dot(picks[e], hb[s, :, c:c + COLS], preferred_element_type=jnp.float32)
                ob[o, e, :, c:c + COLS] = (rows * gates[e]).astype(jnp.bfloat16)
        o_copy(s).start()
        return carry

    lax.fori_loop(0, group, source, 0)
    for s in range(group - slots, group):
        o_copy(s).wait()
    pltpu.make_async_copy(hb.at[0], hid_hbm, hid_sem).wait()


def solution(mesh):
    group = mesh.shape['sp']
    row_spec = P(('dp', 'sp'), None)
    buf_spec = P(('dp', 'sp'), None, None)

    def device_step(x_loc, w_q, w_k, w_v, w_o, ids_loc, probs_loc):
        tok, width = x_loc.shape
        n_exp = probs_loc.shape[1]
        own_exp = n_exp // group
        seq = tok * group
        q_tiles = w_q.shape[1] // TILE
        k_tiles = w_k.shape[1] // TILE
        chips = group // 2
        o_tiles = width // TILE
        bf16 = jnp.bfloat16
        any_spec = pl.BlockSpec(memory_space=pl.ANY)
        vmem_spec = pl.BlockSpec(memory_space=pltpu.VMEM)
        dma = pltpu.SemaphoreType.DMA
        h_all, meta_all = pl.pallas_call(
            functools.partial(block_kernel, group, n_exp),
            out_shape=(jax.ShapeDtypeStruct((seq, width), bf16),
                       jax.ShapeDtypeStruct((group, 2 * n_exp, tok), jnp.float32)),
            in_specs=[any_spec] * 5 + [vmem_spec] * 2,
            out_specs=(any_spec, any_spec),
            scratch_shapes=[
                pltpu.VMEM((tok, width), bf16),
                pltpu.VMEM((SLOTS, width, TILE), bf16),
                pltpu.VMEM((chips, 2, k_tiles, PER_TILE, tok, HEAD), bf16),
                pltpu.VMEM((chips, 2, k_tiles, PER_TILE, HEAD, tok), bf16),
                pltpu.VMEM((q_tiles, PER_TILE, tok, HEAD), bf16),
                pltpu.VMEM((q_tiles + 1, PER_TILE, HEAD, tok), jnp.float32),
                pltpu.VMEM((q_tiles + 1, PER_TILE, 1, tok), jnp.float32),
                pltpu.VMEM((q_tiles + 1, PER_TILE, 1, tok), jnp.float32),
                pltpu.VMEM((q_tiles + 1, PER_TILE, 1, tok), jnp.float32),
                pltpu.VMEM((2, PER_TILE, 2, tok, tok), jnp.float32),
                pltpu.VMEM((2, PER_TILE, 2 * tok, tok), bf16),
                pltpu.VMEM((tok, q_tiles * TILE), bf16),
                pltpu.VMEM((o_tiles, tok, TILE), bf16),
                pltpu.VMEM((2 * n_exp, tok), jnp.float32),
                dma, dma((SLOTS,)),
                dma((14,)), dma((2 * k_tiles,)), dma((2 * k_tiles,)), dma((2 * k_tiles,)), dma((2 * chips,)),
                dma((8,)), dma((o_tiles,)), dma((o_tiles,)), dma((2 * o_tiles,)), dma((chips,)),
                dma((group - 1,)), dma((group - 1,)), dma,
            ],
            compiler_params=pltpu.CompilerParams(collective_id=0, has_side_effects=True,
                                                 vmem_limit_bytes=VMEM_LIMIT),
            name="block",
        )(x_loc, w_q, w_k, w_v, w_o, ids_loc.T, probs_loc.T)

        hidden_out, buf = pl.pallas_call(
            functools.partial(dispatch_kernel, n_exp, own_exp),
            out_shape=(jax.ShapeDtypeStruct((tok, width), bf16),
                       jax.ShapeDtypeStruct((own_exp, seq, width), bf16)),
            in_specs=[vmem_spec, any_spec],
            out_specs=(any_spec, any_spec),
            scratch_shapes=[pltpu.VMEM((group, tok, width), bf16), pltpu.VMEM((OUT_SLOTS, own_exp, tok, width), bf16),
                            dma((group,)), dma((OUT_SLOTS,)), dma],
            compiler_params=pltpu.CompilerParams(vmem_limit_bytes=VMEM_LIMIT),
            name="dispatch",
        )(meta_all, h_all)
        return hidden_out, buf

    return jax.shard_map(device_step, mesh=mesh,
                         in_specs=(row_spec, P(), P(), P(), P(), row_spec, row_spec),
                         out_specs=(row_spec, buf_spec), check_vma=False)
```

```python
import functools
import math

import jax
import jax.numpy as jnp
from jax import lax
from jax.experimental import pallas as pl
from jax.experimental.pallas import tpu as pltpu
from jax.sharding import PartitionSpec as P

HEAD = 128
EXP2_SCALE = math.log2(math.e) / math.sqrt(HEAD)
MESH = pl.DeviceIdType.MESH
TILE = 512
SLOTS = 8
PER_TILE = TILE // HEAD
AHEAD = 3
VMEM_LIMIT = 67_000_000
VIA_NEXT = ((0, 1, 3, 4, 6, 7, 9, 10, 12, 13, 15), (0, 3, 6, 9, 12, 15), (2, 5, 8, 11, 14), (0, 1, 2, 4, 5, 6, 8, 9, 10, 12, 13, 14))
LAG = 3
OUT_SLOTS = 5
COLS = 512


def block_kernel(group, n_exp, x_hbm, wq, wk, wv, wo, ids_ref, probs_ref, h_all, meta_all,
                 xb, wbuf, kb, vb, q_s, acc, top_s, mass_s, keep_s, s_b, e_b, o_s, h_s, meta_s,
                 x_sem, w_sem, k_send, kr_l, kr_r, kr_o, kr_p, h_send, hr_l, hr_r, hr_o, hr_p, m_send, m_recv, m_loc):
    tok = xb.shape[0]
    chips = group // 2
    q_tiles = wq.shape[1] // TILE
    k_tiles = wk.shape[1] // TILE
    kv_tiles = 2 * k_tiles
    o_tiles = wo.shape[1] // TILE
    me = lax.axis_index("sp")
    core = lax.rem(me, 2)
    chip = lax.div(me, 2)
    right = lax.rem(me + 2, group)
    left = lax.rem(me + group - 2, group)
    partner = me + 1 - 2 * core
    opp = lax.rem(me + 4, group)
    last = chips - 1

    def remote(src, dst, send, recv, dev):
        return pltpu.make_async_remote_copy(src_ref=src, dst_ref=dst, send_sem=send, recv_sem=recv,
                                            device_id={"sp": dev}, device_id_type=MESH)

    def got(ref, sem):
        pltpu.make_async_copy(ref, ref, sem).wait()

    def w_copy(arr, col, slot):
        if not isinstance(col, int):
            col = pl.multiple_of(col, TILE)
        return pltpu.make_async_copy(arr.at[:, pl.ds(col, TILE)], wbuf.at[slot], w_sem.at[slot])

    x_copy = pltpu.make_async_copy(x_hbm, xb, x_sem)
    x_copy.start()
    w_copy(wk, 0, 0).start()

    barrier = pltpu.get_barrier_semaphore()
    for d in range(1, group):
        pl.semaphore_signal(barrier, inc=1, device_id={"sp": lax.rem(me + d, group)}, device_id_type=MESH)
    x_copy.wait()
    w_copy(wk, TILE, 1).start()

    sends_right = chip < last
    sends_left_k = chip == 0
    sends_left_v = chip < 2
    gets_left = chip > 0
    gets_right_k = chip == last
    fwd_k = (chip > 0) & (chip < last)
    gets_opp = chip >= 2

    def k_tile(p, carry):
        w_copy(wk, 0, p).wait()
        w_copy(wv, p * TILE, k_tiles + p).start()

        @pl.when(p == k_tiles - 1)
        def _():
            w_copy(wq, 0, kv_tiles).start()

        y = jnp.dot(xb[...], wbuf[p], preferred_element_type=jnp.float32).astype(jnp.bfloat16)
        for h in range(PER_TILE):
            kb[0, 0, p, h] = y[:, h * HEAD:(h + 1) * HEAD]

        @pl.when(p == 0)
        def _():
            pl.semaphore_wait(barrier, group - 1)

        src = kb.at[0, 0, p]

        @pl.when(sends_right)
        def _():
            remote(src, kb.at[3, 0, p], k_send.at[0], kr_l.at[p], right).start()

        @pl.when(sends_left_k)
        def _():
            remote(src, kb.at[1, 0, p], k_send.at[1], kr_r.at[p], left).start()

        @pl.when(core == 0)
        def _():
            remote(src, kb.at[0, 1, p], k_send.at[2], kr_p.at[0], partner).start()

        return carry

    lax.fori_loop(0, k_tiles, k_tile, 0)

    def v_tile(p, carry):
        w_copy(wv, 0, k_tiles + p).wait()
        w_copy(wq, (1 + p) * TILE, kv_tiles + 1 + p).start()
        y = jnp.dot(xb[...], wbuf[k_tiles + p], preferred_element_type=jnp.float32)
        for h in range(PER_TILE):
            vb[0, 0, p, h] = jnp.transpose(y[:, h * HEAD:(h + 1) * HEAD]).astype(jnp.bfloat16)
        src = vb.at[0, 0, p]

        @pl.when(sends_right)
        def _():
            remote(src, vb.at[3, 0, p], k_send.at[3], kr_l.at[k_tiles + p], right).start()

        @pl.when(sends_left_v)
        def _():
            remote(src, vb.at[1, 0, p], k_send.at[4], kr_r.at[k_tiles + p], left).start()

        @pl.when(core == 0)
        def _():
            remote(src, vb.at[0, 1, p], k_send.at[5], kr_p.at[4], partner).start()

        return carry

    lax.fori_loop(0, k_tiles, v_tile, 0)

    def q_tile(n, carry):
        slot = lax.rem(kv_tiles + n, SLOTS)
        w_copy(wq, 0, slot).wait()
        ahead = lax.rem(kv_tiles + AHEAD + n, SLOTS)

        @pl.when(n + AHEAD < q_tiles)
        def _():
            w_copy(wq, (n + AHEAD) * TILE, ahead).start()

        @pl.when(n + AHEAD >= q_tiles)
        def _():
            w_copy(wo, (n + AHEAD - q_tiles) * TILE, ahead).start()

        y = jnp.dot(xb[...], wbuf[slot], preferred_element_type=jnp.float32).astype(jnp.bfloat16)
        for h in range(PER_TILE):
            q_s[n, h] = y[:, h * HEAD:(h + 1) * HEAD]
        return carry

    lax.fori_loop(0, q_tiles, q_tile, 0)
    for n in range(AHEAD, o_tiles):
        w_copy(wo, n * TILE, (kv_tiles + q_tiles + n) % SLOTS).start()

    def k_partner(r, p):
        remote(kb.at[r, 0, p], kb.at[r, 1, p], k_send.at[5 + r], kr_p.at[r], partner).start()

    def v_partner(r, p):
        remote(vb.at[r, 0, p], vb.at[r, 1, p], k_send.at[8 + r], kr_p.at[4 + r], partner).start()

    @pl.when(gets_left)
    def _():
        for p in range(k_tiles):
            got(kb.at[3, 0, p], kr_l.at[p])

            @pl.when(fwd_k)
            def _():
                remote(kb.at[3, 0, p], kb.at[2, 0, p], k_send.at[12], kr_o.at[p], right).start()

            k_partner(3, p)

    expert = lax.broadcasted_iota(jnp.int32, (n_exp, tok), 0)
    hit0 = expert == ids_ref[0:1, :]
    hit1 = expert == ids_ref[1:2, :]
    probs = probs_ref[...]
    p0 = jnp.sum(jnp.where(hit0, probs, 0.0), axis=0, keepdims=True)
    p1 = jnp.sum(jnp.where(hit1, probs, 0.0), axis=0, keepdims=True)
    total = p0 + p1
    hits = hit0 | hit1
    before = (lax.broadcasted_iota(jnp.int32, (tok, tok), 0)
              < lax.broadcasted_iota(jnp.int32, (tok, tok), 1)).astype(jnp.float32).astype(jnp.bfloat16)
    earlier = jnp.dot(hits.astype(jnp.float32).astype(jnp.bfloat16), before, preferred_element_type=jnp.float32)
    meta_s[0:n_exp, :] = jnp.where(hits, earlier, -1.0)
    meta_s[n_exp:2 * n_exp, :] = jnp.where(hit0, p0 / total, jnp.where(hit1, p1 / total, 0.0))

    def attend(r, parts, lo=0, hi=None, first=False, diagonal=False):
        hi = q_tiles if hi is None else hi
        spare = q_tiles
        keys = parts * tok
        if diagonal:
            key_i = lax.broadcasted_iota(jnp.int32, (tok, tok), 0)
            row_i = lax.broadcasted_iota(jnp.int32, (tok, tok), 1)
            seen = row_i >= key_i

        def score(g, into, h, side):
            kp = lax.div(g, PER_TILE)
            kh = lax.rem(g, PER_TILE)
            q = q_s[g, h]
            top = None if first else top_s[g, h]
            old = top
            for o in range(parts):
                s = lax.dot_general(kb[r, o, kp, kh], q, (((1,), (1,)), ((), ())), preferred_element_type=jnp.float32)
                if diagonal and o == 0:
                    s = jnp.where(seen, s, -1e30)
                s_b[side, h, o] = s
                high = jnp.max(s, axis=0, keepdims=True)
                top = high if top is None else jnp.maximum(top, high)
            top_s[into, h] = top
            if not first:
                keep_s[into, h] = jnp.exp2((old - top) * EXP2_SCALE)

        def weigh(g, h, side):
            top = top_s[g, h]
            mass = None
            for o in range(parts):
                e = jnp.exp2((s_b[side, h, o] - top) * EXP2_SCALE)
                e_b[side, h, o * tok:(o + 1) * tok, :] = e.astype(jnp.bfloat16)
                part = jnp.sum(e, axis=0, keepdims=True)
                mass = part if mass is None else mass + part
            mass_s[g, h] = mass if first else mass + keep_s[g, h] * mass_s[g, h]

        def apply(g, into, h, side):
            kp = lax.div(g, PER_TILE)
            kh = lax.rem(g, PER_TILE)
            v = jnp.concatenate([vb[r, o, kp, kh] for o in range(parts)], axis=1)
            out = jnp.dot(v, e_b[side, h, 0:keys, :], preferred_element_type=jnp.float32)
            acc[into, h] = out if first else out + keep_s[into, h] * acc[into, h]

        def head_groups(i, carry):
            g = lo + 2 * i
            below = jnp.maximum(g - 1, lo)
            below_into = lax.select(g == lo, spare, g - 1)
            above = jnp.minimum(g + 2, hi - 1)
            above_into = lax.select(g == hi - 2, spare, g + 2)
            for h in range(PER_TILE):
                weigh(g, h, 0)
                score(g + 1, g + 1, h, 1)
                apply(below, below_into, h, 1)
            for h in range(PER_TILE):
                weigh(g + 1, h, 1)
                score(above, above_into, h, 0)
                apply(g, g, h, 0)
            return carry

        for h in range(PER_TILE):
            score(lo, lo, h, 0)
        lax.fori_loop(0, (hi - lo) // 2, head_groups, 0)
        for h in range(PER_TILE):
            apply(hi - 1, hi - 1, h, 1)

    for h in range(PER_TILE):
        e_b[1, h] = jnp.zeros((2 * tok, tok), jnp.bfloat16)
        acc[q_tiles, h] = jnp.zeros((HEAD, tok), jnp.float32)
        keep_s[q_tiles, h] = jnp.zeros((1, tok), jnp.float32)

    @pl.when(core == 0)
    def _():
        attend(0, 1, first=True, diagonal=True)

    @pl.when(core == 1)
    def _():
        got(kb.at[0, 1], kr_p.at[0])
        got(vb.at[0, 1], kr_p.at[4])
        attend(0, 2, first=True, diagonal=True)

    m_rows = meta_all.at[me]
    loc = pltpu.make_async_copy(meta_s, m_rows, m_loc)
    loc.start()
    for d in range(1, group):
        remote(meta_s, m_rows, m_send.at[d - 1], m_recv.at[d - 1], lax.rem(me + d, group)).start()

    def values_on_left():
        for p in range(k_tiles):
            got(vb.at[1, 0, p], kr_r.at[k_tiles + p])
            remote(vb.at[1, 0, p], vb.at[2, 0, p], k_send.at[13], kr_o.at[k_tiles + p], left).start()

    @pl.when(chip == last)
    def _():
        values_on_left()

    @pl.when(gets_left)
    def _():
        for p in range(k_tiles):
            got(vb.at[3, 0, p], kr_l.at[k_tiles + p])
            v_partner(3, p)

        @pl.when(gets_right_k)
        def _():
            for p in range(k_tiles):
                got(kb.at[1, 0, p], kr_r.at[p])
                k_partner(1, p)
                v_partner(1, p)

        got(kb.at[3, 1], kr_p.at[3])
        got(vb.at[3, 1], kr_p.at[7])
        attend(3, 2)

    def take_opp():
        for p in range(k_tiles):
            got(kb.at[2, 0, p], kr_o.at[p])
            k_partner(2, p)
            got(vb.at[2, 0, p], kr_o.at[k_tiles + p])
            v_partner(2, p)

    @pl.when(gets_right_k)
    def _():
        got(kb.at[1, 1], kr_p.at[1])
        got(vb.at[1, 1], kr_p.at[5])
        attend(1, 2, hi=q_tiles - 2)
        take_opp()
        attend(1, 2, lo=q_tiles - 2)

    @pl.when(gets_opp)
    def _():
        @pl.when(jnp.logical_not(gets_right_k))
        def _():
            take_opp()

        got(kb.at[2, 1], kr_p.at[2])
        got(vb.at[2, 1], kr_p.at[6])
        attend(2, 2)

    def finish(g, carry):
        for h in range(PER_TILE):
            o = jnp.transpose(acc[g, h] * (1.0 / mass_s[g, h]))
            o_s[:, pl.ds(pl.multiple_of(g * TILE + h * HEAD, HEAD), HEAD)] = o.astype(jnp.bfloat16)
        return carry

    lax.fori_loop(0, q_tiles, finish, 0)

    @pl.when(chip == 0)
    def _():
        got(kb.at[0, 0], k_send.at[1])
        got(vb.at[0, 0], k_send.at[4])
        values_on_left()

    def rows_of(dev):
        return pl.ds(pl.multiple_of(dev * tok, tok), tok)

    def piece(dev, n):
        col = n * TILE
        if not isinstance(col, int):
            col = pl.multiple_of(col, TILE)
        return h_all.at[rows_of(dev), pl.ds(col, TILE)]

    def to_left(n):
        remote(h_s.at[n], piece(me, n), h_send.at[1], hr_r.at[n], left).start()

    def o_tile(n, carry):
        slot = lax.rem(kv_tiles + q_tiles + n, SLOTS)
        w_copy(wo, 0, slot).wait()
        y = jnp.dot(o_s[...], wbuf[slot], preferred_element_type=jnp.float32)
        x = xb[:, pl.ds(pl.multiple_of(n * TILE, TILE), TILE)].astype(jnp.float32)
        h_s[n] = (x + y).astype(jnp.bfloat16)
        remote(h_s.at[n], piece(me, n), h_send.at[0], hr_l.at[n], right).start()

        @pl.when(chip > 0)
        def _():
            to_left(n)

        remote(h_s.at[n], piece(me, n), h_send.at[2], hr_p.at[0], partner).start()
        pltpu.make_async_copy(h_s.at[n], piece(me, n), x_sem).start()
        return carry

    lax.fori_loop(0, o_tiles, o_tile, 0)

    @pl.when(chip == 0)
    def _():
        got(vb.at[0, 0], k_send.at[13])
        for n in range(o_tiles):
            to_left(n)


    def of_chips(which):
        hit = jnp.bool_(False)
        for c in which:
            hit = hit | (chip == c)
        return hit

    halves = 2 * o_tiles
    on_right = [[m in VIA_NEXT[(c - 1) % chips] for m in range(halves)] for c in range(chips)]
    on_left = [[m not in VIA_NEXT[(c + 1) % chips] for m in range(halves)] for c in range(chips)]

    def half_piece(dev, m):
        return h_all.at[rows_of(dev), pl.ds(m * (TILE // 2), TILE // 2)]

    def from_left(n):
        got(piece(left, n), hr_l.at[n])
        for m in (2 * n, 2 * n + 1):
            @pl.when(of_chips([c for c in range(chips) if on_right[c][m]]))
            def _(m=m):
                remote(half_piece(left, m), half_piece(left, m), h_send.at[6], hr_o.at[m], right).start()

        remote(piece(left, n), piece(left, n), h_send.at[5], hr_p.at[3], partner).start()

    def from_right(n):
        got(piece(right, n), hr_r.at[n])
        for m in (2 * n, 2 * n + 1):
            @pl.when(of_chips([c for c in range(chips) if on_left[c][m]]))
            def _(m=m):
                remote(half_piece(right, m), half_piece(right, m), h_send.at[7], hr_o.at[m], left).start()

        remote(piece(right, n), piece(right, n), h_send.at[3], hr_p.at[1], partner).start()

    def in_turn(early, late):
        for n in range(o_tiles + LAG):
            if n < o_tiles:
                early(n)
            if n >= LAG:
                late(n - LAG)

    early_right = (chip == 0) | (chip == last)

    @pl.when(early_right)
    def _():
        in_turn(from_right, from_left)

    @pl.when(jnp.logical_not(early_right))
    def _():
        in_turn(from_left, from_right)

    for n in range(halves):
        got(half_piece(opp, n), hr_o.at[n])
        remote(half_piece(opp, n), half_piece(opp, n), h_send.at[4], hr_p.at[2], partner).start()

    mine = h_all.at[rows_of(me)]
    got(mine, x_sem)
    for i in range(6):
        got(mine, h_send.at[i])
    for c in range(chips):
        @pl.when(chip == c)
        def _():
            for i, on in ((6, on_right[c]), (7, on_left[c])):
                if sum(on):
                    got(h_all.at[rows_of(me), pl.ds(0, sum(on) * (TILE // 2))], h_send.at[i])
    for r in range(chips):
        got(h_all.at[rows_of(lax.rem(partner + 2 * r, group))], hr_p.at[r])
    k_own = kb.at[0, 0]
    v_own = vb.at[0, 0]
    for when, waits in ((sends_right, ((k_own, 0), (v_own, 3))), (chip == 1, ((v_own, 4),)),
                        (core == 0, ((k_own, 2), (v_own, 5))), (gets_left, ((k_own, 8), (v_own, 11))),
                        (gets_right_k, ((k_own, 6), (v_own, 9))), (gets_opp, ((k_own, 7), (v_own, 10))),
                        (fwd_k, ((k_own, 12),)), (chip == last, ((v_own, 13),))):
        @pl.when(when)
        def _(waits=waits):
            for ref, i in waits:
                got(ref, k_send.at[i])

    loc.wait()
    for d in range(1, group):
        got(meta_s, m_send.at[d - 1])
        got(meta_all.at[lax.rem(me + group - d, group)], m_recv.at[d - 1])


def dispatch_kernel(n_exp, own_exp, meta_ref, h_hbm, hid_hbm, buf_hbm, hb, ob, h_sem, o_sem, hid_sem):
    group, tok, width = hb.shape
    slots = ob.shape[0]
    me = lax.axis_index("sp")
    row = lax.broadcasted_iota(jnp.int32, (tok, tok), 0).astype(jnp.float32)

    def o_copy(s):
        rows = pl.ds(s * tok if isinstance(s, int) else pl.multiple_of(s * tok, tok), tok)
        return pltpu.make_async_copy(ob.at[lax.rem(s, slots)], buf_hbm.at[:, rows], o_sem.at[lax.rem(s, slots)])

    def read(sources):
        for s in sources:
            pltpu.make_async_copy(h_hbm.at[pl.ds(s * tok, tok)], hb.at[s], h_sem.at[s]).start()

    read(range(2))

    def source(s, carry):
        pltpu.make_async_copy(hb.at[s], hb.at[s], h_sem.at[s]).wait()

        @pl.when(s == 0)
        def _():
            read(range(2, 5))

        @pl.when(s == 1)
        def _():
            read(range(5, group))

        @pl.when(s == me)
        def _():
            pltpu.make_async_copy(hb.at[s], hid_hbm, hid_sem).start()

        @pl.when(s >= slots)
        def _():
            o_copy(s - slots).wait()

        picks, gates = [], []
        for e in range(own_exp):
            expert = me * own_exp + e
            pick = row == meta_ref[s, pl.ds(expert, 1), :]
            gates.append(jnp.sum(jnp.where(pick, meta_ref[s, pl.ds(n_exp + expert, 1), :], 0.0), axis=1, keepdims=True))
            picks.append(pick.astype(jnp.float32).astype(jnp.bfloat16))
        o = lax.rem(s, slots)
        for c in range(0, width, COLS):
            for e in range(own_exp):
                rows = jnp.dot(picks[e], hb[s, :, c:c + COLS], preferred_element_type=jnp.float32)
                ob[o, e, :, c:c + COLS] = (rows * gates[e]).astype(jnp.bfloat16)
        o_copy(s).start()
        return carry

    lax.fori_loop(0, group, source, 0)
    for s in range(group - slots, group):
        o_copy(s).wait()
    pltpu.make_async_copy(hb.at[0], hid_hbm, hid_sem).wait()


def solution(mesh):
    group = mesh.shape['sp']
    row_spec = P(('dp', 'sp'), None)
    buf_spec = P(('dp', 'sp'), None, None)

    def device_step(x_loc, w_q, w_k, w_v, w_o, ids_loc, probs_loc):
        tok, width = x_loc.shape
        n_exp = probs_loc.shape[1]
        own_exp = n_exp // group
        seq = tok * group
        q_tiles = w_q.shape[1] // TILE
        k_tiles = w_k.shape[1] // TILE
        chips = group // 2
        o_tiles = width // TILE
        bf16 = jnp.bfloat16
        any_spec = pl.BlockSpec(memory_space=pl.ANY)
        vmem_spec = pl.BlockSpec(memory_space=pltpu.VMEM)
        dma = pltpu.SemaphoreType.DMA
        h_all, meta_all = pl.pallas_call(
            functools.partial(block_kernel, group, n_exp),
            out_shape=(jax.ShapeDtypeStruct((seq, width), bf16),
                       jax.ShapeDtypeStruct((group, 2 * n_exp, tok), jnp.float32)),
            in_specs=[any_spec] * 5 + [vmem_spec] * 2,
            out_specs=(any_spec, any_spec),
            scratch_shapes=[
                pltpu.VMEM((tok, width), bf16),
                pltpu.VMEM((SLOTS, width, TILE), bf16),
                pltpu.VMEM((chips, 2, k_tiles, PER_TILE, tok, HEAD), bf16),
                pltpu.VMEM((chips, 2, k_tiles, PER_TILE, HEAD, tok), bf16),
                pltpu.VMEM((q_tiles, PER_TILE, tok, HEAD), bf16),
                pltpu.VMEM((q_tiles + 1, PER_TILE, HEAD, tok), jnp.float32),
                pltpu.VMEM((q_tiles + 1, PER_TILE, 1, tok), jnp.float32),
                pltpu.VMEM((q_tiles + 1, PER_TILE, 1, tok), jnp.float32),
                pltpu.VMEM((q_tiles + 1, PER_TILE, 1, tok), jnp.float32),
                pltpu.VMEM((2, PER_TILE, 2, tok, tok), jnp.float32),
                pltpu.VMEM((2, PER_TILE, 2 * tok, tok), bf16),
                pltpu.VMEM((tok, q_tiles * TILE), bf16),
                pltpu.VMEM((o_tiles, tok, TILE), bf16),
                pltpu.VMEM((2 * n_exp, tok), jnp.float32),
                dma, dma((SLOTS,)),
                dma((14,)), dma((2 * k_tiles,)), dma((2 * k_tiles,)), dma((2 * k_tiles,)), dma((2 * chips,)),
                dma((8,)), dma((o_tiles,)), dma((o_tiles,)), dma((2 * o_tiles,)), dma((chips,)),
                dma((group - 1,)), dma((group - 1,)), dma,
            ],
            compiler_params=pltpu.CompilerParams(collective_id=0, has_side_effects=True,
                                                 vmem_limit_bytes=VMEM_LIMIT),
            name="block",
        )(x_loc, w_q, w_k, w_v, w_o, ids_loc.T, probs_loc.T)

        hidden_out, buf = pl.pallas_call(
            functools.partial(dispatch_kernel, n_exp, own_exp),
            out_shape=(jax.ShapeDtypeStruct((tok, width), bf16),
                       jax.ShapeDtypeStruct((own_exp, seq, width), bf16)),
            in_specs=[vmem_spec, any_spec],
            out_specs=(any_spec, any_spec),
            scratch_shapes=[pltpu.VMEM((group, tok, width), bf16), pltpu.VMEM((OUT_SLOTS, own_exp, tok, width), bf16),
                            dma((group,)), dma((OUT_SLOTS,)), dma],
            compiler_params=pltpu.CompilerParams(vmem_limit_bytes=VMEM_LIMIT),
            name="dispatch",
        )(meta_all, h_all)
        return hidden_out, buf

    return jax.shard_map(device_step, mesh=mesh,
                         in_specs=(row_spec, P(), P(), P(), P(), row_spec, row_spec),
                         out_specs=(row_spec, buf_spec), check_vma=False)
```
